32 devices in a mesh: dp: 8 (over z, y), row: 2 (over x), col: 2 (over core).
Axes of the slice: x: 2, y: 2, z: 4, core: 2. Of those that a mesh axis runs over, the one named last changes fastest.
Arguments:
- stream: bfloat16 [4096, 2560], P(('dp', 'row'), 'col'), may hold values from -45 to 45
- scale_first: float32 [2560], P('col'), may hold values from -0.5 to 0.5
- branch_weight: bfloat16 [2560, 2560], P('col', ('row', 'dp')), may hold values from -0.125 to 0.125
- branch_bias: float32 [2560], P('row'), may hold values from -3 to 3
- mixer_weight: bfloat16 [2560, 2560], P('col', ('row', 'dp')), may hold values from -0.125 to 0.125
- mixer_bias: float32 [2560], P('row'), may hold values from -3 to 3
- conv_weight: float32 [4, 2560], P(None, 'row'), may hold values from -3 to 3
- conv_bias: float32 [2560], P('row'), may hold values from -2 to 2
- decay_weight: bfloat16 [10, 256, 256], P('row'), may hold values from -0.375 to 0.375
- decay_bias: float32 [2560], P('row'), may hold values from -3 to 3
- input_weight: bfloat16 [10, 256, 256], P('row'), may hold values from -0.375 to 0.375
- input_bias: float32 [2560], P('row'), may hold values from -3 to 3
- decay_param: float32 [2560], P('row'), may hold values from -13 to -4
- output_weight: bfloat16 [2560, 2560], P('row', ('col', 'dp')), may hold values from -0.3125 to 0.3125
- output_bias: float32 [2560], P('col'), may hold values from -3 to 3
- scale_second: float32 [2560], P('col'), may hold values from -0.5 to 0.5
- gate_weight: bfloat16 [2560, 7680], P('col', ('row', 'dp')), may hold values from -0.125 to 0.125
- gate_bias: float32 [7680], P('row'), may hold values from -3 to 3
- up_weight: bfloat16 [2560, 7680], P('col', ('row', 'dp')), may hold values from -0.125 to 0.125
- up_bias: float32 [7680], P('row'), may hold values from -3 to 3
- down_weight: bfloat16 [7680, 2560], P('row', ('col', 'dp')), may hold values from -0.09375 to 0.09375
- down_bias: float32 [2560], P('col'), may hold values from -3 to 3
- cotangent: bfloat16 [4096, 2560], P(('dp', 'row'), 'col'), may hold values from -6 to 6
Outputs:
- result: bfloat16 [4096, 2560], P(('dp', 'row'), 'col')
- grad_stream: float32 [4096, 2560], P(('dp', 'row'), 'col')
- grad_scale_first: float32 [2560], P('col')
- grad_branch_weight: float32 [2560, 2560], P('col', ('row', 'dp'))
- grad_branch_bias: float32 [2560], P('row')
- grad_mixer_weight: float32 [2560, 2560], P('col', ('row', 'dp'))
- grad_mixer_bias: float32 [2560], P('row')
- grad_conv_weight: float32 [4, 2560], P(None, 'row')
- grad_conv_bias: float32 [2560], P('row')
- grad_decay_weight: float32 [10, 256, 256], P('row')
- grad_decay_bias: float32 [2560], P('row')
- grad_input_weight: float32 [10, 256, 256], P('row')
- grad_input_bias: float32 [2560], P('row')
- grad_decay_param: float32 [2560], P('row')
- grad_output_weight: float32 [2560, 2560], P('row', ('col', 'dp'))
- grad_output_bias: float32 [2560], P('col')
- grad_scale_second: float32 [2560], P('col')
- grad_gate_weight: float32 [2560, 7680], P('col', ('row', 'dp'))
- grad_gate_bias: float32 [7680], P('row')
- grad_up_weight: float32 [2560, 7680], P('col', ('row', 'dp'))
- grad_up_bias: float32 [7680], P('row')
- grad_down_weight: float32 [7680, 2560], P('row', ('col', 'dp'))
- grad_down_bias: float32 [2560], P('col')
The draws below stay inside these ranges and needn't reach their ends.
All inputs are finite; a program needn't handle non-finite values.
Results may differ from the reference program's by a relative error of at most 0.022.
Values may be sent and summed in bfloat16 or wider, within the bound.
A program may use at most 320 MiB of HBM per device.

```python
import math
import jax
import jax.numpy as jnp
from jax import lax

D = 2560
FF = 7680
HEADS = 10
CONV = 4
TOK = 256
LEN = 4096
BLK = 256
TOKENS = 4096


def draw_stream(key, part):
    base_key, row_key, col_key = jax.random.split(key, 3)
    base_values = jnp.clip(jax.random.normal(base_key, (TOKENS, D), jnp.float32), -5.0, 5.0)
    row_scale = jnp.exp(jax.random.uniform(row_key, (TOKENS, 1), jnp.float32, math.log(0.3), math.log(3.0)))
    col_scale = jnp.exp(jax.random.uniform(col_key, (HEADS,), jnp.float32, math.log(0.3), math.log(3.0)))
    return (base_values * row_scale * jnp.repeat(col_scale, D // HEADS)[None, :]).astype(jnp.bfloat16)


def draw_decay_param(key, part):
    low_rate = 0.1 / LEN
    high_rate = 1.0 / 30.0
    decay_rate = jnp.exp(jax.random.uniform(key, (D,), jnp.float32, math.log(low_rate), math.log(high_rate)))
    return jnp.log(jnp.expm1(decay_rate / 4.0))


def levels(rng, shape, cuts, smallest, largest):
    gain, own = 1.0, jax.random.fold_in(rng, 6)
    for dim, parts in cuts:
        steps = jnp.exp(jax.random.uniform(jax.random.fold_in(own, dim), (parts,), jnp.float32, smallest / len(cuts), largest / len(cuts)))
        gain = gain * jnp.repeat(steps, shape[dim] // parts).reshape([-1 if axis == dim else 1 for axis in range(len(shape))])
    return gain


def scatter_about(stream_key, extent, deviation, most, pieces=(), kind=jnp.bfloat16):
    drawn = deviation * jax.random.normal(stream_key, extent, jnp.float32)
    if pieces:
        drawn = drawn * levels(stream_key, extent, pieces, -0.22, 0.18)
    return jnp.clip(drawn, -most, most).astype(kind)


def setup_inputs(seed: int = 0) -> dict:
    arg_keys = jax.random.split(jax.random.key(seed), 24)
    stream = draw_stream(jax.random.fold_in(arg_keys[23], 71), 0)
    scale_first = jnp.clip(jax.random.uniform(arg_keys[1], (D,), jnp.float32, -0.5, 0.5) * levels(arg_keys[1], (D,), ((0, 2),), -0.4, 0.0), -0.5, 0.5)
    branch_weight = scatter_about(arg_keys[2], (D, D), D ** -0.5, 0.125, ((0, 2), (1, 16)))
    branch_bias = scatter_about(arg_keys[3], (D,), 0.5, 3.0, ((0, 2),), jnp.float32)
    mixer_weight = scatter_about(arg_keys[4], (D, D), D ** -0.5, 0.125, ((0, 2), (1, 16)))
    mixer_bias = scatter_about(arg_keys[5], (D,), 0.5, 3.0, ((0, 2),), jnp.float32)
    conv_weight = scatter_about(arg_keys[6], (CONV, D), 0.5, 3.0, ((1, 2),), jnp.float32)
    conv_bias = scatter_about(arg_keys[7], (D,), 0.3, 2.0, ((0, 2),), jnp.float32)
    decay_weight = scatter_about(arg_keys[8], (HEADS, BLK, BLK), BLK ** -0.5, 0.375, ((0, 2),))
    decay_bias = scatter_about(arg_keys[9], (D,), 0.5, 3.0, ((0, 2),), jnp.float32)
    input_weight = scatter_about(arg_keys[10], (HEADS, BLK, BLK), BLK ** -0.5, 0.375, ((0, 2),))
    input_bias = scatter_about(arg_keys[11], (D,), 0.5, 3.0, ((0, 2),), jnp.float32)
    decay_param = draw_decay_param(jax.random.fold_in(arg_keys[23], 71), 0)
    output_weight = scatter_about(arg_keys[13], (D, D), (D // 8) ** -0.5, 0.3125, ((0, 2), (1, 16)))
    output_bias = scatter_about(arg_keys[14], (D,), 0.5, 3.0, ((0, 2),), jnp.float32)
    scale_second = jnp.clip(jax.random.uniform(arg_keys[15], (D,), jnp.float32, -0.5, 0.5) * levels(arg_keys[15], (D,), ((0, 2),), -0.4, 0.0), -0.5, 0.5)
    gate_weight = scatter_about(arg_keys[16], (D, FF), D ** -0.5, 0.125, ((0, 2), (1, 16)))
    gate_bias = scatter_about(arg_keys[17], (FF,), 0.5, 3.0, ((0, 2),), jnp.float32)
    up_weight = scatter_about(arg_keys[18], (D, FF), D ** -0.5, 0.125, ((0, 2), (1, 16)))
    up_bias = scatter_about(arg_keys[19], (FF,), 0.5, 3.0, ((0, 2),), jnp.float32)
    down_weight = scatter_about(arg_keys[20], (FF, D), (FF // 2) ** -0.5, 0.09375, ((0, 2), (1, 16)))
    down_bias = scatter_about(arg_keys[21], (D,), 0.5, 3.0, ((0, 2),), jnp.float32)
    cotangent = scatter_about(arg_keys[22], (TOKENS, D), 1.0, 6.0, ((0, 16), (1, 2)))
    return {"stream": stream, "scale_first": scale_first, "branch_weight": branch_weight, "branch_bias": branch_bias, "mixer_weight": mixer_weight, "mixer_bias": mixer_bias, "conv_weight": conv_weight, "conv_bias": conv_bias, "decay_weight": decay_weight, "decay_bias": decay_bias, "input_weight": input_weight, "input_bias": input_bias, "decay_param": decay_param, "output_weight": output_weight, "output_bias": output_bias, "scale_second": scale_second, "gate_weight": gate_weight, "gate_bias": gate_bias, "up_weight": up_weight, "up_bias": up_bias, "down_weight": down_weight, "down_bias": down_bias, "cotangent": cotangent}


@jax.custom_vjp
def low(v):
    return lax.optimization_barrier(v.astype(jnp.bfloat16)).astype(jnp.float32)

@jax.custom_vjp
def low_back(v):
    return v

def low_keep(v):
    return (low(v), None)

def low_pass(kept, grad):
    return (grad,)

def back_keep(v):
    return (v, None)

def back_low(kept, grad):
    return (low(grad),)
low.defvjp(low_keep, low_pass)
low_back.defvjp(back_keep, back_low)
EPSILON = 1e-06
SQRT_FLOOR = 0.0001

def matmul(left_side, right_side):
    return jnp.dot(left_side, right_side, precision=lax.Precision.HIGHEST, preferred_element_type=jnp.float32)

def normalize(values, scale_vec):
    inverse = lax.rsqrt(lax.optimization_barrier(jnp.mean(values * values, axis=-1, keepdims=True)) + EPSILON)
    return values * inverse * (1.0 + scale_vec)

def gelu_tanh(values):
    return jax.nn.gelu(values, approximate=True)

def block_diag(values, weight):
    head_count = weight.shape[0]
    head_parts = values.reshape(values.shape[0], head_count, weight.shape[1])
    mapped = jnp.einsum('thi,hij->thj', head_parts, weight, precision=lax.Precision.HIGHEST)
    return mapped.reshape(values.shape[0], -1)

def gates_of(decay_pre, input_pre, decay_param, conv_low, starts):
    rate_gate = jax.nn.sigmoid(decay_pre)
    in_gate = jax.nn.sigmoid(input_pre)
    log_decay = -8.0 * jax.nn.softplus(decay_param) * rate_gate
    retain = jnp.where(starts, 0.0, jnp.exp(log_decay))
    multiplier = jnp.where(starts, 1.0, jnp.sqrt(jnp.maximum(-jnp.expm1(2.0 * log_decay), SQRT_FLOOR)))
    return (retain, multiplier * in_gate * conv_low)

def recur_step(carried, item_pair):
    updated = item_pair[0] * carried + item_pair[1]
    return (updated, updated)

def forward(stream, scale_first, branch_weight, branch_bias, mixer_weight, mixer_bias, conv_weight, conv_bias, decay_weight, decay_bias, input_weight, input_bias, decay_param, output_weight, output_bias, scale_second, gate_weight, gate_bias, up_weight, up_bias, down_weight, down_bias):
    token_count = stream.shape[0]
    model_width = stream.shape[1]
    blocks = token_count // TOK
    margin = CONV - 1
    position = jnp.arange(token_count, dtype=jnp.int32) % LEN

    def run_block(carried, inputs):
        state_in, tail_rows = carried
        rows_in, positions = inputs
        row_count = rows_in.shape[0]
        normed_first = low(normalize(rows_in, scale_first))
        branch_pre = low_back(matmul(normed_first, branch_weight)) + branch_bias
        branch_act = gelu_tanh(branch_pre)
        mixer_pre = low_back(matmul(normed_first, mixer_weight)) + mixer_bias
        padded = jnp.concatenate([tail_rows, mixer_pre], axis=0)
        conv_out = conv_bias + jnp.zeros_like(mixer_pre)
        for offset in range(CONV):
            in_reach = (positions >= offset)[:, None]
            conv_out = conv_out + jnp.where(in_reach, conv_weight[offset] * padded[margin - offset:margin - offset + row_count], 0.0)
        conv_low = low(conv_out)
        decay_pre = low_back(block_diag(conv_low, decay_weight)) + decay_bias
        input_pre = low_back(block_diag(conv_low, input_weight)) + input_bias
        starts = (positions == 0)[:, None]
        retain, source = gates_of(decay_pre, input_pre, decay_param, conv_low, starts)
        state_last, states = lax.scan(recur_step, state_in, (retain, source))
        mixed_out = low(states * branch_act)
        first_out = rows_in + low_back(matmul(mixed_out, output_weight)) + output_bias
        normed_second = low(normalize(first_out, scale_second))
        gate_pre = low_back(matmul(normed_second, gate_weight)) + gate_bias
        up_pre = low_back(matmul(normed_second, up_weight)) + up_bias
        hidden = low(gelu_tanh(gate_pre) * up_pre)
        output = first_out + low_back(matmul(hidden, down_weight)) + down_bias
        return ((state_last, padded[row_count:]), output)
    initial = (jnp.zeros((model_width,), stream.dtype), jnp.zeros((margin, model_width), stream.dtype))
    final_carry, outputs = lax.scan(jax.checkpoint(run_block), initial, (stream.reshape(blocks, TOK, model_width), position.reshape(blocks, TOK)))
    return outputs.reshape(token_count, model_width)

def reference(stream, scale_first, branch_weight, branch_bias, mixer_weight, mixer_bias, conv_weight, conv_bias, decay_weight, decay_bias, input_weight, input_bias, decay_param, output_weight, output_bias, scale_second, gate_weight, gate_bias, up_weight, up_bias, down_weight, down_bias, cotangent):
    params = [array.astype(jnp.float32) for array in (stream, scale_first, branch_weight, branch_bias, mixer_weight, mixer_bias, conv_weight, conv_bias, decay_weight, decay_bias, input_weight, input_bias, decay_param, output_weight, output_bias, scale_second, gate_weight, gate_bias, up_weight, up_bias, down_weight, down_bias)]
    result, pullback = jax.vjp(forward, *params)
    gradients = pullback(cotangent.astype(jnp.float32))
    return (result.astype(jnp.bfloat16), gradients[0], gradients[1], gradients[2], gradients[3], gradients[4], gradients[5], gradients[6], gradients[7], gradients[8], gradients[9], gradients[10], gradients[11], gradients[12], gradients[13], gradients[14], gradients[15], gradients[16], gradients[17], gradients[18], gradients[19], gradients[20], gradients[21])
```

```python
import jax
import jax.numpy as jnp
from jax import lax
from jax.experimental import pallas as pl
from jax.experimental.pallas import tpu as pltpu
from jax.sharding import Mesh, PartitionSpec as P

D = 2560
CONV = 4
LEN = 4096
EPSILON = 1e-06
SQRT_FLOOR = 0.0001
TEAM = 4
NT = (((1,), (1,)), ((), ()))
TN = (((0,), (0,)), ((), ()))
F32 = jnp.float32
BF16 = jnp.bfloat16
DP = ("t", "f")
ORDER = ("t", "f", "col")


def dot_nn(a, b):
    return jnp.dot(a, b, preferred_element_type=F32)


def dot_nt(a, b):
    return lax.dot_general(a, b, NT, preferred_element_type=F32)


def dot_tn(a, b):
    return lax.dot_general(a, b, TN, preferred_element_type=F32)


def gather(x, axes, dim):
    return lax.all_gather(x, axes, axis=dim, tiled=True)


def scatter(x, axes, dim):
    return lax.psum_scatter(x, axes, scatter_dimension=dim, tiled=True)


def swap(x, axes, split, concat):
    return lax.all_to_all(x, axes, split_axis=split, concat_axis=concat, tiled=True)


def from_behind(x, axis, by):
    peers = lax.axis_size(axis)
    pairs = [(i, i + by) for i in range(peers) if 0 <= i + by < peers]
    return lax.ppermute(x, axis, pairs)


def scan_rows(retain, source, backward):
    rows, width = retain.shape
    tiles = rows // 8

    def kernel(r_ref, s_ref, c_ref, h_ref):
        row = lax.broadcasted_iota(jnp.int32, (8, width), 0)

        def step(i, carry):
            decay, state = carry
            at = pl.ds(pl.multiple_of(8 * (tiles - 1 - i if backward else i), 8), 8)
            r, s = r_ref[at, :], s_ref[at, :]
            for by in (1, 2, 4):
                keep = row < 8 - by if backward else row >= by
                shift = 8 - by if backward else by
                r_by = jnp.where(keep, pltpu.roll(r, shift, 0), 1.0)
                s_by = jnp.where(keep, pltpu.roll(s, shift, 0), 0.0)
                s = r * s_by + s
                r = r * r_by
            s = s + r * state
            r = r * decay
            c_ref[at, :] = r
            h_ref[at, :] = s
            end = 0 if backward else 7
            return r[end : end + 1, :], s[end : end + 1, :]

        lax.fori_loop(0, tiles, step, (jnp.ones((1, width), F32), jnp.zeros((1, width), F32)))

    return pl.pallas_call(
        kernel,
        out_shape=(jax.ShapeDtypeStruct((rows, width), F32),) * 2,
        in_specs=[pl.BlockSpec(memory_space=pltpu.VMEM)] * 2,
        out_specs=(pl.BlockSpec(memory_space=pltpu.VMEM),) * 2,
        name="scan_back" if backward else "scan_rows",
    )(retain, source)


def carry_in(decay, state, backward):
    count, mine = lax.axis_size(ORDER), lax.axis_index(ORDER)
    ends = lax.all_gather(jnp.stack([decay, state]), ORDER)
    running = jnp.zeros_like(state)
    for i in range(count - 1):
        peer = count - 1 - i if backward else i
        ahead = peer > mine if backward else peer < mine
        running = jnp.where(ahead, ends[peer, 0] * running + ends[peer, 1], running)
    return running


def gelu_tanh(values):
    return jax.nn.gelu(values, approximate=True)


def gates_of(decay_pre, input_pre, decay_param, conv_low, starts):
    rate_gate = jax.nn.sigmoid(decay_pre)
    in_gate = jax.nn.sigmoid(input_pre)
    log_decay = -8.0 * jax.nn.softplus(decay_param) * rate_gate
    retain = jnp.where(starts, 0.0, jnp.exp(log_decay))
    multiplier = jnp.where(
        starts, 1.0, jnp.sqrt(jnp.maximum(-jnp.expm1(2.0 * log_decay), SQRT_FLOOR))
    )
    return (retain, multiplier * in_gate * conv_low)


def feature_total(values):
    return lax.psum(values, "col")


def normalize(values, scale_vec):
    inverse = lax.rsqrt(
        feature_total(jnp.sum(values * values, axis=1, keepdims=True)) / D + EPSILON
    )
    return (values * inverse * (1.0 + scale_vec), inverse)


def normalize_back(gradient, values, inverse, scale_vec):
    weighted = gradient * (1.0 + scale_vec)
    scale_grad = jnp.sum(gradient * values * inverse, axis=0)
    inner_sum = feature_total(jnp.sum(weighted * values, axis=1, keepdims=True))
    return (inverse * weighted - values * inverse**3 * inner_sum / D, scale_grad)


def to_tokens(block):
    rows = gather(block, "row", 0)
    both = swap(rows.reshape(2, block.shape[0], block.shape[1]), "col", 0, 2)
    return rows, both[0]


def to_stream(partial):
    tokens, width = partial.shape
    halves = jnp.stack([partial[:, : width // 2], partial[:, width // 2 :]])
    return scatter(swap(halves, "col", 0, 1)[0], "row", 0)


def square_down(down_weight):
    width = down_weight.shape[1]
    share = down_weight.shape[0] // (2 * TEAM)
    pieces = down_weight.T.reshape(width, 2 * TEAM, share).transpose(1, 0, 2)
    pieces = swap(pieces, ("t", "col"), 0, 0)
    every = lax.all_gather(pieces, "f").reshape(-1, TEAM, 2, width, share)
    return every.transpose(2, 1, 0, 3, 4).reshape(-1, share)


def square_down_back(grad, fleet):
    share = grad.shape[1]
    every = grad.reshape(2, TEAM, fleet, -1, share).transpose(2, 1, 0, 3, 4)
    summed = scatter(every.reshape(fleet, 2 * TEAM, -1, share), "f", 0)[0]
    pieces = swap(summed, ("t", "col"), 0, 0)
    return pieces.transpose(0, 2, 1).reshape(2 * TEAM * share, -1)


def ffn_columns(weight):
    block = gather(weight.T, "f", 0)
    return swap(block, "col", 0, 1)


def ffn_columns_back(grad):
    return scatter(swap(grad, "col", 1, 0), "f", 0).T


def on_device(
    stream,
    scale_first,
    branch_weight,
    branch_bias,
    mixer_weight,
    mixer_bias,
    conv_weight,
    conv_bias,
    decay_weight,
    decay_bias,
    input_weight,
    input_bias,
    decay_param,
    output_weight,
    output_bias,
    scale_second,
    gate_weight,
    gate_bias,
    up_weight,
    up_bias,
    down_weight,
    down_bias,
    cotangent,
):
    fleet = lax.axis_size("f")
    mixer_t = gather(gather(mixer_weight.T, DP, 0), "col", 1)
    branch_t = gather(gather(branch_weight.T, DP, 0), "col", 1)
    output_t = gather(gather(output_weight.T, DP, 0), "col", 0)
    inner = mixer_t.shape[0]
    stream_wide = stream.astype(F32)
    normed_first, inverse_first = normalize(stream_wide, scale_first)
    first_rows, first_all = to_tokens(normed_first.astype(BF16))
    mixer_pre = dot_nt(first_all, mixer_t) + mixer_bias
    branch_pre = dot_nt(first_all, branch_t) + branch_bias
    branch_act, branch_back = jax.vjp(gelu_tanh, branch_pre)

    steps = mixer_pre.shape[0]
    first_token = lax.axis_index(ORDER) * steps
    position = (first_token + jnp.arange(steps, dtype=jnp.int32)) % LEN
    margin = CONV - 1
    left_edge = from_behind(mixer_pre[steps - margin :], ORDER, 1)
    padded = jnp.concatenate([left_edge, mixer_pre], axis=0)
    conv_out = conv_bias + jnp.zeros_like(mixer_pre)
    for offset in range(CONV):
        in_reach = (position >= offset)[:, None]
        conv_out = conv_out + jnp.where(
            in_reach, conv_weight[offset] * padded[margin - offset : margin - offset + steps], 0.0
        )
    conv_low = conv_out.astype(BF16)
    conv_wide = conv_low.astype(F32)
    heads, block = decay_weight.shape[0], decay_weight.shape[1]
    conv_heads = conv_low.reshape(steps, heads, block)
    parts = [conv_low[:, h * block : (h + 1) * block] for h in range(heads)]
    decay_pre = jnp.concatenate([dot_nn(x, decay_weight[h]) for h, x in enumerate(parts)], 1) + decay_bias
    input_pre = jnp.concatenate([dot_nn(x, input_weight[h]) for h, x in enumerate(parts)], 1) + input_bias
    starts = (position == 0)[:, None]

    def gate_values(decay_in, input_in, param_in, conv_in):
        return gates_of(decay_in, input_in, param_in, conv_in, starts)

    (retain, source), gate_back = jax.vjp(gate_values, decay_pre, input_pre, decay_param, conv_wide)
    cumulative, local_state = scan_rows(retain, source, False)
    state_in = carry_in(cumulative[-1], local_state[-1], False)
    states = local_state + cumulative * state_in
    mixed_low = (states * branch_act).astype(BF16)
    out_proj = to_stream(dot_nt(mixed_low, output_t).astype(BF16)).astype(F32)
    first_out = stream_wide + out_proj + output_bias
    normed_second, inverse_second = normalize(first_out, scale_second)

    gate_t = ffn_columns(gate_weight)
    up_t = ffn_columns(up_weight)
    down_t = square_down(down_weight)
    share = gate_t.shape[0]
    mine = (lax.axis_index("t") * 2 + lax.axis_index("col")) * share
    gate_b = lax.dynamic_slice(gate_bias, (mine,), (share,))
    up_b = lax.dynamic_slice(up_bias, (mine,), (share,))

    def everywhere(x):
        return gather(gather(x, ("t", "row"), 0), "col", 1)

    def home(x):
        return scatter(scatter(x.astype(BF16), "col", 1), ("t", "row"), 0).astype(F32)

    second_all = everywhere(normed_second.astype(BF16))
    cot_all = everywhere(cotangent)
    gate_pre = dot_nt(second_all, gate_t) + gate_b
    up_pre = dot_nt(second_all, up_t) + up_b
    hidden, hidden_back = jax.vjp(lambda g, u: gelu_tanh(g) * u, gate_pre, up_pre)
    hidden_low = hidden.astype(BF16)
    delta_hidden = dot_nn(cot_all, down_t)
    delta_gate, delta_up = hidden_back(delta_hidden)
    gate_low, up_low = delta_gate.astype(BF16), delta_up.astype(BF16)
    delta_second = home(dot_nn(gate_low, gate_t) + dot_nn(up_low, up_t))
    down_proj = home(dot_nt(hidden_low, down_t))
    result = (first_out + down_proj + down_bias).astype(BF16)
    delta_result = cotangent.astype(F32)
    grad_gate = ffn_columns_back(dot_tn(gate_low, second_all).astype(BF16)).astype(F32)
    grad_up = ffn_columns_back(dot_tn(up_low, second_all).astype(BF16)).astype(F32)
    grad_down = square_down_back(dot_tn(cot_all, hidden_low).astype(BF16), fleet).astype(F32)

    norm_second_part, grad_scale_second = normalize_back(
        delta_second, first_out, inverse_second, scale_second
    )
    delta_first = delta_result + norm_second_part
    out_rows, out_all = to_tokens(delta_first.astype(BF16))
    delta_mixed = dot_nn(out_all, output_t)
    grad_output = scatter(dot_tn(out_rows, gather(mixed_low, "col", 0)).astype(BF16), DP, 0)
    delta_state = delta_mixed * branch_act
    (delta_branch,) = branch_back(delta_mixed * states)
    branch_low = delta_branch.astype(BF16)
    grad_branch = scatter(dot_tn(gather(branch_low, "col", 0), first_rows).astype(BF16), DP, 0)
    ones_row = jnp.ones((1, inner), F32)
    retain_next = jnp.concatenate([retain[1:], ones_row], axis=0)
    suffix, local_back = scan_rows(retain_next, delta_state, True)
    back_in = carry_in(retain[0] * suffix[0], retain[0] * local_back[0], True)
    back_state = local_back + suffix * back_in
    state_prev = jnp.concatenate([state_in[None], states[:-1]], axis=0)
    delta_decay_pre, delta_input_pre, grad_decay_param, delta_conv = gate_back(
        (back_state * state_prev, back_state)
    )
    decay_low = delta_decay_pre.astype(BF16)
    input_low = delta_input_pre.astype(BF16)

    def split(x):
        return [x[:, h * block : (h + 1) * block] for h in range(heads)]

    grad_decay_weight = jnp.stack([dot_tn(a, b) for a, b in zip(parts, split(decay_low))])
    grad_input_weight = jnp.stack([dot_tn(a, b) for a, b in zip(parts, split(input_low))])
    delta_conv = delta_conv + jnp.concatenate(
        [dot_nt(a, decay_weight[h]) for h, a in enumerate(split(decay_low))], 1
    )
    delta_conv = delta_conv + jnp.concatenate(
        [dot_nt(a, input_weight[h]) for h, a in enumerate(split(input_low))], 1
    )
    delta_padded = jnp.zeros_like(padded)
    conv_grads = []
    for offset in range(CONV):
        in_reach = (position >= offset)[:, None]
        masked = jnp.where(in_reach, delta_conv, 0.0)
        conv_grads.append(
            jnp.sum(masked * padded[margin - offset : margin - offset + steps], axis=0)
        )
        delta_padded = delta_padded + jnp.pad(
            masked * conv_weight[offset], ((margin - offset, offset), (0, 0))
        )
    grad_conv_weight = jnp.stack(conv_grads, axis=0)
    right_edge = from_behind(delta_padded[:margin], ORDER, -1)
    delta_mixer = delta_padded[margin:] + jnp.pad(right_edge, ((steps - margin, 0), (0, 0)))
    mixer_low = delta_mixer.astype(BF16)
    grad_mixer = scatter(dot_tn(gather(mixer_low, "col", 0), first_rows).astype(BF16), DP, 0)
    delta_normed_first = to_stream(
        (dot_nn(branch_low, branch_t) + dot_nn(mixer_low, mixer_t)).astype(BF16)
    ).astype(F32)
    norm_first_part, grad_scale_first = normalize_back(
        delta_normed_first, stream_wide, inverse_first, scale_first
    )
    grad_stream = delta_first + norm_first_part

    stream_sums = lax.psum(
        jnp.stack(
            [
                grad_scale_first,
                grad_scale_second,
                jnp.sum(delta_first, axis=0),
                jnp.sum(delta_result, axis=0),
            ]
        ),
        ("t", "f", "row"),
    )

    def spread(x):
        return lax.dynamic_update_slice(jnp.zeros_like(gate_bias), x, (mine,))

    small = [
        jnp.sum(delta_branch, axis=0),
        jnp.sum(delta_mixer, axis=0),
        jnp.sum(delta_conv, axis=0),
        jnp.sum(delta_decay_pre, axis=0),
        jnp.sum(delta_input_pre, axis=0),
        grad_decay_param,
        spread(jnp.sum(delta_gate, axis=0)),
        spread(jnp.sum(delta_up, axis=0)),
        grad_conv_weight.reshape(-1),
    ]
    sizes = [x.shape[0] for x in small]
    total = lax.psum(jnp.concatenate(small), ORDER)
    sums, at = [], 0
    for size in sizes:
        sums.append(total[at : at + size])
        at += size
    grad_decay_weight, grad_input_weight = lax.psum((grad_decay_weight, grad_input_weight), ORDER)
    return (
        result,
        grad_stream,
        stream_sums[0],
        grad_branch.T.astype(F32),
        sums[0],
        grad_mixer.T.astype(F32),
        sums[1],
        sums[8].reshape(CONV, inner),
        sums[2],
        grad_decay_weight,
        sums[3],
        grad_input_weight,
        sums[4],
        sums[5],
        grad_output.T.astype(F32),
        stream_sums[2],
        stream_sums[1],
        grad_gate,
        sums[6],
        grad_up,
        sums[7],
        grad_down,
        stream_sums[3],
    )


def solution(mesh):
    shape = mesh.devices.shape
    names = mesh.axis_names
    fleet = mesh.shape["dp"] // TEAM
    at = names.index("dp")
    split_mesh = Mesh(
        mesh.devices.reshape(shape[:at] + (TEAM, fleet) + shape[at + 1 :]),
        names[:at] + DP + names[at + 1 :],
    )
    tokens, fan_in = P((*DP, "row"), "col"), P("col", ("row", *DP))
    fan_out, inner, wide = P("row", ("col", *DP)), P("row"), P("col")
    heads = P("row", None, None)
    return jax.shard_map(
        on_device,
        mesh=split_mesh,
        in_specs=(
            tokens, wide, fan_in, inner, fan_in, inner, P(None, "row"), inner,
            heads, inner, heads, inner, inner, fan_out, wide, wide,
            fan_in, inner, fan_in, inner, fan_out, wide, tokens,
        ),
        out_specs=(
            tokens, tokens, wide, fan_in, inner, fan_in, inner, P(None, "row"), inner,
            heads, inner, heads, inner, inner, fan_out, wide, wide,
            fan_in, inner, fan_in, inner, fan_out, wide,
        ),
        check_vma=False,
    )
```

```python
import jax
import jax.numpy as jnp
from jax import lax
from jax.experimental import pallas as pl
from jax.experimental.pallas import tpu as pltpu
from jax.sharding import Mesh, PartitionSpec as P


D = 2560
CONV = 4
LEN = 4096
EPSILON = 1e-06
SQRT_FLOOR = 0.0001
TEAM = 4
NT = (((1,), (1,)), ((), ()))
TN = (((0,), (0,)), ((), ()))
F32 = jnp.float32
BF16 = jnp.bfloat16
DP = ("t", "f")
ORDER = ("t", "f", "col")


def dot_nn(a, b):
    return jnp.dot(a, b, preferred_element_type=F32)


def dot_nt(a, b):
    return lax.dot_general(a, b, NT, preferred_element_type=F32)


def dot_tn(a, b):
    return lax.dot_general(a, b, TN, preferred_element_type=F32)


MESH = pl.DeviceIdType.MESH
ANY = pl.BlockSpec(memory_space=pl.ANY)
VMEM = pl.BlockSpec(memory_space=pltpu.VMEM)


def peer_of(axis, k):
    n, me = lax.axis_size(axis), lax.axis_index(axis)
    if k == 0:
        return me
    if n == 2:
        return 1 - me
    if n == 4:
        return (me + 1 - 2 * (me % 2), (me + 2) % 4, 3 - me)[k - 1]
    return (me + k) % n


def source_of(axis, k):
    n, me = lax.axis_size(axis), lax.axis_index(axis)
    return peer_of(axis, k) if n in (2, 4) else (me + n - k) % n


def offsets(axis):
    n = lax.axis_size(axis)
    return (1, 3, 2) if n == 4 else tuple(range(1, n))


def grid_of(axes, far_first=False):
    grid = [()]
    for axis in axes:
        near = (0,) + offsets(axis)
        grid = [tag + (k,) for tag in grid for k in (near[::-1] if far_first else near)]
    return grid


def hail(peers):
    for peer in peers:
        pl.semaphore_signal(pltpu.get_barrier_semaphore(), inc=1, device_id=peer, device_id_type=MESH)


def greet(peers):
    hail(peers)
    pl.semaphore_wait(pltpu.get_barrier_semaphore(), len(peers))


def only(condition, act):
    if condition is None:
        act()
    else:
        pl.when(condition)(act)


def along(*axes):
    return [{axis: peer_of(axis, k)} for axis in axes for k in offsets(axis)]


def across(*axes):
    return [
        {axis: peer_of(axis, k) for axis, k in zip(axes, tag)} for tag in grid_of(axes) if any(tag)
    ]


class Copies:
    def __init__(self):
        self.sent = []

    def push(self, src, dst, send, recv, peer, condition=None):
        copy = pltpu.make_async_remote_copy(
            src_ref=src, dst_ref=dst, send_sem=send, recv_sem=recv, device_id=peer, device_id_type=MESH
        )
        only(condition, copy.start)
        self.sent.append((condition, copy.wait_send))

    def arrive(self, dst, send, recv, peer):
        pltpu.make_async_remote_copy(
            src_ref=dst, dst_ref=dst, send_sem=send, recv_sem=recv, device_id=peer, device_id_type=MESH
        ).wait_recv()

    def keep(self, src, dst, sem):
        copy = pltpu.make_async_copy(src, dst, sem)
        copy.start()
        self.sent.append((None, copy.wait))

    def drain(self):
        for condition, wait in self.sent:
            only(condition, wait)


def leading(ref, coords):
    return ref.at[tuple(coords)]


class Gather(Copies):
    def __init__(self, src, out, axes, sems, place=leading):
        super().__init__()
        self.src, self.out, self.axes, self.place = src, out, axes, place
        self.send, self.recv, self.own = sems
        self.size, self.at = lax.axis_size(axes[0]), lax.axis_index(axes[0])
        self.nobody = (0,) * len(axes)
        self.waves = {}
        line = [0] + [v for far in range(1, self.size) for v in (-far, far)]
        for v in line:
            for rest in grid_of(axes[1:]):
                tag = (v,) + rest
                if any(tag):
                    self.waves.setdefault(sum(1 for k in tag if k), []).append(tag)

    @staticmethod
    def scratch(axes):
        sizes = [lax.axis_size(a) for a in axes]
        shape = (2 * sizes[0] - 1,) + tuple(sizes[1:])
        return [pltpu.SemaphoreType.DMA(shape), pltpu.SemaphoreType.DMA(shape), pltpu.SemaphoreType.DMA]

    def index(self, tag):
        return (tag[0] + self.size - 1,) + tag[1:]

    def exists(self, far):
        if far == 0:
            return None
        return self.at + far >= 0 if far < 0 else self.at + far < self.size

    def slot(self, tag):
        rest = [source_of(a, k) for a, k in zip(self.axes[1:], tag[1:])]
        return self.place(self.out, [self.at + tag[0]] + rest)

    def spread(self, tag):
        last = max([i for i, k in enumerate(tag) if k], default=-1)
        here = self.exists(tag[0])
        src = self.slot(tag) if any(tag) else self.src

        def send(there, peer, condition):
            if here is not None and condition is not None:
                condition = here & condition
            elif condition is None:
                condition = here
            at = self.index(there)
            self.push(src, self.slot(tag), self.send.at[at], self.recv.at[at], peer, condition)

        if last <= 0:
            if 0 <= tag[0] < self.size - 1:
                send((tag[0] + 1,) + tag[1:], {self.axes[0]: self.at - 1}, self.at > 0)
            if -self.size + 1 < tag[0] <= 0:
                send((tag[0] - 1,) + tag[1:], {self.axes[0]: self.at + 1}, self.at < self.size - 1)
        for level in range(max(last, 0) + 1, len(self.axes)):
            axis = self.axes[level]
            for k in offsets(axis):
                send(tag[:level] + (k,) + tag[level + 1 :], {axis: peer_of(axis, k)}, None)

    def begin(self):
        self.spread(self.nobody)
        self.keep(self.src, self.slot(self.nobody), self.own)

    def stage(self, wave):
        for tag in self.waves.get(wave, ()):
            last = max(i for i, k in enumerate(tag) if k)
            if last:
                peer = {self.axes[last]: peer_of(self.axes[last], tag[last])}
            else:
                peer = {self.axes[0]: self.at + (1 if tag[0] > 0 else -1)}
            at = self.index(tag)
            only(
                self.exists(tag[0]),
                lambda: self.arrive(self.slot(tag), self.send.at[at], self.recv.at[at], peer),
            )
            self.spread(tag)


def sum_into(out, parts):
    rows = out.shape[0]
    step = next(n for n in (32, 16, 8, rows) if rows % n == 0)

    def some(i, carry):
        at = pl.ds(pl.multiple_of(i * step, step), step)
        total = parts[0][at, :].astype(F32)
        for part in parts[1:]:
            total = total + part[at, :].astype(F32)
        out[at, :] = total.astype(out.dtype)
        return carry

    lax.fori_loop(0, rows // step, some, 0)


class Reduce(Copies):
    def __init__(self, src, out, axes, scratch, place=leading):
        super().__init__()
        n = len(axes)
        self.src, self.out, self.axes, self.place = src, out, axes, place
        self.part = {i + 1: scratch[i] for i in range(n - 1)}
        rest = scratch[n - 1 :]
        self.come = rest[:n]
        self.send = rest[n : 2 * n]
        self.recv = rest[2 * n : 3 * n]

    @staticmethod
    def count(axes):
        return 4 * len(axes) - 1

    @staticmethod
    def scratch(axes, block, dtype):
        sizes = tuple(lax.axis_size(a) for a in axes)
        n = len(axes)
        parts = [pltpu.VMEM(sizes[:i] + block, dtype) for i in range(1, n)]
        come = [pltpu.VMEM((sizes[i] - 1,) + sizes[:i] + block, dtype) for i in range(n)]
        sems = [pltpu.SemaphoreType.DMA((sizes[i] - 1,) + sizes[:i]) for i in range(n)]
        return parts + come + sems + sems

    def coords(self, tag):
        return tuple(peer_of(a, k) for a, k in zip(self.axes, tag))

    def forward(self, tag, src):
        level = len(tag) - 1
        k, prefix = tag[-1], tag[:-1]
        axis = self.axes[level]
        self.push(
            src,
            self.come[level].at[(k - 1,) + self.coords(prefix)],
            self.send[level].at[(k - 1,) + prefix],
            self.recv[level].at[(k - 1,) + prefix],
            {axis: peer_of(axis, k)},
        )

    def order(self, level):
        return sorted(grid_of(self.axes[:level], True), key=lambda tag: tag[-1:] == (0,))

    def begin(self):
        for tag in self.order(len(self.axes)):
            if tag[-1]:
                self.forward(tag, self.place(self.src, self.coords(tag)))

    def held(self, level, coords):
        return self.place(self.src, coords) if level == len(self.axes) else self.part[level].at[coords]

    def step(self, level, tag):
        axis = self.axes[level]
        here = self.coords(tag)
        parts = [self.held(level + 1, here + (lax.axis_index(axis),))]
        for k in offsets(axis):
            slot = self.come[level].at[(k - 1,) + here]
            at = (k - 1,) + tag
            self.arrive(slot, self.send[level].at[at], self.recv[level].at[at], {axis: source_of(axis, k)})
            parts.append(slot)
        target = self.held(level, here) if level else self.out
        sum_into(target, parts)
        if level and tag[-1]:
            self.forward(tag, target)

    def stage(self, wave):
        level = len(self.axes) - wave
        if level >= 0:
            for tag in self.order(level):
                self.step(level, tag)


class Settle(Reduce):
    def __init__(self, src, out, axes, scratch, place):
        Copies.__init__(self)
        n = len(axes)
        self.src, self.out, self.axes, self.place = src, out, axes, place
        self.come, self.send, self.recv = scratch[:n], scratch[n : 2 * n], scratch[2 * n :]

    @staticmethod
    def scratch(axes, block, dtype):
        return Reduce.scratch(axes, block, dtype)[len(axes) - 1 :]

    def held(self, level, coords):
        return self.place(self.src, coords + tuple(lax.axis_index(a) for a in self.axes[level:]))


class Spread(Copies):
    def __init__(self, src, out, axes, sems):
        super().__init__()
        self.src, self.out, self.axes = src, out, axes
        self.send, self.recv, self.own = sems
        self.waves = {}
        for tag in grid_of(axes):
            if any(tag):
                self.waves.setdefault(sum(1 for k in tag if k), []).append(tag)

    @staticmethod
    def scratch(axes):
        shape = shape_of(axes)
        return [pltpu.SemaphoreType.DMA(shape), pltpu.SemaphoreType.DMA(shape), pltpu.SemaphoreType.DMA]

    def slot(self, tag):
        return self.out.at[tuple(source_of(a, k) for a, k in zip(self.axes, tag))]

    def spread(self, tag):
        last = max([i for i, k in enumerate(tag) if k], default=-1)
        for level in range(last + 1, len(self.axes)):
            axis = self.axes[level]
            for k in offsets(axis):
                at = tag[:level] + (k,) + tag[level + 1 :]
                src = self.slot(tag) if any(tag) else self.src
                self.push(src, self.slot(tag), self.send.at[at], self.recv.at[at], {axis: peer_of(axis, k)})

    def begin(self):
        nobody = (0,) * len(self.axes)
        self.spread(nobody)
        self.keep(self.src, self.slot(nobody), self.own)

    def stage(self, wave):
        for tag in self.waves.get(wave, ()):
            last = max(i for i, k in enumerate(tag) if k)
            peer = {self.axes[last]: peer_of(self.axes[last], tag[last])}
            self.arrive(self.slot(tag), self.send.at[tag], self.recv.at[tag], peer)
            self.spread(tag)


class Fan(Copies):
    def __init__(self, src, out, axis, sems):
        super().__init__()
        self.src, self.out, self.axis = src, out, axis
        self.send, self.recv, self.own = sems
        self.half = lax.axis_size(axis) // 2

    @staticmethod
    def scratch(axis):
        n = lax.axis_size(axis)
        return [pltpu.SemaphoreType.DMA((n,)), pltpu.SemaphoreType.DMA((n, 2)), pltpu.SemaphoreType.DMA]

    def slot(self, owner, core):
        width = self.src.shape[-1]
        return self.out.at[owner % self.half, :, pl.ds(pl.multiple_of(core * width, width), width)]

    def begin(self):
        me, core = lax.axis_index(self.axis), lax.axis_index("col")
        target = me // self.half
        slot = self.slot(me, core)
        self.copies = []
        for k in offsets(self.axis):
            peer = {self.axis: peer_of(self.axis, k), "col": target}
            for c in (0, 1):

                @pl.when(core == c)
                def _(c=c):
                    pltpu.make_async_remote_copy(
                        src_ref=self.src, dst_ref=slot, send_sem=self.send.at[k], recv_sem=self.recv.at[k, c],
                        device_id=peer, device_id_type=MESH,
                    ).start()

        @pl.when(target == core)
        def _():
            pltpu.make_async_copy(self.src, slot, self.own).start()

        for c in (0, 1):

            @pl.when((target != core) & (core == c))
            def _(c=c):
                pltpu.make_async_remote_copy(
                    src_ref=self.src, dst_ref=slot, send_sem=self.send.at[0], recv_sem=self.recv.at[0, c],
                    device_id={"col": 1 - core}, device_id_type=MESH,
                ).start()

    def stage(self, wave):
        if wave != 1:
            return
        me, core = lax.axis_index(self.axis), lax.axis_index("col")
        for k in (0,) + offsets(self.axis):
            owner = source_of(self.axis, k)
            for c in (0, 1):
                expected = owner // self.half == core
                if k == 0:
                    expected = expected & (core != c)

                @pl.when(expected)
                def _(k=k, c=c, owner=owner):
                    slot = self.slot(owner, c)
                    self.arrive(slot, self.send.at[k], self.recv.at[k, c], {self.axis: owner, "col": c} if k else {"col": 1 - core})

    def drain(self):
        me, core = lax.axis_index(self.axis), lax.axis_index("col")
        target = me // self.half
        slot = self.slot(me, core)

        def left(k, peer):
            pltpu.make_async_remote_copy(
                src_ref=self.src, dst_ref=slot, send_sem=self.send.at[k], recv_sem=self.recv.at[k, 0],
                device_id=peer, device_id_type=MESH,
            ).wait_send()

        for k in offsets(self.axis):
            left(k, {self.axis: peer_of(self.axis, k), "col": target})

        @pl.when(target == core)
        def _():
            pltpu.make_async_copy(self.src, slot, self.own).wait()

        @pl.when(target != core)
        def _():
            left(0, {"col": 1 - core})


class Fold(Copies):
    def __init__(self, src, out, axis, scratch):
        super().__init__()
        self.src, self.out, self.axis = src, out, axis
        self.come, self.send, self.recv, self.own = scratch
        self.half = lax.axis_size(axis) // 2

    @staticmethod
    def scratch(axis, block, dtype):
        n = lax.axis_size(axis)
        return [
            pltpu.VMEM((n,) + block, dtype),
            pltpu.SemaphoreType.DMA((n, 2)),
            pltpu.SemaphoreType.DMA((n,)),
            pltpu.SemaphoreType.DMA,
        ]

    def each(self, visit, cores=(0, 1)):
        me, core = lax.axis_index(self.axis), lax.axis_index("col")
        for k in offsets(self.axis) + (0,):
            owner = peer_of(self.axis, k)
            for c in cores:

                @pl.when(owner // self.half == core)
                def _(k=k, c=c, owner=owner):
                    piece = self.src.at[c, owner % self.half]
                    if k:
                        visit(k, c, piece, {self.axis: owner, "col": c})
                    else:

                        @pl.when(core == c)
                        def _():
                            visit(k, None, piece, None)

                        @pl.when(core != c)
                        def _():
                            visit(k, c, piece, {"col": 1 - core})

    def begin(self, cores=(0, 1)):
        def start(k, c, piece, peer):
            if peer is None:
                pltpu.make_async_copy(piece, self.come.at[k], self.own).start()
            else:
                pltpu.make_async_remote_copy(
                    src_ref=piece, dst_ref=self.come.at[k], send_sem=self.send.at[k, c], recv_sem=self.recv.at[k],
                    device_id=peer, device_id_type=MESH,
                ).start()

        self.each(start, cores)

    def stage(self, wave):
        if wave != 1:
            return
        me, core = lax.axis_index(self.axis), lax.axis_index("col")
        holder = me // self.half
        for k in offsets(self.axis):
            peer = {self.axis: source_of(self.axis, k), "col": holder}
            self.arrive(self.come.at[k], self.send.at[k, 0], self.recv.at[k], peer)

        @pl.when(holder != core)
        def _():
            self.arrive(self.come.at[0], self.send.at[0, 0], self.recv.at[0], {"col": 1 - core})

        @pl.when(holder == core)
        def _():
            pltpu.make_async_copy(self.src.at[0, 0], self.come.at[0], self.own).wait()

        sum_into(self.out, [self.come.at[k] for k in (0,) + offsets(self.axis)])

    def drain(self):
        def left(k, c, piece, peer):
            if peer is not None:
                pltpu.make_async_remote_copy(
                    src_ref=piece, dst_ref=self.come.at[k], send_sem=self.send.at[k, c], recv_sem=self.recv.at[k],
                    device_id=peer, device_id_type=MESH,
                ).wait_send()

        self.each(left)


class Trade(Copies):
    def __init__(self, src, out, scratch):
        super().__init__()
        self.src, self.out = src, out
        self.cut, self.send, self.recv, self.own = scratch

    @staticmethod
    def scratch(piece, dtype):
        shape = shape_of(("t", "col"))
        sems = [pltpu.SemaphoreType.DMA(shape), pltpu.SemaphoreType.DMA(shape), pltpu.SemaphoreType.DMA]
        return [pltpu.VMEM(shape + piece, dtype)] + sems

    def begin(self):
        share = self.cut.shape[-1]
        for i in range(2 * TEAM):
            self.cut[i // 2, i % 2] = self.src[:, i * share : (i + 1) * share]
        t, c = lax.axis_index("t"), lax.axis_index("col")
        for tag in grid_of(("t", "col")):
            to = peer_of("t", tag[0]), peer_of("col", tag[1])
            if any(tag):
                peer = {"t": to[0], "col": to[1]}
                self.push(self.cut.at[to], self.out.at[c, t], self.send.at[tag], self.recv.at[tag], peer)
        self.keep(self.cut.at[t, c], self.out.at[c, t], self.own)

    def stage(self, wave):
        if wave == 1:
            for tag in grid_of(("t", "col")):
                if any(tag):
                    peer = source_of("t", tag[0]), source_of("col", tag[1])
                    slot = self.out.at[peer[1], peer[0]]
                    self.arrive(slot, self.send.at[tag], self.recv.at[tag], {"t": peer[0], "col": peer[1]})


class Undeal(Copies):
    def __init__(self, src, out, scratch):
        super().__init__()
        self.src, self.out = src, out
        self.come, self.part, self.send, self.recv, self.send_on, self.recv_on, self.own = scratch

    @staticmethod
    def scratch(block, dtype):
        f, t, c = (lax.axis_size(a) for a in ("f", "t", "col"))
        first, second = pltpu.SemaphoreType.DMA((f - 1, t, c)), pltpu.SemaphoreType.DMA((t, c))
        return [
            pltpu.VMEM((f - 1, t, c) + block, dtype),
            pltpu.VMEM((t, c) + block, dtype),
            first, first, second, second, pltpu.SemaphoreType.DMA,
        ]

    def begin(self):
        for tag in grid_of(("t", "col"), True):
            to = peer_of("t", tag[0]), peer_of("col", tag[1])
            for k in offsets("f"):
                at = (k - 1,) + tag
                self.push(
                    self.src.at[(peer_of("f", k),) + to], self.come.at[(k - 1,) + to],
                    self.send.at[at], self.recv.at[at], {"f": peer_of("f", k)},
                )

    def stage(self, wave):
        t, c, f = (lax.axis_index(a) for a in ("t", "col", "f"))
        if wave == 1:
            for tag in grid_of(("t", "col"), True):
                to = peer_of("t", tag[0]), peer_of("col", tag[1])
                parts = [self.src.at[(f,) + to]]
                for k in offsets("f"):
                    at = (k - 1,) + tag
                    slot = self.come.at[(k - 1,) + to]
                    self.arrive(slot, self.send.at[at], self.recv.at[at], {"f": source_of("f", k)})
                    parts.append(slot)
                sum_into(self.part.at[to], parts)
                if any(tag):
                    self.push(
                        self.part.at[to], self.out.at[t, c], self.send_on.at[tag], self.recv_on.at[tag],
                        {"t": to[0], "col": to[1]},
                    )
                else:
                    self.keep(self.part.at[to], self.out.at[t, c], self.own)
        if wave == 2:
            for tag in grid_of(("t", "col")):
                if any(tag):
                    peer = source_of("t", tag[0]), source_of("col", tag[1])
                    self.arrive(
                        self.out.at[peer], self.send_on.at[tag], self.recv_on.at[tag], {"t": peer[0], "col": peer[1]}
                    )


def run_jobs(jobs, order):
    done = [-1] * len(jobs)
    for i in tuple(order) + tuple(range(len(jobs))) * 7:
        done[i] += 1
        if done[i]:
            jobs[i].stage(done[i])
        else:
            jobs[i].begin()
    for job in jobs:
        job.drain()


def exchange(cid, peers, plan, operands, out_shapes, out_spaces, order=(), through=None):
    n_in, n_out = len(operands), len(out_shapes)
    in_specs, aliases = [VMEM] * n_in, {}
    if through is not None:
        aliases[n_in] = n_out
        operands, in_specs = list(operands) + [through], in_specs + [ANY]
        out_shapes, out_spaces = list(out_shapes) + [like(through.shape, through.dtype)], list(out_spaces) + [ANY]
    scratch = [s for job in plan for s in job[4]]

    def kernel(*refs):
        n_op, n_res = len(in_specs), len(out_shapes)
        ins, outs, rest = refs[:n_in], refs[n_op : n_op + n_out], refs[n_op + n_res :]
        greet(peers())
        jobs = []
        for make, src, out, options, own in plan:
            mine, rest = rest[: len(own)], rest[len(own) :]
            jobs.append(make(ins[src], outs[out], *options[0], mine, **options[1]))
        run_jobs(jobs, order)

    return pl.pallas_call(
        kernel,
        out_shape=tuple(out_shapes),
        in_specs=in_specs,
        out_specs=tuple(out_spaces),
        scratch_shapes=scratch,
        input_output_aliases=aliases,
        compiler_params=pltpu.CompilerParams(collective_id=cid, has_side_effects=True),
    )(*operands)


class Swap(Copies):
    def __init__(self, src, out, sems):
        super().__init__()
        self.src, self.out = src, out
        self.send, self.recv = sems

    @staticmethod
    def scratch():
        return [pltpu.SemaphoreType.DMA, pltpu.SemaphoreType.DMA]

    def begin(self):
        other = 1 - lax.axis_index("col")
        self.push(self.src.at[other], self.out, self.send, self.recv, {"col": other})

    def stage(self, wave):
        if wave == 1:
            self.arrive(self.out, self.send, self.recv, {"col": 1 - lax.axis_index("col")})


class AllReduce(Copies):
    def __init__(self, src, out, axes, scratch):
        super().__init__()
        n = Reduce.count(axes)
        self.depth = len(axes)
        self.reduce = Reduce(src, scratch[n], axes, scratch[:n])
        self.gather = Spread(scratch[n], out, axes, scratch[n + 1 :])

    @staticmethod
    def scratch(axes, block, dtype):
        return Reduce.scratch(axes, block, dtype) + [pltpu.VMEM(block, dtype)] + Spread.scratch(axes)

    def begin(self):
        self.reduce.begin()

    def stage(self, wave):
        if wave <= self.depth:
            self.reduce.stage(wave)
        if wave == self.depth:
            self.gather.begin()
        if wave > self.depth:
            self.gather.stage(wave - self.depth)

    def drain(self):
        self.reduce.drain()
        self.gather.drain()


def shape_of(axes):
    return tuple(lax.axis_size(a) for a in axes)


def lanes_of(width):
    def place(ref, coords):
        return ref.at[tuple(coords[:-1]) + (slice(None), pl.ds(pl.multiple_of(coords[-1] * width, width), width))]

    return place


def col_first(ref, coords):
    return ref.at[(coords[-1],) + tuple(coords[:-1])]


def like(shape, dtype):
    return jax.ShapeDtypeStruct(shape, dtype)


def pair_sum(values, cid, through=None):
    share = 128 // len(values)
    wide = jnp.concatenate([jnp.broadcast_to(v, (v.shape[0], share)) for v in values], axis=1)
    both, *passed = exchange(
        cid, lambda: along("col"),
        [(Gather, 0, 0, ((PAIR,), {}), Gather.scratch(PAIR))],
        [wide], [like((2,) + wide.shape, F32)], [VMEM], through=through,
    )
    total = both[0] + both[1]
    return [total[:, i * share : i * share + 1] for i in range(len(values))] + passed


def recurrence(retain, source, lead, backward, cid):
    rows, width = retain.shape
    tiles = rows // 8
    sizes = shape_of(ORDER)
    count = sizes[0] * sizes[1] * sizes[2]
    lines = width // 128
    block = (-(-2 * lines // 8) * 8, 128)

    def kernel(r_ref, s_ref, lead_ref, h_ref, in_ref, c_ref, mine, ends, send, recv, own):
        peers = across(*ORDER)
        hail(peers)
        row = lax.broadcasted_iota(jnp.int32, (8, width), 0)

        def tile(i):
            return pl.ds(pl.multiple_of(8 * (tiles - 1 - i if backward else i), 8), 8)

        def step(i, carry):
            decay, state = carry
            at = tile(i)
            r, s = r_ref[at, :], s_ref[at, :]
            for by in (1, 2, 4):
                keep = row < 8 - by if backward else row >= by
                shift = 8 - by if backward else by
                r_by = jnp.where(keep, pltpu.roll(r, shift, 0), 1.0)
                s_by = jnp.where(keep, pltpu.roll(s, shift, 0), 0.0)
                s = r * s_by + s
                r = r * r_by
            s = s + r * state
            r = r * decay
            c_ref[at, :] = r
            h_ref[at, :] = s
            end = 0 if backward else 7
            return r[end : end + 1, :], s[end : end + 1, :]

        one = jnp.ones((1, width), F32)
        decay, state = lax.fori_loop(0, tiles, step, (one, jnp.zeros((1, width), F32)))
        decay, state = lead_ref[0:1, :] * decay, lead_ref[0:1, :] * state
        for j in range(lines):
            mine[j : j + 1, :] = decay[:, 128 * j : 128 * (j + 1)]
            mine[lines + j : lines + j + 1, :] = state[:, 128 * j : 128 * (j + 1)]
        pl.semaphore_wait(pltpu.get_barrier_semaphore(), len(peers))
        jobs = Copies()
        here = tuple(lax.axis_index(a) for a in ORDER)
        for tag in grid_of(ORDER):
            if any(tag):
                peer = {a: peer_of(a, k) for a, k in zip(ORDER, tag)}
                jobs.push(mine, ends.at[here], send.at[tag], recv.at[tag], peer)
        jobs.keep(mine, ends.at[here], own)
        for tag in grid_of(ORDER):
            if any(tag):
                peer = {a: source_of(a, k) for a, k in zip(ORDER, tag)}
                jobs.arrive(ends.at[tuple(peer[a] for a in ORDER)], send.at[tag], recv.at[tag], peer)
        jobs.drain()
        me = (here[0] * sizes[1] + here[1]) * sizes[2] + here[2]
        entering = jnp.zeros((lines, 128), F32)
        for i in range(count):
            peer = count - 1 - i if backward else i
            t, rest = divmod(peer, sizes[1] * sizes[2])
            f, c = divmod(rest, sizes[2])
            pair = ends[t, f, c]
            ahead = jnp.where(peer > me if backward else peer < me, 1, 0)
            entering = jnp.where(ahead == 1, pair[:lines] * entering + pair[lines : 2 * lines], entering)
        entering = jnp.concatenate([entering[j : j + 1, :] for j in range(lines)], axis=1)
        in_ref[...] = jnp.broadcast_to(entering, (8, width))

        def fix(i, carry):
            at = tile(i)
            h_ref[at, :] = h_ref[at, :] + c_ref[at, :] * entering
            return carry

        lax.fori_loop(0, tiles, fix, 0)

    states, entering = pl.pallas_call(
        kernel,
        out_shape=(like((rows, width), F32), like((8, width), F32)),
        in_specs=[VMEM] * 3,
        out_specs=(VMEM, VMEM),
        scratch_shapes=[
            pltpu.VMEM((rows, width), F32),
            pltpu.VMEM(block, F32),
            pltpu.VMEM(sizes + block, F32),
            pltpu.SemaphoreType.DMA(sizes),
            pltpu.SemaphoreType.DMA(sizes),
            pltpu.SemaphoreType.DMA,
        ],
        compiler_params=pltpu.CompilerParams(collective_id=cid, has_side_effects=True),
        name="back_states" if backward else "states",
    )(retain, source, jnp.broadcast_to(lead, (8, width)))
    return states, entering[0]


def from_behind(x, axis, by):
    peers = lax.axis_size(axis)
    pairs = [(i, i + by) for i in range(peers) if 0 <= i + by < peers]
    return lax.ppermute(x, axis, pairs)


def gelu_tanh(values):
    return jax.nn.gelu(values, approximate=True)


def gates_of(decay_pre, input_pre, decay_param, conv_low, starts):
    rate_gate = jax.nn.sigmoid(decay_pre)
    in_gate = jax.nn.sigmoid(input_pre)
    log_decay = -8.0 * jax.nn.softplus(decay_param) * rate_gate
    retain = jnp.where(starts, 0.0, jnp.exp(log_decay))
    multiplier = jnp.where(
        starts, 1.0, jnp.sqrt(jnp.maximum(-jnp.expm1(2.0 * log_decay), SQRT_FLOOR))
    )
    return (retain, multiplier * in_gate * conv_low)


def normalize_back(gradient, values, inverse, scale_vec, cid, through=None):
    weighted = gradient * (1.0 + scale_vec)
    scale_grad = jnp.sum(gradient * values * inverse, axis=0)
    inner_sum, *passed = pair_sum([jnp.sum(weighted * values, axis=1, keepdims=True)], cid, through)
    return (inverse * weighted - values * inverse**3 * inner_sum / D, scale_grad, *passed)


def arrange(own, other):
    first = lax.axis_index("col") == 0
    return jnp.where(first, own, other), jnp.where(first, other, own)


def halves(x):
    width = x.shape[1] // 2
    return jnp.stack([x[:, :width], x[:, width:]])


def half_of(x):
    width = x.shape[1] // 2
    return jnp.where(lax.axis_index("col") == 0, x[:, :width], x[:, width:])


TOKEN_AXES = ("t", "row", "col")
WEIGHT_AXES = ("t", "f", "col")
PAIR = ("col",)


def fetch_first(mixer, branch, output, stream, scale, down):
    t, f, c = shape_of(WEIGHT_AXES)
    width, inner = mixer.shape
    piece = (down.shape[0], down.shape[1] // (2 * TEAM))
    place = lanes_of(inner)
    axes = (WEIGHT_AXES,)
    plan = [
        (Gather, 0, 0, (axes, {"place": place}), Gather.scratch(WEIGHT_AXES)),
        (Fan, 3, 3, (("row",), {}), Fan.scratch("row")),
        (Gather, 1, 1, (axes, {"place": place}), Gather.scratch(WEIGHT_AXES)),
        (Gather, 2, 2, (axes, {"place": col_first}), Gather.scratch(WEIGHT_AXES)),
        (Gather, 4, 4, ((PAIR,), {}), Gather.scratch(PAIR)),
        (Trade, 5, 5, ((), {}), Trade.scratch(piece, BF16)),
    ]
    wide = like((t, f, width, 2 * inner), BF16)
    outs = [wide, wide, like((c, t, f) + output.shape, BF16), like((1, stream.shape[0], 2 * stream.shape[1]), BF16)]
    outs += [like((2, 1, scale.shape[0]), F32), like((2, TEAM) + piece, BF16)]
    mixer_t, branch_t, output_t, tokens, scale, down = exchange(
        0, lambda: along("t", "f") + across("row", "col") + diagonal("t", "col"), plan,
        [mixer, branch, output, stream, scale[None], down], outs, [ANY] * 4 + [VMEM, ANY],
        order=(0, 1, 2, 3, 4, 0, 5, 2, 3),
    )
    return mixer_t.reshape(-1, 2 * inner), branch_t.reshape(-1, 2 * inner), output_t.reshape(-1, output.shape[1]), tokens[0], scale.reshape(-1), down


def fetch_second(normed, cotangent, gate, up, down):
    t, r, _ = shape_of(TOKEN_AXES)
    fleet = lax.axis_size("f")
    rows, width = normed.shape
    units, inner = gate.shape
    share = down.shape[-1]
    half = fleet // 2
    token, fan = Gather.scratch(TOKEN_AXES), Fan.scratch("f")
    place = lanes_of(width)

    def kernel(n_ref, c_ref, g_ref, u_ref, d_ref, n_all, c_all, gw, uw, d_all, g_out, u_out, held, sem, *rest):
        normed_job = Gather(n_ref, n_all, TOKEN_AXES, rest[:3], place)
        cot_job = Gather(c_ref, c_all, TOKEN_AXES, rest[3:6], place)
        gate_job, up_job = Fan(g_ref, gw, "f", rest[6:9]), Fan(u_ref, uw, "f", rest[9:12])
        down_job = Gather(d_ref, d_all, ("f",), rest[12:15], lambda ref, at: ref.at[:, :, at[0]])
        jobs = (normed_job, gate_job, up_job, down_job, cot_job)
        greet(along("t", "row") + across("f", "col"))
        for job in jobs:
            job.begin()
        normed_job.stage(1)
        cot_job.stage(1)
        normed_job.stage(2)
        normed_job.stage(3)
        normed_job.drain()
        for job in (gate_job, up_job):
            job.stage(1)
            job.drain()
        blocks = t * r

        def fetch(i):
            return pltpu.make_async_copy(n_all.at[i // r, i % r], held.at[i % 2], sem.at[i % 2])

        fetch(0).start()

        def product(i, carry):
            @pl.when(i + 1 < blocks)
            def _():
                fetch(i + 1).start()

            fetch(i).wait()
            at = pl.ds(pl.multiple_of(i * rows, rows), rows)
            for weight, out in ((gw, g_out), (uw, u_out)):
                for j in range(half):
                    out[at, j * units : (j + 1) * units] = dot_nt(held[i % 2], weight[j])
            return carry

        lax.fori_loop(0, blocks, product, 0)
        cot_job.stage(2)
        down_job.stage(1)
        cot_job.stage(3)
        for job in (down_job, cot_job):
            job.drain()

    every = like((t, r, rows, 2 * width), BF16)
    weight = like((half, units, 2 * inner), BF16)
    first = like((t * r * rows, share), F32)
    n_all, c_all, gate_t, up_t, down_t, gate_out, up_out = pl.pallas_call(
        kernel,
        out_shape=(every, every, weight, weight, like(down.shape[:2] + (fleet,) + down.shape[2:], BF16), first, first),
        in_specs=[VMEM] * 5,
        out_specs=(ANY, ANY, VMEM, VMEM, ANY, VMEM, VMEM),
        scratch_shapes=[pltpu.VMEM((2, rows, 2 * width), BF16), pltpu.SemaphoreType.DMA((2,))]
        + token + token + fan + fan + Gather.scratch(("f",)),
        compiler_params=pltpu.CompilerParams(collective_id=1, has_side_effects=True),
        name="fetch_second",
    )(normed, cotangent, gate, up, down)
    return (
        n_all.reshape(-1, 2 * width),
        c_all.reshape(-1, 2 * width),
        gate_t.reshape(-1, 2 * inner),
        up_t.reshape(-1, 2 * inner),
        down_t.reshape(-1, share),
        gate_out,
        up_out,
    )


def diagonal(*axes):
    pairs = zip(across(*axes), [tag for tag in grid_of(axes) if any(tag)])
    return [peer for peer, tag in pairs if all(tag)]


def team_peers():
    return along("t", "row") + across("f", "col") + diagonal("t", "col")


def send_second(gate, up, hidden, gate_t, up_t, second_all, cot_all, late):
    t, r, _ = shape_of(TOKEN_AXES)
    fleet = lax.axis_size("f")
    tokens, wide = second_all.shape
    share = gate.shape[1]
    rows, width = tokens // (t * r), wide // 2
    half = fleet // 2
    units = share // half
    shard = width // (TEAM * fleet)
    block, weight, piece = (rows, width), (units, width), (shard, share)
    lane, tile = 512, wide // 4
    part, chunk = tile // shard, 256
    place = lanes_of(width)
    settle, fold = Settle.scratch(TOKEN_AXES, block, BF16), Fold.scratch("f", weight, BF16)
    undeal = Undeal.scratch(piece, BF16)

    def kernel(*refs):
        g_ref, u_ref, h_ref, gw_ref, uw_ref, all_ref, cot_ref, _ = refs[:8]
        delta_ref, grad_g, grad_u, grad_d = refs[8:12]
        src, fold_g, fold_u, down, gt_ref, ut_ref, ht_ref, tiles, tile_sem = refs[12:21]
        rest = refs[21:]
        sums = Settle(src, delta_ref, TOKEN_AXES, rest[: len(settle)], place)
        rest = rest[len(settle) :]
        g_job = Fold(fold_g, grad_g, "f", rest[: len(fold)])
        u_job = Fold(fold_u, grad_u, "f", rest[len(fold) : 2 * len(fold)])
        d_job = Undeal(down, grad_d, rest[2 * len(fold) :])

        def fetch(ref, i):
            at = pl.ds(pl.multiple_of(i * tile, tile), tile)
            return pltpu.make_async_copy(ref.at[:, at], tiles.at[i % 2], tile_sem.at[i % 2])

        def turn(src_ref, out_ref):
            def some(i, carry):
                at = pl.ds(pl.multiple_of(i * chunk, chunk), chunk)
                out_ref[:, at] = src_ref[at, :].T
                return carry

            lax.fori_loop(0, tokens // chunk, some, 0)

        def down_gradients(i, carry):
            @pl.when(i + 1 < wide // tile)
            def _():
                fetch(cot_ref, i + 1).start()

            @pl.when(i + 1 == wide // tile)
            def _():
                fetch(all_ref, 0).start()

            fetch(cot_ref, i).wait()
            value = dot_nn(ht_ref[...], tiles[i % 2]).T.astype(BF16)
            for j in range(part):
                n = i * part + j
                down[n % fleet, n // fleet % TEAM, n // (TEAM * fleet)] = value[j * shard : (j + 1) * shard]
            return carry

        fetch(cot_ref, 0).start()
        turn(h_ref, ht_ref)
        greet(team_peers())
        lax.fori_loop(0, wide // tile, down_gradients, 0)
        d_job.begin()
        before = None
        for tag in sums.order(2):
            coords = sums.coords(tag)
            at = pl.ds(pl.multiple_of((coords[0] * r + coords[1]) * rows, rows), rows)

            def product(j, carry, at=at, coords=coords):
                col = pl.ds(pl.multiple_of(j * lane, lane), lane)
                value = dot_nn(g_ref[at, :], gw_ref[:, col]) + dot_nn(u_ref[at, :], uw_ref[:, col])
                src[coords[0], coords[1], :, col] = value.astype(BF16)
                return carry

            lax.fori_loop(0, wide // lane, product, 0)
            for k in offsets("col"):
                sums.forward(tag + (k,), place(src, sums.coords(tag + (k,))))
            if before is not None:
                sums.step(2, before)
            before = tag
        sums.step(2, before)
        middle = sums.order(1)
        sums.step(1, middle[0])
        d_job.stage(1)

        def gradients(i, carry):
            @pl.when(i + 1 < wide // tile)
            def _():
                fetch(all_ref, i + 1).start()

            fetch(all_ref, i).wait()
            h, at = i // (width // tile), pl.ds(pl.multiple_of(i % (width // tile) * tile, tile), tile)
            for left, out in ((gt_ref, fold_g), (ut_ref, fold_u)):
                value = dot_nn(left[...], tiles[i % 2]).astype(BF16)
                for j in range(half):
                    out[h, j, :, at] = value[j * units : (j + 1) * units]
            return carry

        turn(g_ref, gt_ref)
        turn(u_ref, ut_ref)
        for h in (0, 1):
            first = h * (width // tile)
            lax.fori_loop(first, first + width // tile, gradients, 0)
            g_job.begin((h,))
            u_job.begin((h,))
            sums.step(1, middle[1 + h])
        for tag in middle[3:]:
            sums.step(1, tag)
        sums.stage(3)
        g_job.stage(1)
        u_job.stage(1)
        d_job.stage(2)
        for job in (sums, g_job, u_job, d_job):
            job.drain()

    delta, grad_gate, grad_up, grad_down = pl.pallas_call(
        kernel,
        out_shape=(like(block, F32), like(weight, BF16), like(weight, BF16), like((TEAM, 2) + piece, BF16)),
        in_specs=[VMEM] * 5 + [ANY] * 3,
        out_specs=(VMEM,) * 4,
        scratch_shapes=[
            pltpu.VMEM((t, r, rows, wide), BF16),
            pltpu.VMEM((2, half) + weight, BF16),
            pltpu.VMEM((2, half) + weight, BF16),
            pltpu.VMEM((fleet, TEAM, 2) + piece, BF16),
            pltpu.VMEM((share, tokens), BF16),
            pltpu.VMEM((share, tokens), BF16),
            pltpu.VMEM((share, tokens), BF16),
            pltpu.VMEM((2, tokens, tile), BF16),
            pltpu.SemaphoreType.DMA((2,)),
        ]
        + settle + fold + fold + undeal,
        compiler_params=pltpu.CompilerParams(
            collective_id=2, has_side_effects=True, vmem_limit_bytes=67_000_000
        ),
        name="send_second",
    )(gate, up, hidden, gate_t, up_t, second_all, cot_all, late)
    grad_down = grad_down.reshape(2 * TEAM, shard, share).transpose(0, 2, 1).reshape(-1, shard)
    return delta, grad_gate, grad_up, grad_down


def to_stream(partial, cid):
    rows, width = partial.shape
    block = (rows, width // 2)
    (out,) = exchange(
        cid, lambda: across("row", "col"),
        [(Fold, 0, 0, (("row",), {}), Fold.scratch("row", block, BF16))],
        [halves(partial).reshape((2, 1) + block)], [like(block, F32)], [VMEM],
    )
    return out


def to_tokens(block, mixed, through, cid):
    rows, width = block.shape
    out, both, through = exchange(
        cid, lambda: across("row", "col"),
        [
            (Fan, 0, 0, (("row",), {}), Fan.scratch("row")),
            (Gather, 1, 1, ((PAIR,), {}), Gather.scratch(PAIR)),
        ],
        [block, mixed], [like((1, rows, 2 * width), BF16), like((2,) + mixed.shape, BF16)], [VMEM] * 2,
        through=through,
    )
    return out[0], both.reshape(-1, mixed.shape[1]), through


def core_rows(x, cid):
    (other,) = exchange(
        cid, lambda: along("col"), [(Swap, 0, 0, ((), {}), Swap.scratch())], [halves(x)],
        [like((x.shape[0], x.shape[1] // 2), x.dtype)], [VMEM],
    )
    return jnp.concatenate(arrange(half_of(x), other), axis=0)


def dealt(x, axes, dtype):
    sizes = shape_of(axes)
    members = sizes[0] * sizes[1] * sizes[2]
    width = -(-x.size // (members * 8 * 128)) * 128
    flat = jnp.pad(x.reshape(-1), (0, members * 8 * width - x.size))
    return flat.reshape(sizes + (8, width)).astype(dtype)


STREAM_AXES = ("t", "f", "row")


def finish_block(normed, branch, mixer, delta, cid):
    rows, width = delta.shape
    token = (rows, width // 2)
    plan = [
        (Fold, 0, 0, (("row",), {}), Fold.scratch("row", token, BF16)),
        (Swap, 1, 1, ((), {}), Swap.scratch()),
        (Gather, 2, 2, ((PAIR,), {}), Gather.scratch(PAIR)),
        (Gather, 3, 3, ((PAIR,), {}), Gather.scratch(PAIR)),
    ]
    outs = [like(token, F32), like(token, BF16), like((2,) + branch.shape, BF16), like((2,) + mixer.shape, BF16)]
    delta, other, branch, mixer = exchange(
        cid, lambda: across("row", "col"), plan,
        [halves(delta).reshape((2, 1) + token), halves(normed), branch, mixer], outs, [VMEM] * 4,
    )
    rows = jnp.concatenate(arrange(half_of(normed), other), axis=0)
    return delta, rows, branch.reshape(-1, branch.shape[2]), mixer.reshape(-1, mixer.shape[2])


def send_first(grads, inner_sums, head_grads, stream_sums, through, cid):
    sizes = shape_of(DP)
    n = len(grads)
    block = (grads[0].shape[0] // (sizes[0] * sizes[1]), grads[0].shape[1])
    axes_of = (ORDER, STREAM_AXES, ORDER)
    sums = (inner_sums, stream_sums, head_grads)
    lanes = head_grads.shape[-1]
    small = [dealt(x, axes, F32) for x, axes in zip(sums[:2], axes_of)]
    small.append(head_grads.reshape(shape_of(ORDER) + (-1, lanes)).astype(BF16))
    plan = [
        (AllReduce, n + i, n + i, ((axes,), {}), AllReduce.scratch(axes, x.shape[3:], x.dtype))
        for i, (x, axes) in enumerate(zip(small, axes_of))
    ]
    plan += [(Reduce, i, i, ((DP,), {}), Reduce.scratch(DP, block, BF16)) for i in range(n)]
    bulk = tuple(range(3, 3 + n))
    got = exchange(
        cid, lambda: along("t", "f", "row", "col"), plan,
        [g.reshape(sizes + block) for g in grads] + small,
        [like(block, F32)] * n + [like(x.shape, x.dtype) for x in small], [VMEM] * (n + 3),
        order=(0, 1, 2) * 3 + bulk + (0, 1, 2) + bulk * 2, through=through,
    )
    return got[:n], [x.reshape(-1)[: y.size].reshape(y.shape).astype(F32) for x, y in zip(got[n:-1], sums)], got[-1]


def on_device(
    stream,
    scale_first,
    branch_weight,
    branch_bias,
    mixer_weight,
    mixer_bias,
    conv_weight,
    conv_bias,
    decay_weight,
    decay_bias,
    input_weight,
    input_bias,
    decay_param,
    output_weight,
    output_bias,
    scale_second,
    gate_weight,
    gate_bias,
    up_weight,
    up_bias,
    down_weight,
    down_bias,
    cotangent,
):
    mixer_t, branch_t, output_t, stream_all, scale_all, down_pieces = fetch_first(
        mixer_weight.T, branch_weight.T, output_weight.T, stream, scale_first, down_weight.T
    )
    inner = mixer_t.shape[0]
    stream_wide = stream.astype(F32)
    tokens_wide = stream_all.astype(F32)
    inverse_all = lax.rsqrt(jnp.sum(tokens_wide * tokens_wide, axis=1, keepdims=True) / D + EPSILON)
    normed_first = (tokens_wide * inverse_all * (1.0 + scale_all)).astype(BF16)
    mixer_pre = dot_nt(normed_first, mixer_t) + mixer_bias
    branch_pre = dot_nt(normed_first, branch_t) + branch_bias
    branch_act, branch_back = jax.vjp(gelu_tanh, branch_pre)

    steps = mixer_pre.shape[0]
    first_token = lax.axis_index(ORDER) * steps
    position = (first_token + jnp.arange(steps, dtype=jnp.int32)) % LEN
    margin = CONV - 1
    left_edge = from_behind(mixer_pre[steps - margin :], ORDER, 1)
    padded = jnp.concatenate([left_edge, mixer_pre], axis=0)
    conv_out = conv_bias + jnp.zeros_like(mixer_pre)
    for offset in range(CONV):
        in_reach = (position >= offset)[:, None]
        conv_out = conv_out + jnp.where(
            in_reach, conv_weight[offset] * padded[margin - offset : margin - offset + steps], 0.0
        )
    conv_low = conv_out.astype(BF16)
    conv_wide = conv_low.astype(F32)
    heads, block = decay_weight.shape[0], decay_weight.shape[1]
    parts = [conv_low[:, h * block : (h + 1) * block] for h in range(heads)]
    decay_pre = jnp.concatenate([dot_nn(x, decay_weight[h]) for h, x in enumerate(parts)], 1) + decay_bias
    input_pre = jnp.concatenate([dot_nn(x, input_weight[h]) for h, x in enumerate(parts)], 1) + input_bias
    starts = (position == 0)[:, None]

    def gate_values(decay_in, input_in, param_in, conv_in):
        return gates_of(decay_in, input_in, param_in, conv_in, starts)

    (retain, source), gate_back = jax.vjp(gate_values, decay_pre, input_pre, decay_param, conv_wide)
    ones_row = jnp.ones((1, inner), F32)
    states, state_in = recurrence(retain, source, ones_row, False, 3)
    mixed_low = (states * branch_act).astype(BF16)
    first_out = stream_wide + to_stream(dot_nt(mixed_low, output_t).astype(BF16), 4) + output_bias
    second_total, first_total = pair_sum(
        [jnp.sum(x * x, axis=1, keepdims=True) for x in (first_out, stream_wide)], 5
    )
    inverse_second = lax.rsqrt(second_total / D + EPSILON)
    inverse_first = lax.rsqrt(first_total / D + EPSILON)
    normed_second = first_out * inverse_second * (1.0 + scale_second)

    share = down_weight.shape[0] // (2 * TEAM)
    second_all, cot_all, gate_t, up_t, down_t, gate_pre, up_pre = fetch_second(
        normed_second.astype(BF16), cotangent, gate_weight.T, up_weight.T, down_pieces
    )
    mine = (lax.axis_index("t") * 2 + lax.axis_index("col")) * share
    gate_b = lax.dynamic_slice(gate_bias, (mine,), (share,))
    up_b = lax.dynamic_slice(up_bias, (mine,), (share,))

    gate_pre = gate_pre + gate_b
    up_pre = up_pre + up_b
    hidden, hidden_back = jax.vjp(lambda g, u: gelu_tanh(g) * u, gate_pre, up_pre)
    hidden_low = hidden.astype(BF16)
    delta_hidden = dot_nn(cot_all, down_t)
    delta_gate, delta_up = hidden_back(delta_hidden)
    gate_low, up_low = delta_gate.astype(BF16), delta_up.astype(BF16)
    down_part = dot_nt(hidden_low, down_t).astype(BF16)
    down_rows = lax.psum_scatter(down_part, "col", scatter_dimension=1, tiled=True)
    delta_second, grad_gate, grad_up, grad_down = send_second(
        gate_low, up_low, hidden_low, gate_t, up_t, second_all, cot_all, down_part
    )
    delta_result = cotangent.astype(F32)

    norm_second_part, grad_scale_second = normalize_back(
        delta_second, first_out, inverse_second, scale_second, 6
    )
    delta_first = delta_result + norm_second_part
    out_all, mixed_rows, down_rows = to_tokens(delta_first.astype(BF16), mixed_low, down_rows, 7)
    down_proj = lax.psum_scatter(down_rows, ("t", "row"), scatter_dimension=0, tiled=True)
    output_part = dot_tn(core_rows(out_all, 9), mixed_rows).astype(BF16)
    grad_output = lax.psum_scatter(output_part, DP, scatter_dimension=0, tiled=True)
    delta_mixed = dot_nn(out_all, output_t)
    delta_state = delta_mixed * branch_act
    (delta_branch,) = branch_back(delta_mixed * states)
    branch_low = delta_branch.astype(BF16)
    retain_next = jnp.concatenate([retain[1:], ones_row], axis=0)
    back_state, _ = recurrence(retain_next, delta_state, retain[:1], True, 8)
    state_prev = jnp.concatenate([state_in[None], states[:-1]], axis=0)
    delta_decay_pre, delta_input_pre, grad_decay_param, delta_conv = gate_back(
        (back_state * state_prev, back_state)
    )
    decay_low = delta_decay_pre.astype(BF16)
    input_low = delta_input_pre.astype(BF16)

    def split(x):
        return [x[:, h * block : (h + 1) * block] for h in range(heads)]

    grad_decay_weight = jnp.stack([dot_tn(a, b) for a, b in zip(parts, split(decay_low))])
    grad_input_weight = jnp.stack([dot_tn(a, b) for a, b in zip(parts, split(input_low))])
    delta_conv = delta_conv + jnp.concatenate(
        [dot_nt(a, decay_weight[h]) for h, a in enumerate(split(decay_low))], 1
    )
    delta_conv = delta_conv + jnp.concatenate(
        [dot_nt(a, input_weight[h]) for h, a in enumerate(split(input_low))], 1
    )
    delta_padded = jnp.zeros_like(padded)
    conv_grads = []
    for offset in range(CONV):
        in_reach = (position >= offset)[:, None]
        masked = jnp.where(in_reach, delta_conv, 0.0)
        conv_grads.append(
            jnp.sum(masked * padded[margin - offset : margin - offset + steps], axis=0)
        )
        delta_padded = delta_padded + jnp.pad(
            masked * conv_weight[offset], ((margin - offset, offset), (0, 0))
        )
    grad_conv_weight = jnp.stack(conv_grads, axis=0)
    right_edge = from_behind(delta_padded[:margin], ORDER, -1)
    delta_mixer = delta_padded[margin:] + jnp.pad(right_edge, ((steps - margin, 0), (0, 0)))
    mixer_low = delta_mixer.astype(BF16)

    def spread(x):
        return lax.dynamic_update_slice(jnp.zeros_like(gate_bias), x, (mine,))

    small = [
        jnp.sum(delta_branch, axis=0),
        jnp.sum(delta_mixer, axis=0),
        jnp.sum(delta_conv, axis=0),
        jnp.sum(delta_decay_pre, axis=0),
        jnp.sum(delta_input_pre, axis=0),
        grad_decay_param,
        spread(jnp.sum(delta_gate, axis=0)),
        spread(jnp.sum(delta_up, axis=0)),
        grad_conv_weight.reshape(-1),
    ]
    delta_normed_part = dot_nn(branch_low, branch_t) + dot_nn(mixer_low, mixer_t)
    delta_normed_first, first_rows, branch_rows, mixer_rows = finish_block(
        normed_first, branch_low, mixer_low, delta_normed_part.astype(BF16), 10
    )
    norm_first_part, grad_scale_first = normalize_back(
        delta_normed_first, stream_wide, inverse_first, scale_first, 12
    )
    (grad_mixer, grad_branch), (total, stream_sums, head_grads), down_proj = send_first(
        [dot_tn(mixer_rows, first_rows).astype(BF16), dot_tn(branch_rows, first_rows).astype(BF16)],
        jnp.concatenate(small),
        jnp.stack([grad_decay_weight, grad_input_weight]),
        jnp.stack(
            [grad_scale_second, jnp.sum(delta_first, axis=0), jnp.sum(delta_result, axis=0), grad_scale_first]
        ),
        down_proj,
        13,
    )
    result = (first_out + down_proj.astype(F32) + down_bias).astype(BF16)
    grad_stream = delta_first + norm_first_part
    sums, at = [], 0
    for x in small:
        sums.append(total[at : at + x.shape[0]])
        at += x.shape[0]
    return (
        result,
        grad_stream,
        stream_sums[3],
        grad_branch.T,
        sums[0],
        grad_mixer.T,
        sums[1],
        sums[8].reshape(CONV, inner),
        sums[2],
        head_grads[0],
        sums[3],
        head_grads[1],
        sums[4],
        sums[5],
        grad_output.T.astype(F32),
        stream_sums[1],
        stream_sums[0],
        grad_gate.T.astype(F32),
        sums[6],
        grad_up.T.astype(F32),
        sums[7],
        grad_down.astype(F32),
        stream_sums[2],
    )


def solution(mesh):
    shape = mesh.devices.shape
    names = mesh.axis_names
    fleet = mesh.shape["dp"] // TEAM
    at = names.index("dp")
    split_mesh = Mesh(
        mesh.devices.reshape(shape[:at] + (TEAM, fleet) + shape[at + 1 :]),
        names[:at] + DP + names[at + 1 :],
    )
    tokens, fan_in = P((*DP, "row"), "col"), P("col", ("row", *DP))
    fan_out, inner, wide = P("row", ("col", *DP)), P("row"), P("col")
    heads = P("row", None, None)
    return jax.shard_map(
        on_device,
        mesh=split_mesh,
        in_specs=(
            tokens, wide, fan_in, inner, fan_in, inner, P(None, "row"), inner,
            heads, inner, heads, inner, inner, fan_out, wide, wide,
            fan_in, inner, fan_in, inner, fan_out, wide, tokens,
        ),
        out_specs=(
            tokens, tokens, wide, fan_in, inner, fan_in, inner, P(None, "row"), inner,
            heads, inner, heads, inner, inner, fan_out, wide, wide,
            fan_in, inner, fan_in, inner, fan_out, wide,
        ),
        check_vma=False,
    )
```

```python
import jax
import jax.numpy as jnp
from jax import lax
from jax.experimental import pallas as pl
from jax.experimental.pallas import tpu as pltpu
from jax.sharding import Mesh, PartitionSpec as P


D = 2560
CONV = 4
LEN = 4096
EPSILON = 1e-06
SQRT_FLOOR = 0.0001
TEAM = 4
NT = (((1,), (1,)), ((), ()))
TN = (((0,), (0,)), ((), ()))
F32 = jnp.float32
BF16 = jnp.bfloat16
DP = ("t", "f")
ORDER = ("t", "f", "col")


def dot_nn(a, b):
    return jnp.dot(a, b, preferred_element_type=F32)


def dot_nt(a, b):
    return lax.dot_general(a, b, NT, preferred_element_type=F32)


def dot_tn(a, b):
    return lax.dot_general(a, b, TN, preferred_element_type=F32)


MESH = pl.DeviceIdType.MESH
ANY = pl.BlockSpec(memory_space=pl.ANY)
VMEM = pl.BlockSpec(memory_space=pltpu.VMEM)


def peer_of(axis, k):
    n, me = lax.axis_size(axis), lax.axis_index(axis)
    if k == 0:
        return me
    if n == 2:
        return 1 - me
    if n == 4:
        return (me + 1 - 2 * (me % 2), (me + 2) % 4, 3 - me)[k - 1]
    return (me + k) % n


def source_of(axis, k):
    n, me = lax.axis_size(axis), lax.axis_index(axis)
    return peer_of(axis, k) if n in (2, 4) else (me + n - k) % n


def offsets(axis):
    n = lax.axis_size(axis)
    return (1, 3, 2) if n == 4 else tuple(range(1, n))


def grid_of(axes, far_first=False):
    grid = [()]
    for axis in axes:
        near = (0,) + offsets(axis)
        grid = [tag + (k,) for tag in grid for k in (near[::-1] if far_first else near)]
    return grid


def hail(peers):
    for peer in peers:
        pl.semaphore_signal(pltpu.get_barrier_semaphore(), inc=1, device_id=peer, device_id_type=MESH)


def greet(peers):
    hail(peers)
    pl.semaphore_wait(pltpu.get_barrier_semaphore(), len(peers))


def only(condition, act):
    if condition is None:
        act()
    else:
        pl.when(condition)(act)


def along(*axes):
    return [{axis: peer_of(axis, k)} for axis in axes for k in offsets(axis)]


def across(*axes):
    return [
        {axis: peer_of(axis, k) for axis, k in zip(axes, tag)} for tag in grid_of(axes) if any(tag)
    ]


class Copies:
    def __init__(self):
        self.sent = []

    def push(self, src, dst, send, recv, peer, condition=None):
        copy = pltpu.make_async_remote_copy(
            src_ref=src, dst_ref=dst, send_sem=send, recv_sem=recv, device_id=peer, device_id_type=MESH
        )
        only(condition, copy.start)
        self.sent.append((condition, copy.wait_send))

    def arrive(self, dst, send, recv, peer):
        pltpu.make_async_remote_copy(
            src_ref=dst, dst_ref=dst, send_sem=send, recv_sem=recv, device_id=peer, device_id_type=MESH
        ).wait_recv()

    def keep(self, src, dst, sem):
        copy = pltpu.make_async_copy(src, dst, sem)
        copy.start()
        self.sent.append((None, copy.wait))

    def drain(self):
        for condition, wait in self.sent:
            only(condition, wait)


def leading(ref, coords):
    return ref.at[tuple(coords)]


class Gather(Copies):
    def __init__(self, src, out, axes, sems, place=leading):
        super().__init__()
        self.src, self.out, self.axes, self.place = src, out, axes, place
        self.send, self.recv, self.own = sems
        self.size, self.at = lax.axis_size(axes[0]), lax.axis_index(axes[0])
        self.nobody = (0,) * len(axes)
        self.waves = {}
        line = [0] + [v for far in range(1, self.size) for v in (-far, far)]
        for v in line:
            for rest in grid_of(axes[1:]):
                tag = (v,) + rest
                if any(tag):
                    self.waves.setdefault(sum(1 for k in tag if k), []).append(tag)

    @staticmethod
    def scratch(axes):
        sizes = [lax.axis_size(a) for a in axes]
        shape = (2 * sizes[0] - 1,) + tuple(sizes[1:])
        return [pltpu.SemaphoreType.DMA(shape), pltpu.SemaphoreType.DMA(shape), pltpu.SemaphoreType.DMA]

    def index(self, tag):
        return (tag[0] + self.size - 1,) + tag[1:]

    def exists(self, far):
        if far == 0:
            return None
        return self.at + far >= 0 if far < 0 else self.at + far < self.size

    def slot(self, tag):
        rest = [source_of(a, k) for a, k in zip(self.axes[1:], tag[1:])]
        return self.place(self.out, [self.at + tag[0]] + rest)

    def spread(self, tag):
        last = max([i for i, k in enumerate(tag) if k], default=-1)
        here = self.exists(tag[0])
        src = self.slot(tag) if any(tag) else self.src

        def send(there, peer, condition):
            if here is not None and condition is not None:
                condition = here & condition
            elif condition is None:
                condition = here
            at = self.index(there)
            self.push(src, self.slot(tag), self.send.at[at], self.recv.at[at], peer, condition)

        if last <= 0:
            if 0 <= tag[0] < self.size - 1:
                send((tag[0] + 1,) + tag[1:], {self.axes[0]: self.at - 1}, self.at > 0)
            if -self.size + 1 < tag[0] <= 0:
                send((tag[0] - 1,) + tag[1:], {self.axes[0]: self.at + 1}, self.at < self.size - 1)
        for level in range(max(last, 0) + 1, len(self.axes)):
            axis = self.axes[level]
            for k in offsets(axis):
                send(tag[:level] + (k,) + tag[level + 1 :], {axis: peer_of(axis, k)}, None)

    def begin(self):
        self.spread(self.nobody)
        self.keep(self.src, self.slot(self.nobody), self.own)

    def stage(self, wave):
        for tag in self.waves.get(wave, ()):
            last = max(i for i, k in enumerate(tag) if k)
            if last:
                peer = {self.axes[last]: peer_of(self.axes[last], tag[last])}
            else:
                peer = {self.axes[0]: self.at + (1 if tag[0] > 0 else -1)}
            at = self.index(tag)
            only(
                self.exists(tag[0]),
                lambda: self.arrive(self.slot(tag), self.send.at[at], self.recv.at[at], peer),
            )
            self.spread(tag)


def sum_into(out, parts):
    rows = out.shape[0]
    step = next(n for n in (32, 16, 8, rows) if rows % n == 0)

    def some(i, carry):
        at = pl.ds(pl.multiple_of(i * step, step), step)
        total = parts[0][at, :].astype(F32)
        for part in parts[1:]:
            total = total + part[at, :].astype(F32)
        out[at, :] = total.astype(out.dtype)
        return carry

    lax.fori_loop(0, rows // step, some, 0)


class Reduce(Copies):
    def __init__(self, src, out, axes, scratch, place=leading):
        super().__init__()
        n = len(axes)
        self.src, self.out, self.axes, self.place = src, out, axes, place
        self.part = {i + 1: scratch[i] for i in range(n - 1)}
        rest = scratch[n - 1 :]
        self.come = rest[:n]
        self.send = rest[n : 2 * n]
        self.recv = rest[2 * n : 3 * n]

    @staticmethod
    def count(axes):
        return 4 * len(axes) - 1

    @staticmethod
    def scratch(axes, block, dtype):
        sizes = tuple(lax.axis_size(a) for a in axes)
        n = len(axes)
        parts = [pltpu.VMEM(sizes[:i] + block, dtype) for i in range(1, n)]
        come = [pltpu.VMEM((sizes[i] - 1,) + sizes[:i] + block, dtype) for i in range(n)]
        sems = [pltpu.SemaphoreType.DMA((sizes[i] - 1,) + sizes[:i]) for i in range(n)]
        return parts + come + sems + sems

    def coords(self, tag):
        return tuple(peer_of(a, k) for a, k in zip(self.axes, tag))

    def forward(self, tag, src):
        level = len(tag) - 1
        k, prefix = tag[-1], tag[:-1]
        axis = self.axes[level]
        self.push(
            src,
            self.come[level].at[(k - 1,) + self.coords(prefix)],
            self.send[level].at[(k - 1,) + prefix],
            self.recv[level].at[(k - 1,) + prefix],
            {axis: peer_of(axis, k)},
        )

    def order(self, level):
        return sorted(grid_of(self.axes[:level], True), key=lambda tag: tag[-1:] == (0,))

    def begin(self):
        for tag in self.order(len(self.axes)):
            if tag[-1]:
                self.forward(tag, self.place(self.src, self.coords(tag)))

    def held(self, level, coords):
        return self.place(self.src, coords) if level == len(self.axes) else self.part[level].at[coords]

    def step(self, level, tag):
        axis = self.axes[level]
        here = self.coords(tag)
        parts = [self.held(level + 1, here + (lax.axis_index(axis),))]
        for k in offsets(axis):
            slot = self.come[level].at[(k - 1,) + here]
            at = (k - 1,) + tag
            self.arrive(slot, self.send[level].at[at], self.recv[level].at[at], {axis: source_of(axis, k)})
            parts.append(slot)
        target = self.held(level, here) if level else self.out
        sum_into(target, parts)
        if level and tag[-1]:
            self.forward(tag, target)

    def stage(self, wave):
        level = len(self.axes) - wave
        if level >= 0:
            for tag in self.order(level):
                self.step(level, tag)


class Settle(Reduce):
    def __init__(self, src, out, axes, scratch, place):
        Copies.__init__(self)
        n = len(axes)
        self.src, self.out, self.axes, self.place = src, out, axes, place
        self.come, self.send, self.recv = scratch[:n], scratch[n : 2 * n], scratch[2 * n :]

    @staticmethod
    def scratch(axes, block, dtype):
        return Reduce.scratch(axes, block, dtype)[len(axes) - 1 :]

    def held(self, level, coords):
        return self.place(self.src, coords + tuple(lax.axis_index(a) for a in self.axes[level:]))


class Spread(Copies):
    def __init__(self, src, out, axes, sems):
        super().__init__()
        self.src, self.out, self.axes = src, out, axes
        self.send, self.recv, self.own = sems
        self.waves = {}
        for tag in grid_of(axes):
            if any(tag):
                self.waves.setdefault(sum(1 for k in tag if k), []).append(tag)

    @staticmethod
    def scratch(axes):
        shape = shape_of(axes)
        return [pltpu.SemaphoreType.DMA(shape), pltpu.SemaphoreType.DMA(shape), pltpu.SemaphoreType.DMA]

    def slot(self, tag):
        return self.out.at[tuple(source_of(a, k) for a, k in zip(self.axes, tag))]

    def spread(self, tag):
        last = max([i for i, k in enumerate(tag) if k], default=-1)
        for level in range(last + 1, len(self.axes)):
            axis = self.axes[level]
            for k in offsets(axis):
                at = tag[:level] + (k,) + tag[level + 1 :]
                src = self.slot(tag) if any(tag) else self.src
                self.push(src, self.slot(tag), self.send.at[at], self.recv.at[at], {axis: peer_of(axis, k)})

    def begin(self):
        nobody = (0,) * len(self.axes)
        self.spread(nobody)
        self.keep(self.src, self.slot(nobody), self.own)

    def stage(self, wave):
        for tag in self.waves.get(wave, ()):
            last = max(i for i, k in enumerate(tag) if k)
            peer = {self.axes[last]: peer_of(self.axes[last], tag[last])}
            self.arrive(self.slot(tag), self.send.at[tag], self.recv.at[tag], peer)
            self.spread(tag)


class Widen(Copies):
    def __init__(self, src, out, scratch):
        super().__init__()
        self.src, self.out = src, out

    def begin(self):
        pass

    def stage(self, wave):
        if wave == 1:
            sum_into(self.out, [self.src])


class Join(Widen):
    def stage(self, wave):
        if wave == 1:
            share = self.src.shape[-1]
            for i in range(2 * TEAM):
                self.out[:, i * share : (i + 1) * share] = self.src[i // 2, i % 2].astype(self.out.dtype)


class Fan(Copies):
    def __init__(self, src, out, axis, sems):
        super().__init__()
        self.src, self.out, self.axis = src, out, axis
        self.send, self.recv, self.own = sems
        self.half = lax.axis_size(axis) // 2

    @staticmethod
    def scratch(axis):
        n = lax.axis_size(axis)
        return [pltpu.SemaphoreType.DMA((n,)), pltpu.SemaphoreType.DMA((n, 2)), pltpu.SemaphoreType.DMA]

    def slot(self, owner, core):
        width = self.src.shape[-1]
        return self.out.at[owner % self.half, :, pl.ds(pl.multiple_of(core * width, width), width)]

    def begin(self):
        me, core = lax.axis_index(self.axis), lax.axis_index("col")
        target = me // self.half
        slot = self.slot(me, core)
        self.copies = []
        for k in offsets(self.axis):
            peer = {self.axis: peer_of(self.axis, k), "col": target}
            for c in (0, 1):

                @pl.when(core == c)
                def _(c=c):
                    pltpu.make_async_remote_copy(
                        src_ref=self.src, dst_ref=slot, send_sem=self.send.at[k], recv_sem=self.recv.at[k, c],
                        device_id=peer, device_id_type=MESH,
                    ).start()

        @pl.when(target == core)
        def _():
            pltpu.make_async_copy(self.src, slot, self.own).start()

        for c in (0, 1):

            @pl.when((target != core) & (core == c))
            def _(c=c):
                pltpu.make_async_remote_copy(
                    src_ref=self.src, dst_ref=slot, send_sem=self.send.at[0], recv_sem=self.recv.at[0, c],
                    device_id={"col": 1 - core}, device_id_type=MESH,
                ).start()

    def stage(self, wave):
        if wave != 1:
            return
        me, core = lax.axis_index(self.axis), lax.axis_index("col")
        for k in (0,) + offsets(self.axis):
            owner = source_of(self.axis, k)
            for c in (0, 1):
                expected = owner // self.half == core
                if k == 0:
                    expected = expected & (core != c)

                @pl.when(expected)
                def _(k=k, c=c, owner=owner):
                    slot = self.slot(owner, c)
                    self.arrive(slot, self.send.at[k], self.recv.at[k, c], {self.axis: owner, "col": c} if k else {"col": 1 - core})

    def drain(self):
        me, core = lax.axis_index(self.axis), lax.axis_index("col")
        target = me // self.half
        slot = self.slot(me, core)

        def left(k, peer):
            pltpu.make_async_remote_copy(
                src_ref=self.src, dst_ref=slot, send_sem=self.send.at[k], recv_sem=self.recv.at[k, 0],
                device_id=peer, device_id_type=MESH,
            ).wait_send()

        for k in offsets(self.axis):
            left(k, {self.axis: peer_of(self.axis, k), "col": target})

        @pl.when(target == core)
        def _():
            pltpu.make_async_copy(self.src, slot, self.own).wait()

        @pl.when(target != core)
        def _():
            left(0, {"col": 1 - core})


class Fold(Copies):
    def __init__(self, src, out, axis, scratch):
        super().__init__()
        self.src, self.out, self.axis = src, out, axis
        self.come, self.send, self.recv, self.own = scratch
        self.half = lax.axis_size(axis) // 2

    @staticmethod
    def scratch(axis, block, dtype):
        n = lax.axis_size(axis)
        return [
            pltpu.VMEM((n,) + block, dtype),
            pltpu.SemaphoreType.DMA((n, 2)),
            pltpu.SemaphoreType.DMA((n,)),
            pltpu.SemaphoreType.DMA,
        ]

    def each(self, visit, cores=(0, 1)):
        me, core = lax.axis_index(self.axis), lax.axis_index("col")
        for k in offsets(self.axis) + (0,):
            owner = peer_of(self.axis, k)
            for c in cores:

                @pl.when(owner // self.half == core)
                def _(k=k, c=c, owner=owner):
                    piece = self.src.at[c, owner % self.half]
                    if k:
                        visit(k, c, piece, {self.axis: owner, "col": c})
                    else:

                        @pl.when(core == c)
                        def _():
                            visit(k, None, piece, None)

                        @pl.when(core != c)
                        def _():
                            visit(k, c, piece, {"col": 1 - core})

    def begin(self, cores=(0, 1)):
        def start(k, c, piece, peer):
            if peer is None:
                pltpu.make_async_copy(piece, self.come.at[k], self.own).start()
            else:
                pltpu.make_async_remote_copy(
                    src_ref=piece, dst_ref=self.come.at[k], send_sem=self.send.at[k, c], recv_sem=self.recv.at[k],
                    device_id=peer, device_id_type=MESH,
                ).start()

        self.each(start, cores)

    def stage(self, wave):
        if wave != 1:
            return
        me, core = lax.axis_index(self.axis), lax.axis_index("col")
        holder = me // self.half
        for k in offsets(self.axis):
            peer = {self.axis: source_of(self.axis, k), "col": holder}
            self.arrive(self.come.at[k], self.send.at[k, 0], self.recv.at[k], peer)

        @pl.when(holder != core)
        def _():
            self.arrive(self.come.at[0], self.send.at[0, 0], self.recv.at[0], {"col": 1 - core})

        @pl.when(holder == core)
        def _():
            pltpu.make_async_copy(self.src.at[0, 0], self.come.at[0], self.own).wait()

        sum_into(self.out, [self.come.at[k] for k in (0,) + offsets(self.axis)])

    def drain(self):
        def left(k, c, piece, peer):
            if peer is not None:
                pltpu.make_async_remote_copy(
                    src_ref=piece, dst_ref=self.come.at[k], send_sem=self.send.at[k, c], recv_sem=self.recv.at[k],
                    device_id=peer, device_id_type=MESH,
                ).wait_send()

        self.each(left)


class Trade(Copies):
    def __init__(self, src, out, scratch):
        super().__init__()
        self.src, self.out = src, out
        self.cut, self.send, self.recv, self.own = scratch

    @staticmethod
    def scratch(piece, dtype):
        shape = shape_of(("t", "col"))
        sems = [pltpu.SemaphoreType.DMA(shape), pltpu.SemaphoreType.DMA(shape), pltpu.SemaphoreType.DMA]
        return [pltpu.VMEM(shape + piece, dtype)] + sems

    def begin(self):
        share = self.cut.shape[-1]
        for i in range(2 * TEAM):
            self.cut[i // 2, i % 2] = self.src[:, i * share : (i + 1) * share]
        t, c = lax.axis_index("t"), lax.axis_index("col")
        for tag in grid_of(("t", "col")):
            to = peer_of("t", tag[0]), peer_of("col", tag[1])
            if any(tag):
                peer = {"t": to[0], "col": to[1]}
                self.push(self.cut.at[to], self.out.at[c, t], self.send.at[tag], self.recv.at[tag], peer)
        self.keep(self.cut.at[t, c], self.out.at[c, t], self.own)

    def stage(self, wave):
        if wave == 1:
            for tag in grid_of(("t", "col")):
                if any(tag):
                    peer = source_of("t", tag[0]), source_of("col", tag[1])
                    slot = self.out.at[peer[1], peer[0]]
                    self.arrive(slot, self.send.at[tag], self.recv.at[tag], {"t": peer[0], "col": peer[1]})


class Undeal(Copies):
    def __init__(self, src, out, scratch):
        super().__init__()
        self.src, self.out = src, out
        self.come, self.part, self.send, self.recv, self.send_on, self.recv_on, self.own = scratch

    @staticmethod
    def scratch(block, dtype):
        f, t, c = (lax.axis_size(a) for a in ("f", "t", "col"))
        first, second = pltpu.SemaphoreType.DMA((f - 1, t, c)), pltpu.SemaphoreType.DMA((t, c))
        return [
            pltpu.VMEM((f - 1, t, c) + block, dtype),
            pltpu.VMEM((t, c) + block, dtype),
            first, first, second, second, pltpu.SemaphoreType.DMA,
        ]

    def begin(self):
        for tag in grid_of(("t", "col"), True):
            to = peer_of("t", tag[0]), peer_of("col", tag[1])
            for k in offsets("f"):
                at = (k - 1,) + tag
                self.push(
                    self.src.at[(peer_of("f", k),) + to], self.come.at[(k - 1,) + to],
                    self.send.at[at], self.recv.at[at], {"f": peer_of("f", k)},
                )

    def stage(self, wave):
        t, c, f = (lax.axis_index(a) for a in ("t", "col", "f"))
        if wave == 1:
            for tag in grid_of(("t", "col"), True):
                to = peer_of("t", tag[0]), peer_of("col", tag[1])
                parts = [self.src.at[(f,) + to]]
                for k in offsets("f"):
                    at = (k - 1,) + tag
                    slot = self.come.at[(k - 1,) + to]
                    self.arrive(slot, self.send.at[at], self.recv.at[at], {"f": source_of("f", k)})
                    parts.append(slot)
                sum_into(self.part.at[to], parts)
                if any(tag):
                    self.push(
                        self.part.at[to], self.out.at[t, c], self.send_on.at[tag], self.recv_on.at[tag],
                        {"t": to[0], "col": to[1]},
                    )
                else:
                    self.keep(self.part.at[to], self.out.at[t, c], self.own)
        if wave == 2:
            for tag in grid_of(("t", "col")):
                if any(tag):
                    peer = source_of("t", tag[0]), source_of("col", tag[1])
                    self.arrive(
                        self.out.at[peer], self.send_on.at[tag], self.recv_on.at[tag], {"t": peer[0], "col": peer[1]}
                    )


def run_jobs(jobs, order):
    done = [-1] * len(jobs)
    for i in tuple(order) + tuple(range(len(jobs))) * 7:
        done[i] += 1
        if done[i]:
            jobs[i].stage(done[i])
        else:
            jobs[i].begin()
    for job in jobs:
        job.drain()


def exchange(cid, peers, plan, operands, out_shapes, out_spaces, order=(), through=None):
    n_in, n_out = len(operands), len(out_shapes)
    in_specs, aliases = [VMEM] * n_in, {}
    if through is not None:
        aliases[n_in] = n_out
        operands, in_specs = list(operands) + [through], in_specs + [ANY]
        out_shapes, out_spaces = list(out_shapes) + [like(through.shape, through.dtype)], list(out_spaces) + [ANY]
    scratch = [s for job in plan for s in job[4]]

    def kernel(*refs):
        n_op, n_res = len(in_specs), len(out_shapes)
        ins, outs, rest = refs[:n_in], refs[n_op : n_op + n_out], refs[n_op + n_res :]
        greet(peers())
        jobs = []
        for make, src, out, options, own in plan:
            mine, rest = rest[: len(own)], rest[len(own) :]
            jobs.append(make(ins[src], outs[out], *options[0], mine, **options[1]))
        run_jobs(jobs, order)

    return pl.pallas_call(
        kernel,
        out_shape=tuple(out_shapes),
        in_specs=in_specs,
        out_specs=tuple(out_spaces),
        scratch_shapes=scratch,
        input_output_aliases=aliases,
        compiler_params=pltpu.CompilerParams(collective_id=cid, has_side_effects=True),
    )(*operands)


class Swap(Copies):
    def __init__(self, src, out, sems):
        super().__init__()
        self.src, self.out = src, out
        self.send, self.recv = sems

    @staticmethod
    def scratch():
        return [pltpu.SemaphoreType.DMA, pltpu.SemaphoreType.DMA]

    def begin(self):
        other = 1 - lax.axis_index("col")
        self.push(self.src.at[other], self.out, self.send, self.recv, {"col": other})

    def stage(self, wave):
        if wave == 1:
            self.arrive(self.out, self.send, self.recv, {"col": 1 - lax.axis_index("col")})


class AllReduce(Copies):
    def __init__(self, src, out, axes, scratch):
        super().__init__()
        n = Reduce.count(axes)
        self.depth = len(axes)
        self.reduce = Reduce(src, scratch[n], axes, scratch[:n])
        self.gather = Spread(scratch[n], out, axes, scratch[n + 1 :])

    @staticmethod
    def scratch(axes, block, dtype):
        return Reduce.scratch(axes, block, dtype) + [pltpu.VMEM(block, dtype)] + Spread.scratch(axes)

    def begin(self):
        self.reduce.begin()

    def stage(self, wave):
        if wave <= self.depth:
            self.reduce.stage(wave)
        if wave == self.depth:
            self.gather.begin()
        if wave > self.depth:
            self.gather.stage(wave - self.depth)

    def drain(self):
        self.reduce.drain()
        self.gather.drain()


def shape_of(axes):
    return tuple(lax.axis_size(a) for a in axes)


def lanes_of(width):
    def place(ref, coords):
        return ref.at[tuple(coords[:-1]) + (slice(None), pl.ds(pl.multiple_of(coords[-1] * width, width), width))]

    return place


def col_first(ref, coords):
    return ref.at[(coords[-1],) + tuple(coords[:-1])]


def like(shape, dtype):
    return jax.ShapeDtypeStruct(shape, dtype)


def pair_sum(values, cid, through=None):
    share = 128 // len(values)
    wide = jnp.concatenate([jnp.broadcast_to(v, (v.shape[0], share)) for v in values], axis=1)
    both, *passed = exchange(
        cid, lambda: along("col"),
        [(Gather, 0, 0, ((PAIR,), {}), Gather.scratch(PAIR))],
        [wide], [like((2,) + wide.shape, F32)], [VMEM], through=through,
    )
    total = both[0] + both[1]
    return [total[:, i * share : i * share + 1] for i in range(len(values))] + passed


def recurrence(retain, source, lead, backward, cid):
    rows, width = retain.shape
    tiles = rows // 8
    sizes = shape_of(ORDER)
    count = sizes[0] * sizes[1] * sizes[2]
    lines = width // 128
    block = (-(-2 * lines // 8) * 8, 128)

    def kernel(r_ref, s_ref, lead_ref, h_ref, in_ref, c_ref, mine, ends, send, recv, own):
        peers = across(*ORDER)
        hail(peers)
        row = lax.broadcasted_iota(jnp.int32, (8, width), 0)

        def tile(i):
            return pl.ds(pl.multiple_of(8 * (tiles - 1 - i if backward else i), 8), 8)

        def step(i, carry):
            decay, state = carry
            at = tile(i)
            r, s = r_ref[at, :], s_ref[at, :]
            for by in (1, 2, 4):
                keep = row < 8 - by if backward else row >= by
                shift = 8 - by if backward else by
                r_by = jnp.where(keep, pltpu.roll(r, shift, 0), 1.0)
                s_by = jnp.where(keep, pltpu.roll(s, shift, 0), 0.0)
                s = r * s_by + s
                r = r * r_by
            s = s + r * state
            r = r * decay
            c_ref[at, :] = r
            h_ref[at, :] = s
            end = 0 if backward else 7
            return r[end : end + 1, :], s[end : end + 1, :]

        one = jnp.ones((1, width), F32)
        decay, state = lax.fori_loop(0, tiles, step, (one, jnp.zeros((1, width), F32)))
        decay, state = lead_ref[0:1, :] * decay, lead_ref[0:1, :] * state
        for j in range(lines):
            mine[j : j + 1, :] = decay[:, 128 * j : 128 * (j + 1)]
            mine[lines + j : lines + j + 1, :] = state[:, 128 * j : 128 * (j + 1)]
        pl.semaphore_wait(pltpu.get_barrier_semaphore(), len(peers))
        jobs = Copies()
        here = tuple(lax.axis_index(a) for a in ORDER)
        for tag in grid_of(ORDER):
            if any(tag):
                peer = {a: peer_of(a, k) for a, k in zip(ORDER, tag)}
                jobs.push(mine, ends.at[here], send.at[tag], recv.at[tag], peer)
        jobs.keep(mine, ends.at[here], own)
        for tag in grid_of(ORDER):
            if any(tag):
                peer = {a: source_of(a, k) for a, k in zip(ORDER, tag)}
                jobs.arrive(ends.at[tuple(peer[a] for a in ORDER)], send.at[tag], recv.at[tag], peer)
        jobs.drain()
        me = (here[0] * sizes[1] + here[1]) * sizes[2] + here[2]
        entering = jnp.zeros((lines, 128), F32)
        for i in range(count):
            peer = count - 1 - i if backward else i
            t, rest = divmod(peer, sizes[1] * sizes[2])
            f, c = divmod(rest, sizes[2])
            pair = ends[t, f, c]
            ahead = jnp.where(peer > me if backward else peer < me, 1, 0)
            entering = jnp.where(ahead == 1, pair[:lines] * entering + pair[lines : 2 * lines], entering)
        entering = jnp.concatenate([entering[j : j + 1, :] for j in range(lines)], axis=1)
        in_ref[...] = jnp.broadcast_to(entering, (8, width))

        def fix(i, carry):
            at = tile(i)
            h_ref[at, :] = h_ref[at, :] + c_ref[at, :] * entering
            return carry

        lax.fori_loop(0, tiles, fix, 0)

    states, entering = pl.pallas_call(
        kernel,
        out_shape=(like((rows, width), F32), like((8, width), F32)),
        in_specs=[VMEM] * 3,
        out_specs=(VMEM, VMEM),
        scratch_shapes=[
            pltpu.VMEM((rows, width), F32),
            pltpu.VMEM(block, F32),
            pltpu.VMEM(sizes + block, F32),
            pltpu.SemaphoreType.DMA(sizes),
            pltpu.SemaphoreType.DMA(sizes),
            pltpu.SemaphoreType.DMA,
        ],
        compiler_params=pltpu.CompilerParams(collective_id=cid, has_side_effects=True),
        name="back_states" if backward else "states",
    )(retain, source, jnp.broadcast_to(lead, (8, width)))
    return states, entering[0]


def from_behind(x, axis, by):
    peers = lax.axis_size(axis)
    pairs = [(i, i + by) for i in range(peers) if 0 <= i + by < peers]
    return lax.ppermute(x, axis, pairs)


def gelu_tanh(values):
    return jax.nn.gelu(values, approximate=True)


def gates_of(decay_pre, input_pre, decay_param, conv_low, starts):
    rate_gate = jax.nn.sigmoid(decay_pre)
    in_gate = jax.nn.sigmoid(input_pre)
    log_decay = -8.0 * jax.nn.softplus(decay_param) * rate_gate
    retain = jnp.where(starts, 0.0, jnp.exp(log_decay))
    multiplier = jnp.where(
        starts, 1.0, jnp.sqrt(jnp.maximum(-jnp.expm1(2.0 * log_decay), SQRT_FLOOR))
    )
    return (retain, multiplier * in_gate * conv_low)


def normalize_back(gradient, values, inverse, scale_vec, cid, through=None):
    weighted = gradient * (1.0 + scale_vec)
    scale_grad = jnp.sum(gradient * values * inverse, axis=0)
    inner_sum, *passed = pair_sum([jnp.sum(weighted * values, axis=1, keepdims=True)], cid, through)
    return (inverse * weighted - values * inverse**3 * inner_sum / D, scale_grad, *passed)


def arrange(own, other):
    first = lax.axis_index("col") == 0
    return jnp.where(first, own, other), jnp.where(first, other, own)


def halves(x):
    width = x.shape[1] // 2
    return jnp.stack([x[:, :width], x[:, width:]])


def half_of(x):
    width = x.shape[1] // 2
    return jnp.where(lax.axis_index("col") == 0, x[:, :width], x[:, width:])


TOKEN_AXES = ("t", "row", "col")
WEIGHT_AXES = ("t", "f", "col")
PAIR = ("col",)


def fetch_first(mixer, branch, output, stream, scale, down):
    t, f, c = shape_of(WEIGHT_AXES)
    width, inner = mixer.shape
    piece = (down.shape[0], down.shape[1] // (2 * TEAM))
    place = lanes_of(inner)
    axes = (WEIGHT_AXES,)
    plan = [
        (Gather, 0, 0, (axes, {"place": place}), Gather.scratch(WEIGHT_AXES)),
        (Fan, 3, 3, (("row",), {}), Fan.scratch("row")),
        (Gather, 1, 1, (axes, {"place": place}), Gather.scratch(WEIGHT_AXES)),
        (Gather, 2, 2, (axes, {"place": col_first}), Gather.scratch(WEIGHT_AXES)),
        (Gather, 4, 4, ((PAIR,), {}), Gather.scratch(PAIR)),
        (Trade, 5, 5, ((), {}), Trade.scratch(piece, BF16)),
    ]
    wide = like((t, f, width, 2 * inner), BF16)
    outs = [wide, wide, like((c, t, f) + output.shape, BF16), like((1, stream.shape[0], 2 * stream.shape[1]), BF16)]
    outs += [like((2, 1, scale.shape[0]), F32), like((2, TEAM) + piece, BF16)]
    mixer_t, branch_t, output_t, tokens, scale, down = exchange(
        0, lambda: along("t", "f") + across("row", "col") + diagonal("t", "col"), plan,
        [mixer, branch, output, stream, scale[None], down], outs, [ANY] * 4 + [VMEM, ANY],
        order=(0, 1, 2, 3, 4, 0, 5, 2, 3),
    )
    return mixer_t.reshape(-1, 2 * inner), branch_t.reshape(-1, 2 * inner), output_t.reshape(-1, output.shape[1]), tokens[0], scale.reshape(-1), down


def fetch_second(normed, cotangent, gate, up, down):
    t, r, _ = shape_of(TOKEN_AXES)
    fleet = lax.axis_size("f")
    rows, width = normed.shape
    units, inner = gate.shape
    share = down.shape[-1]
    half = fleet // 2
    token, fan = Gather.scratch(TOKEN_AXES), Fan.scratch("f")
    place = lanes_of(width)

    def kernel(n_ref, c_ref, g_ref, u_ref, d_ref, n_all, c_all, gw, uw, d_all, g_out, u_out, held, sem, *rest):
        normed_job = Gather(n_ref, n_all, TOKEN_AXES, rest[:3], place)
        cot_job = Gather(c_ref, c_all, TOKEN_AXES, rest[3:6], place)
        gate_job, up_job = Fan(g_ref, gw, "f", rest[6:9]), Fan(u_ref, uw, "f", rest[9:12])
        down_job = Gather(d_ref, d_all, ("f",), rest[12:15], lambda ref, at: ref.at[:, :, at[0]])
        jobs = (normed_job, gate_job, up_job, down_job, cot_job)
        greet(along("t", "row") + across("f", "col"))
        for job in jobs:
            job.begin()
        normed_job.stage(1)
        cot_job.stage(1)
        normed_job.stage(2)
        normed_job.stage(3)
        normed_job.drain()
        for job in (gate_job, up_job):
            job.stage(1)
            job.drain()
        blocks = t * r

        def fetch(i):
            return pltpu.make_async_copy(n_all.at[i // r, i % r], held.at[i % 2], sem.at[i % 2])

        fetch(0).start()

        def product(i, carry):
            @pl.when(i + 1 < blocks)
            def _():
                fetch(i + 1).start()

            fetch(i).wait()
            at = pl.ds(pl.multiple_of(i * rows, rows), rows)
            for weight, out in ((gw, g_out), (uw, u_out)):
                for j in range(half):
                    out[at, j * units : (j + 1) * units] = dot_nt(held[i % 2], weight[j])
            return carry

        lax.fori_loop(0, blocks, product, 0)
        cot_job.stage(2)
        down_job.stage(1)
        cot_job.stage(3)
        for job in (down_job, cot_job):
            job.drain()

    every = like((t, r, rows, 2 * width), BF16)
    weight = like((half, units, 2 * inner), BF16)
    first = like((t * r * rows, share), F32)
    n_all, c_all, gate_t, up_t, down_t, gate_out, up_out = pl.pallas_call(
        kernel,
        out_shape=(every, every, weight, weight, like(down.shape[:2] + (fleet,) + down.shape[2:], BF16), first, first),
        in_specs=[VMEM] * 5,
        out_specs=(ANY, ANY, VMEM, VMEM, ANY, VMEM, VMEM),
        scratch_shapes=[pltpu.VMEM((2, rows, 2 * width), BF16), pltpu.SemaphoreType.DMA((2,))]
        + token + token + fan + fan + Gather.scratch(("f",)),
        compiler_params=pltpu.CompilerParams(collective_id=1, has_side_effects=True),
        name="fetch_second",
    )(normed, cotangent, gate, up, down)
    return (
        n_all.reshape(-1, 2 * width),
        c_all.reshape(-1, 2 * width),
        gate_t.reshape(-1, 2 * inner),
        up_t.reshape(-1, 2 * inner),
        down_t.reshape(-1, share),
        gate_out,
        up_out,
    )


def diagonal(*axes):
    pairs = zip(across(*axes), [tag for tag in grid_of(axes) if any(tag)])
    return [peer for peer, tag in pairs if all(tag)]


def team_peers():
    return along("t", "row") + across("f", "col") + diagonal("t", "col")


def send_second(gate, up, hidden, gate_t, up_t, second_all, cot_all, late):
    t, r, _ = shape_of(TOKEN_AXES)
    fleet = lax.axis_size("f")
    tokens, wide = second_all.shape
    share = gate.shape[1]
    rows, width = tokens // (t * r), wide // 2
    half = fleet // 2
    units = share // half
    shard = width // (TEAM * fleet)
    block, weight, piece = (rows, width), (units, width), (shard, share)
    lane, tile = 512, wide // 4
    part, chunk = tile // shard, 256
    place = lanes_of(width)
    settle, fold = Settle.scratch(TOKEN_AXES, block, BF16), Fold.scratch("f", weight, BF16)
    undeal = Undeal.scratch(piece, BF16)

    def kernel(*refs):
        g_ref, u_ref, h_ref, gw_ref, uw_ref, all_ref, cot_ref, _ = refs[:8]
        delta_ref, grad_g, grad_u, grad_d = refs[8:12]
        src, fold_g, fold_u, down, gt_ref, ut_ref, ht_ref, tiles, tile_sem = refs[12:21]
        rest = refs[21:]
        sums = Settle(src, delta_ref, TOKEN_AXES, rest[: len(settle)], place)
        rest = rest[len(settle) :]
        g_job = Fold(fold_g, grad_g, "f", rest[: len(fold)])
        u_job = Fold(fold_u, grad_u, "f", rest[len(fold) : 2 * len(fold)])
        d_job = Undeal(down, grad_d, rest[2 * len(fold) :])

        def fetch(ref, i):
            at = pl.ds(pl.multiple_of(i * tile, tile), tile)
            return pltpu.make_async_copy(ref.at[:, at], tiles.at[i % 2], tile_sem.at[i % 2])

        def turn(src_ref, out_ref):
            def some(i, carry):
                at = pl.ds(pl.multiple_of(i * chunk, chunk), chunk)
                out_ref[:, at] = src_ref[at, :].T
                return carry

            lax.fori_loop(0, tokens // chunk, some, 0)

        def down_gradients(i, carry):
            @pl.when(i + 1 < wide // tile)
            def _():
                fetch(cot_ref, i + 1).start()

            @pl.when(i + 1 == wide // tile)
            def _():
                fetch(all_ref, 0).start()

            fetch(cot_ref, i).wait()
            value = dot_nn(ht_ref[...], tiles[i % 2]).T.astype(BF16)
            for j in range(part):
                n = i * part + j
                down[n % fleet, n // fleet % TEAM, n // (TEAM * fleet)] = value[j * shard : (j + 1) * shard]
            return carry

        def block_of(tag):
            coords = sums.coords(tag)
            at = pl.ds(pl.multiple_of((coords[0] * r + coords[1]) * rows, rows), rows)

            def product(j, carry):
                col = pl.ds(pl.multiple_of(j * lane, lane), lane)
                value = dot_nn(g_ref[at, :], gw_ref[:, col]) + dot_nn(u_ref[at, :], uw_ref[:, col])
                src[coords[0], coords[1], :, col] = value.astype(BF16)
                return carry

            lax.fori_loop(0, wide // lane, product, 0)
            for k in offsets("col"):
                sums.forward(tag + (k,), place(src, sums.coords(tag + (k,))))

        def gradients(i, carry):
            @pl.when(i + 1 < wide // tile)
            def _():
                fetch(all_ref, i + 1).start()

            fetch(all_ref, i).wait()
            h, at = i // (width // tile), pl.ds(pl.multiple_of(i % (width // tile) * tile, tile), tile)
            for left, out in ((gt_ref, fold_g), (ut_ref, fold_u)):
                value = dot_nn(left[...], tiles[i % 2]).astype(BF16)
                for j in range(half):
                    out[h, j, :, at] = value[j * units : (j + 1) * units]
            return carry

        def half_gradients(h):
            first = h * (width // tile)
            lax.fori_loop(first, first + width // tile, gradients, 0)
            g_job.begin((h,))
            u_job.begin((h,))

        away = [tag for tag in sums.order(2) if tag[-1]]
        home = [tag for tag in sums.order(2) if not tag[-1]]
        team = sums.order(1)
        fetch(cot_ref, 0).start()
        greet(team_peers())
        block_of(away[0])
        turn(h_ref, ht_ref)
        sums.step(2, away[0])
        lax.fori_loop(0, wide // tile, down_gradients, 0)
        d_job.begin()
        block_of(away[1])
        block_of(home[0])
        sums.step(2, away[1])
        block_of(away[2])
        sums.step(2, home[0])
        sums.step(1, team[0])
        turn(g_ref, gt_ref)
        turn(u_ref, ut_ref)
        half_gradients(0)
        sums.step(2, away[2])
        block_of(away[3])
        block_of(home[1])
        sums.step(2, away[3])
        block_of(home[2])
        sums.step(2, home[1])
        sums.step(1, team[1])
        half_gradients(1)
        d_job.stage(1)
        sums.step(2, home[2])
        block_of(home[3])
        sums.step(1, team[2])
        sums.step(2, home[3])
        sums.step(1, team[3])
        sums.stage(3)
        g_job.stage(1)
        u_job.stage(1)
        d_job.stage(2)
        for job in (sums, g_job, u_job, d_job):
            job.drain()

    delta, grad_gate, grad_up, grad_down = pl.pallas_call(
        kernel,
        out_shape=(like(block, F32), like(weight, BF16), like(weight, BF16), like((TEAM, 2) + piece, BF16)),
        in_specs=[VMEM] * 5 + [ANY] * 3,
        out_specs=(VMEM,) * 4,
        scratch_shapes=[
            pltpu.VMEM((t, r, rows, wide), BF16),
            pltpu.VMEM((2, half) + weight, BF16),
            pltpu.VMEM((2, half) + weight, BF16),
            pltpu.VMEM((fleet, TEAM, 2) + piece, BF16),
            pltpu.VMEM((share, tokens), BF16),
            pltpu.VMEM((share, tokens), BF16),
            pltpu.VMEM((share, tokens), BF16),
            pltpu.VMEM((2, tokens, tile), BF16),
            pltpu.SemaphoreType.DMA((2,)),
        ]
        + settle + fold + fold + undeal,
        compiler_params=pltpu.CompilerParams(
            collective_id=2, has_side_effects=True, vmem_limit_bytes=67_000_000
        ),
        name="send_second",
    )(gate, up, hidden, gate_t, up_t, second_all, cot_all, late)
    return delta, grad_gate, grad_up, grad_down


def to_stream(partial, cid):
    rows, width = partial.shape
    block = (rows, width // 2)
    (out,) = exchange(
        cid, lambda: across("row", "col"),
        [(Fold, 0, 0, (("row",), {}), Fold.scratch("row", block, BF16))],
        [halves(partial).reshape((2, 1) + block)], [like(block, F32)], [VMEM],
    )
    return out


class FanSwap(Fan):
    def __init__(self, src, out, sems, other):
        super().__init__(src, out, "row", sems[:3])
        self.send_on, self.recv_on = sems[3:]
        self.other = other

    @staticmethod
    def scratch():
        return Fan.scratch("row") + Swap.scratch()

    def stage(self, wave):
        super().stage(wave)
        other, width = 1 - lax.axis_index("col"), self.src.shape[-1]
        if wave == 1:
            src = self.out.at[0, :, pl.ds(pl.multiple_of(other * width, width), width)]
            self.push(src, self.other, self.send_on, self.recv_on, {"col": other})
        if wave == 2:
            self.arrive(self.other, self.send_on, self.recv_on, {"col": other})

    def drain(self):
        super().drain()
        Copies.drain(self)


def to_tokens(block, mixed, cid):
    rows, width = block.shape
    fan, gather = FanSwap.scratch(), Gather.scratch(PAIR)

    def kernel(block_ref, mixed_ref, out_ref, other_ref, both_ref, *sems):
        greet(across("row", "col"))
        jobs = [
            FanSwap(block_ref, out_ref, sems[: len(fan)], other_ref),
            Gather(mixed_ref, both_ref, PAIR, sems[len(fan) :]),
        ]
        run_jobs(jobs, ())

    out, other, both = pl.pallas_call(
        kernel,
        out_shape=(like((1, rows, 2 * width), BF16), like(block.shape, BF16), like((2,) + mixed.shape, BF16)),
        in_specs=[VMEM] * 2,
        out_specs=(VMEM,) * 3,
        scratch_shapes=fan + gather,
        compiler_params=pltpu.CompilerParams(collective_id=cid, has_side_effects=True),
        name="to_tokens",
    )(block, mixed)
    both_rows = jnp.concatenate(arrange(half_of(out[0]), other), axis=0)
    return out[0], both_rows, both.reshape(-1, mixed.shape[1])


def dealt(x, axes, dtype):
    sizes = shape_of(axes)
    members = sizes[0] * sizes[1] * sizes[2]
    width = -(-x.size // (members * 8 * 128)) * 128
    flat = jnp.pad(x.reshape(-1), (0, members * 8 * width - x.size))
    return flat.reshape(sizes + (8, width)).astype(dtype)


STREAM_AXES = ("t", "f", "row")


def finish_block(normed, branch, mixer, delta, cid):
    rows, width = delta.shape
    token = (rows, width // 2)
    plan = [
        (Fold, 0, 0, (("row",), {}), Fold.scratch("row", token, BF16)),
        (Swap, 1, 1, ((), {}), Swap.scratch()),
        (Gather, 2, 2, ((PAIR,), {}), Gather.scratch(PAIR)),
        (Gather, 3, 3, ((PAIR,), {}), Gather.scratch(PAIR)),
    ]
    outs = [like(token, F32), like(token, BF16), like((2,) + branch.shape, BF16), like((2,) + mixer.shape, BF16)]
    delta, other, branch, mixer = exchange(
        cid, lambda: across("row", "col"), plan,
        [halves(delta).reshape((2, 1) + token), halves(normed), branch, mixer], outs, [VMEM] * 4,
    )
    rows = jnp.concatenate(arrange(half_of(normed), other), axis=0)
    return delta, rows, branch.reshape(-1, branch.shape[2]), mixer.reshape(-1, mixer.shape[2])


def send_first(grads, inner_sums, head_grads, stream_sums, done, through, cid):
    sizes = shape_of(DP)
    n = len(grads)
    block = (grads[0].shape[0] // (sizes[0] * sizes[1]), grads[0].shape[1])
    axes_of = (ORDER, STREAM_AXES, ORDER)
    sums = (inner_sums, stream_sums, head_grads)
    lanes = head_grads.shape[-1]
    small = [dealt(x, axes, F32) for x, axes in zip(sums[:2], axes_of)]
    small.append(head_grads.reshape(shape_of(ORDER) + (-1, lanes)).astype(BF16))
    plan = [
        (AllReduce, n + i, n + i, ((axes,), {}), AllReduce.scratch(axes, x.shape[3:], x.dtype))
        for i, (x, axes) in enumerate(zip(small, axes_of))
    ]
    plan += [(Reduce, i, i, ((DP,), {}), Reduce.scratch(DP, block, BF16)) for i in range(n)]
    bulk = tuple(range(3, 3 + n))
    pieces = done[2].shape
    wide = [like(done[0].shape, F32), like(done[1].shape, F32), like((pieces[2], 2 * TEAM * pieces[3]), F32)]
    plan += [(cut, n + 3 + i, n + 3 + i, ((), {}), []) for i, cut in enumerate((Widen, Widen, Join))]
    rest = tuple(range(3 + n, 6 + n))
    got = exchange(
        cid, lambda: along("t", "f", "row", "col"), plan,
        [g.reshape(sizes + block) for g in grads] + small + list(done),
        [like(block, F32)] * n + [like(x.shape, x.dtype) for x in small] + wide, [VMEM] * (n + 6),
        order=(0, 1, 2) * 3 + bulk + (0, 1, 2) + rest * 2 + bulk * 2, through=through,
    )
    return got[:n], [x.reshape(-1)[: y.size].reshape(y.shape).astype(F32) for x, y in zip(got[n : n + 3], sums)], got[n + 3 : -1], got[-1]


def on_device(
    stream,
    scale_first,
    branch_weight,
    branch_bias,
    mixer_weight,
    mixer_bias,
    conv_weight,
    conv_bias,
    decay_weight,
    decay_bias,
    input_weight,
    input_bias,
    decay_param,
    output_weight,
    output_bias,
    scale_second,
    gate_weight,
    gate_bias,
    up_weight,
    up_bias,
    down_weight,
    down_bias,
    cotangent,
):
    mixer_t, branch_t, output_t, stream_all, scale_all, down_pieces = fetch_first(
        mixer_weight.T, branch_weight.T, output_weight.T, stream, scale_first, down_weight.T
    )
    inner = mixer_t.shape[0]
    stream_wide = stream.astype(F32)
    tokens_wide = stream_all.astype(F32)
    inverse_all = lax.rsqrt(jnp.sum(tokens_wide * tokens_wide, axis=1, keepdims=True) / D + EPSILON)
    normed_first = (tokens_wide * inverse_all * (1.0 + scale_all)).astype(BF16)
    mixer_pre = dot_nt(normed_first, mixer_t) + mixer_bias
    branch_pre = dot_nt(normed_first, branch_t) + branch_bias
    branch_act, branch_back = jax.vjp(gelu_tanh, branch_pre)

    steps = mixer_pre.shape[0]
    first_token = lax.axis_index(ORDER) * steps
    position = (first_token + jnp.arange(steps, dtype=jnp.int32)) % LEN
    margin = CONV - 1
    left_edge = from_behind(mixer_pre[steps - margin :], ORDER, 1)
    padded = jnp.concatenate([left_edge, mixer_pre], axis=0)
    conv_out = conv_bias + jnp.zeros_like(mixer_pre)
    for offset in range(CONV):
        in_reach = (position >= offset)[:, None]
        conv_out = conv_out + jnp.where(
            in_reach, conv_weight[offset] * padded[margin - offset : margin - offset + steps], 0.0
        )
    conv_low = conv_out.astype(BF16)
    conv_wide = conv_low.astype(F32)
    heads, block = decay_weight.shape[0], decay_weight.shape[1]
    parts = [conv_low[:, h * block : (h + 1) * block] for h in range(heads)]
    decay_pre = jnp.concatenate([dot_nn(x, decay_weight[h]) for h, x in enumerate(parts)], 1) + decay_bias
    input_pre = jnp.concatenate([dot_nn(x, input_weight[h]) for h, x in enumerate(parts)], 1) + input_bias
    starts = (position == 0)[:, None]

    def gate_values(decay_in, input_in, param_in, conv_in):
        return gates_of(decay_in, input_in, param_in, conv_in, starts)

    (retain, source), gate_back = jax.vjp(gate_values, decay_pre, input_pre, decay_param, conv_wide)
    ones_row = jnp.ones((1, inner), F32)
    states, state_in = recurrence(retain, source, ones_row, False, 3)
    mixed_low = (states * branch_act).astype(BF16)
    first_out = stream_wide + to_stream(dot_nt(mixed_low, output_t).astype(BF16), 4) + output_bias
    second_total, first_total = pair_sum(
        [jnp.sum(x * x, axis=1, keepdims=True) for x in (first_out, stream_wide)], 5
    )
    inverse_second = lax.rsqrt(second_total / D + EPSILON)
    inverse_first = lax.rsqrt(first_total / D + EPSILON)
    normed_second = first_out * inverse_second * (1.0 + scale_second)

    share = down_weight.shape[0] // (2 * TEAM)
    second_all, cot_all, gate_t, up_t, down_t, gate_pre, up_pre = fetch_second(
        normed_second.astype(BF16), cotangent, gate_weight.T, up_weight.T, down_pieces
    )
    mine = (lax.axis_index("t") * 2 + lax.axis_index("col")) * share
    gate_b = lax.dynamic_slice(gate_bias, (mine,), (share,))
    up_b = lax.dynamic_slice(up_bias, (mine,), (share,))

    gate_pre = gate_pre + gate_b
    up_pre = up_pre + up_b
    hidden, hidden_back = jax.vjp(lambda g, u: gelu_tanh(g) * u, gate_pre, up_pre)
    hidden_low = hidden.astype(BF16)
    delta_hidden = dot_nn(cot_all, down_t)
    delta_gate, delta_up = hidden_back(delta_hidden)
    gate_low, up_low = delta_gate.astype(BF16), delta_up.astype(BF16)
    down_part = dot_nt(hidden_low, down_t).astype(BF16)
    down_rows = lax.psum_scatter(down_part, "col", scatter_dimension=1, tiled=True)
    delta_second, grad_gate, grad_up, grad_down = send_second(
        gate_low, up_low, hidden_low, gate_t, up_t, second_all, cot_all, down_part
    )
    delta_result = cotangent.astype(F32)

    norm_second_part, grad_scale_second, down_rows = normalize_back(
        delta_second, first_out, inverse_second, scale_second, 6, down_rows
    )
    down_proj = lax.psum_scatter(down_rows, ("t", "row"), scatter_dimension=0, tiled=True)
    delta_first = delta_result + norm_second_part
    out_all, out_rows, mixed_rows = to_tokens(delta_first.astype(BF16), mixed_low, 7)
    output_part = dot_tn(out_rows, mixed_rows).astype(BF16)
    grad_output = lax.psum_scatter(output_part, DP, scatter_dimension=0, tiled=True)
    delta_mixed = dot_nn(out_all, output_t)
    delta_state = delta_mixed * branch_act
    (delta_branch,) = branch_back(delta_mixed * states)
    branch_low = delta_branch.astype(BF16)
    retain_next = jnp.concatenate([retain[1:], ones_row], axis=0)
    back_state, _ = recurrence(retain_next, delta_state, retain[:1], True, 8)
    state_prev = jnp.concatenate([state_in[None], states[:-1]], axis=0)
    delta_decay_pre, delta_input_pre, grad_decay_param, delta_conv = gate_back(
        (back_state * state_prev, back_state)
    )
    decay_low = delta_decay_pre.astype(BF16)
    input_low = delta_input_pre.astype(BF16)

    def split(x):
        return [x[:, h * block : (h + 1) * block] for h in range(heads)]

    grad_decay_weight = jnp.stack([dot_tn(a, b) for a, b in zip(parts, split(decay_low))])
    grad_input_weight = jnp.stack([dot_tn(a, b) for a, b in zip(parts, split(input_low))])
    delta_conv = delta_conv + jnp.concatenate(
        [dot_nt(a, decay_weight[h]) for h, a in enumerate(split(decay_low))], 1
    )
    delta_conv = delta_conv + jnp.concatenate(
        [dot_nt(a, input_weight[h]) for h, a in enumerate(split(input_low))], 1
    )
    delta_padded = jnp.zeros_like(padded)
    conv_grads = []
    for offset in range(CONV):
        in_reach = (position >= offset)[:, None]
        masked = jnp.where(in_reach, delta_conv, 0.0)
        conv_grads.append(
            jnp.sum(masked * padded[margin - offset : margin - offset + steps], axis=0)
        )
        delta_padded = delta_padded + jnp.pad(
            masked * conv_weight[offset], ((margin - offset, offset), (0, 0))
        )
    grad_conv_weight = jnp.stack(conv_grads, axis=0)
    right_edge = from_behind(delta_padded[:margin], ORDER, -1)
    delta_mixer = delta_padded[margin:] + jnp.pad(right_edge, ((steps - margin, 0), (0, 0)))
    mixer_low = delta_mixer.astype(BF16)

    def spread(x):
        return lax.dynamic_update_slice(jnp.zeros_like(gate_bias), x, (mine,))

    small = [
        jnp.sum(delta_branch, axis=0),
        jnp.sum(delta_mixer, axis=0),
        jnp.sum(delta_conv, axis=0),
        jnp.sum(delta_decay_pre, axis=0),
        jnp.sum(delta_input_pre, axis=0),
        grad_decay_param,
        spread(jnp.sum(delta_gate, axis=0)),
        spread(jnp.sum(delta_up, axis=0)),
        grad_conv_weight.reshape(-1),
    ]
    delta_normed_part = dot_nn(branch_low, branch_t) + dot_nn(mixer_low, mixer_t)
    delta_normed_first, first_rows, branch_rows, mixer_rows = finish_block(
        normed_first, branch_low, mixer_low, delta_normed_part.astype(BF16), 10
    )
    norm_first_part, grad_scale_first = normalize_back(
        delta_normed_first, stream_wide, inverse_first, scale_first, 12
    )
    (grad_mixer, grad_branch), (total, stream_sums, head_grads), wide_grads, down_proj = send_first(
        [dot_tn(mixer_rows, first_rows).astype(BF16), dot_tn(branch_rows, first_rows).astype(BF16)],
        jnp.concatenate(small),
        jnp.stack([grad_decay_weight, grad_input_weight]),
        jnp.stack(
            [grad_scale_second, jnp.sum(delta_first, axis=0), jnp.sum(delta_result, axis=0), grad_scale_first]
        ),
        (grad_gate, grad_up, grad_down),
        down_proj,
        13,
    )
    result = (first_out + down_proj.astype(F32) + down_bias).astype(BF16)
    grad_stream = delta_first + norm_first_part
    sums, at = [], 0
    for x in small:
        sums.append(total[at : at + x.shape[0]])
        at += x.shape[0]
    return (
        result,
        grad_stream,
        stream_sums[3],
        grad_branch.T,
        sums[0],
        grad_mixer.T,
        sums[1],
        sums[8].reshape(CONV, inner),
        sums[2],
        head_grads[0],
        sums[3],
        head_grads[1],
        sums[4],
        sums[5],
        grad_output.T.astype(F32),
        stream_sums[1],
        stream_sums[0],
        wide_grads[0].T,
        sums[6],
        wide_grads[1].T,
        sums[7],
        wide_grads[2].T,
        stream_sums[2],
    )


def solution(mesh):
    shape = mesh.devices.shape
    names = mesh.axis_names
    fleet = mesh.shape["dp"] // TEAM
    at = names.index("dp")
    split_mesh = Mesh(
        mesh.devices.reshape(shape[:at] + (TEAM, fleet) + shape[at + 1 :]),
        names[:at] + DP + names[at + 1 :],
    )
    tokens, fan_in = P((*DP, "row"), "col"), P("col", ("row", *DP))
    fan_out, inner, wide = P("row", ("col", *DP)), P("row"), P("col")
    heads = P("row", None, None)
    return jax.shard_map(
        on_device,
        mesh=split_mesh,
        in_specs=(
            tokens, wide, fan_in, inner, fan_in, inner, P(None, "row"), inner,
            heads, inner, heads, inner, inner, fan_out, wide, wide,
            fan_in, inner, fan_in, inner, fan_out, wide, tokens,
        ),
        out_specs=(
            tokens, tokens, wide, fan_in, inner, fan_in, inner, P(None, "row"), inner,
            heads, inner, heads, inner, inner, fan_out, wide, wide,
            fan_in, inner, fan_in, inner, fan_out, wide,
        ),
        check_vma=False,
    )
```

```python
import math

import jax
import jax.numpy as jnp
from jax import lax
from jax.experimental import pallas as pl
from jax.experimental.pallas import tpu as pltpu
from jax.sharding import Mesh, PartitionSpec as P


D = 2560
CONV = 4
LEN = 4096
EPSILON = 1e-06
SQRT_FLOOR = 0.0001
GELU = (2.0 / math.pi) ** 0.5
TEAM = 4
NT = (((1,), (1,)), ((), ()))
TN = (((0,), (0,)), ((), ()))
F32 = jnp.float32
BF16 = jnp.bfloat16
DP = ("t", "f")
ORDER = ("t", "f", "col")


def dot_nn(a, b):
    return jnp.dot(a, b, preferred_element_type=F32)


def dot_nt(a, b):
    return lax.dot_general(a, b, NT, preferred_element_type=F32)


def dot_tn(a, b):
    return lax.dot_general(a, b, TN, preferred_element_type=F32)


MESH = pl.DeviceIdType.MESH
ANY = pl.BlockSpec(memory_space=pl.ANY)
VMEM = pl.BlockSpec(memory_space=pltpu.VMEM)


def peer_of(axis, k):
    n, me = lax.axis_size(axis), lax.axis_index(axis)
    if k == 0:
        return me
    if n == 2:
        return 1 - me
    if n == 4:
        return (me + 1 - 2 * (me % 2), (me + 2) % 4, 3 - me)[k - 1]
    return (me + k) % n


def source_of(axis, k):
    n, me = lax.axis_size(axis), lax.axis_index(axis)
    return peer_of(axis, k) if n in (2, 4) else (me + n - k) % n


def offsets(axis):
    n = lax.axis_size(axis)
    return (1, 3, 2) if n == 4 else tuple(range(1, n))


def grid_of(axes, far_first=False):
    grid = [()]
    for axis in axes:
        near = (0,) + offsets(axis)
        grid = [tag + (k,) for tag in grid for k in (near[::-1] if far_first else near)]
    return grid


def hail(peers):
    for peer in peers:
        pl.semaphore_signal(pltpu.get_barrier_semaphore(), inc=1, device_id=peer, device_id_type=MESH)


def greet(peers):
    hail(peers)
    pl.semaphore_wait(pltpu.get_barrier_semaphore(), len(peers))


def only(condition, act):
    if condition is None:
        act()
    else:
        pl.when(condition)(act)


def along(*axes):
    return [{axis: peer_of(axis, k)} for axis in axes for k in offsets(axis)]


def across(*axes):
    return [
        {axis: peer_of(axis, k) for axis, k in zip(axes, tag)} for tag in grid_of(axes) if any(tag)
    ]


class Copies:
    def __init__(self):
        self.sent = []

    def push(self, src, dst, send, recv, peer, condition=None):
        copy = pltpu.make_async_remote_copy(
            src_ref=src, dst_ref=dst, send_sem=send, recv_sem=recv, device_id=peer, device_id_type=MESH
        )
        only(condition, copy.start)
        self.sent.append((condition, copy.wait_send))

    def arrive(self, dst, send, recv, peer):
        pltpu.make_async_remote_copy(
            src_ref=dst, dst_ref=dst, send_sem=send, recv_sem=recv, device_id=peer, device_id_type=MESH
        ).wait_recv()

    def keep(self, src, dst, sem):
        copy = pltpu.make_async_copy(src, dst, sem)
        copy.start()
        self.sent.append((None, copy.wait))

    def drain(self):
        for condition, wait in self.sent:
            only(condition, wait)


def leading(ref, coords):
    return ref.at[tuple(coords)]


class Gather(Copies):
    def __init__(self, src, out, axes, sems, place=leading):
        super().__init__()
        self.src, self.out, self.axes, self.place = src, out, axes, place
        self.send, self.recv, self.own = sems
        self.size, self.at = lax.axis_size(axes[0]), lax.axis_index(axes[0])
        self.nobody = (0,) * len(axes)
        self.waves = {}
        line = [0] + [v for far in range(1, self.size) for v in (-far, far)]
        for v in line:
            for rest in grid_of(axes[1:]):
                tag = (v,) + rest
                if any(tag):
                    self.waves.setdefault(sum(1 for k in tag if k), []).append(tag)

    @staticmethod
    def scratch(axes):
        sizes = [lax.axis_size(a) for a in axes]
        shape = (2 * sizes[0] - 1,) + tuple(sizes[1:])
        return [pltpu.SemaphoreType.DMA(shape), pltpu.SemaphoreType.DMA(shape), pltpu.SemaphoreType.DMA]

    def index(self, tag):
        return (tag[0] + self.size - 1,) + tag[1:]

    def exists(self, far):
        if far == 0:
            return None
        return self.at + far >= 0 if far < 0 else self.at + far < self.size

    def slot(self, tag):
        rest = [source_of(a, k) for a, k in zip(self.axes[1:], tag[1:])]
        return self.place(self.out, [self.at + tag[0]] + rest)

    def spread(self, tag):
        last = max([i for i, k in enumerate(tag) if k], default=-1)
        here = self.exists(tag[0])
        src = self.slot(tag) if any(tag) else self.src

        def send(there, peer, condition):
            if here is not None and condition is not None:
                condition = here & condition
            elif condition is None:
                condition = here
            at = self.index(there)
            self.push(src, self.slot(tag), self.send.at[at], self.recv.at[at], peer, condition)

        if last <= 0:
            if 0 <= tag[0] < self.size - 1:
                send((tag[0] + 1,) + tag[1:], {self.axes[0]: self.at - 1}, self.at > 0)
            if -self.size + 1 < tag[0] <= 0:
                send((tag[0] - 1,) + tag[1:], {self.axes[0]: self.at + 1}, self.at < self.size - 1)
        for level in range(max(last, 0) + 1, len(self.axes)):
            axis = self.axes[level]
            for k in offsets(axis):
                send(tag[:level] + (k,) + tag[level + 1 :], {axis: peer_of(axis, k)}, None)

    def begin(self):
        self.spread(self.nobody)
        self.keep(self.src, self.slot(self.nobody), self.own)

    def stage(self, wave):
        for tag in self.waves.get(wave, ()):
            last = max(i for i, k in enumerate(tag) if k)
            if last:
                peer = {self.axes[last]: peer_of(self.axes[last], tag[last])}
            else:
                peer = {self.axes[0]: self.at + (1 if tag[0] > 0 else -1)}
            at = self.index(tag)
            only(
                self.exists(tag[0]),
                lambda: self.arrive(self.slot(tag), self.send.at[at], self.recv.at[at], peer),
            )
            self.spread(tag)


def sum_into(out, parts):
    rows = out.shape[0]
    step = next(n for n in (32, 16, 8, rows) if rows % n == 0)

    def some(i, carry):
        at = pl.ds(pl.multiple_of(i * step, step), step)
        total = parts[0][at, :].astype(F32)
        for part in parts[1:]:
            total = total + part[at, :].astype(F32)
        out[at, :] = total.astype(out.dtype)
        return carry

    lax.fori_loop(0, rows // step, some, 0)


class Reduce(Copies):
    def __init__(self, src, out, axes, scratch, place=leading):
        super().__init__()
        n = len(axes)
        self.src, self.out, self.axes, self.place = src, out, axes, place
        self.part = {i + 1: scratch[i] for i in range(n - 1)}
        rest = scratch[n - 1 :]
        self.come = rest[:n]
        self.send = rest[n : 2 * n]
        self.recv = rest[2 * n : 3 * n]

    @staticmethod
    def count(axes):
        return 4 * len(axes) - 1

    @staticmethod
    def scratch(axes, block, dtype):
        sizes = tuple(lax.axis_size(a) for a in axes)
        n = len(axes)
        parts = [pltpu.VMEM(sizes[:i] + block, dtype) for i in range(1, n)]
        come = [pltpu.VMEM((sizes[i] - 1,) + sizes[:i] + block, dtype) for i in range(n)]
        sems = [pltpu.SemaphoreType.DMA((sizes[i] - 1,) + sizes[:i]) for i in range(n)]
        return parts + come + sems + sems

    def coords(self, tag):
        return tuple(peer_of(a, k) for a, k in zip(self.axes, tag))

    def forward(self, tag, src):
        level = len(tag) - 1
        k, prefix = tag[-1], tag[:-1]
        axis = self.axes[level]
        self.push(
            src,
            self.come[level].at[(k - 1,) + self.coords(prefix)],
            self.send[level].at[(k - 1,) + prefix],
            self.recv[level].at[(k - 1,) + prefix],
            {axis: peer_of(axis, k)},
        )

    def order(self, level):
        return sorted(grid_of(self.axes[:level], True), key=lambda tag: tag[-1:] == (0,))

    def begin(self):
        for tag in self.order(len(self.axes)):
            if tag[-1]:
                self.forward(tag, self.place(self.src, self.coords(tag)))

    def held(self, level, coords):
        return self.place(self.src, coords) if level == len(self.axes) else self.part[level].at[coords]

    def step(self, level, tag):
        axis = self.axes[level]
        here = self.coords(tag)
        parts = [self.held(level + 1, here + (lax.axis_index(axis),))]
        for k in offsets(axis):
            slot = self.come[level].at[(k - 1,) + here]
            at = (k - 1,) + tag
            self.arrive(slot, self.send[level].at[at], self.recv[level].at[at], {axis: source_of(axis, k)})
            parts.append(slot)
        target = self.held(level, here) if level else self.out
        sum_into(target, parts)
        if level and tag[-1]:
            self.forward(tag, target)

    def stage(self, wave):
        level = len(self.axes) - wave
        if level >= 0:
            for tag in self.order(level):
                self.step(level, tag)


class Settle(Reduce):
    def __init__(self, src, out, axes, scratch, place):
        Copies.__init__(self)
        n = len(axes)
        self.src, self.out, self.axes, self.place = src, out, axes, place
        self.come, self.send, self.recv = scratch[:n], scratch[n : 2 * n], scratch[2 * n :]

    @staticmethod
    def scratch(axes, block, dtype):
        return Reduce.scratch(axes, block, dtype)[len(axes) - 1 :]

    def held(self, level, coords):
        return self.place(self.src, coords + tuple(lax.axis_index(a) for a in self.axes[level:]))


class Spread(Copies):
    def __init__(self, src, out, axes, sems):
        super().__init__()
        self.src, self.out, self.axes = src, out, axes
        self.send, self.recv, self.own = sems
        self.waves = {}
        for tag in grid_of(axes):
            if any(tag):
                self.waves.setdefault(sum(1 for k in tag if k), []).append(tag)

    @staticmethod
    def scratch(axes):
        shape = shape_of(axes)
        return [pltpu.SemaphoreType.DMA(shape), pltpu.SemaphoreType.DMA(shape), pltpu.SemaphoreType.DMA]

    def slot(self, tag):
        return self.out.at[tuple(source_of(a, k) for a, k in zip(self.axes, tag))]

    def spread(self, tag):
        last = max([i for i, k in enumerate(tag) if k], default=-1)
        for level in range(last + 1, len(self.axes)):
            axis = self.axes[level]
            for k in offsets(axis):
                at = tag[:level] + (k,) + tag[level + 1 :]
                src = self.slot(tag) if any(tag) else self.src
                self.push(src, self.slot(tag), self.send.at[at], self.recv.at[at], {axis: peer_of(axis, k)})

    def begin(self):
        nobody = (0,) * len(self.axes)
        self.spread(nobody)
        self.keep(self.src, self.slot(nobody), self.own)

    def stage(self, wave):
        for tag in self.waves.get(wave, ()):
            last = max(i for i, k in enumerate(tag) if k)
            peer = {self.axes[last]: peer_of(self.axes[last], tag[last])}
            self.arrive(self.slot(tag), self.send.at[tag], self.recv.at[tag], peer)
            self.spread(tag)


class Widen(Copies):
    def __init__(self, src, out, scratch):
        super().__init__()
        self.src, self.out = src, out

    def begin(self):
        pass

    def stage(self, wave):
        if wave == 1:
            sum_into(self.out, [self.src])


class Join(Widen):
    def stage(self, wave):
        if wave == 1:
            share = self.src.shape[-1]
            for i in range(2 * TEAM):
                self.out[:, i * share : (i + 1) * share] = self.src[i // 2, i % 2].astype(self.out.dtype)


class Fan(Copies):
    def __init__(self, src, out, axis, sems):
        super().__init__()
        self.src, self.out, self.axis = src, out, axis
        self.send, self.recv, self.own = sems
        self.half = lax.axis_size(axis) // 2

    @staticmethod
    def scratch(axis):
        n = lax.axis_size(axis)
        return [pltpu.SemaphoreType.DMA((n,)), pltpu.SemaphoreType.DMA((n, 2)), pltpu.SemaphoreType.DMA]

    def slot(self, owner, core):
        width = self.src.shape[-1]
        return self.out.at[owner % self.half, :, pl.ds(pl.multiple_of(core * width, width), width)]

    def begin(self):
        me, core = lax.axis_index(self.axis), lax.axis_index("col")
        target = me // self.half
        slot = self.slot(me, core)
        self.copies = []
        for k in offsets(self.axis):
            peer = {self.axis: peer_of(self.axis, k), "col": target}
            for c in (0, 1):

                @pl.when(core == c)
                def _(c=c):
                    pltpu.make_async_remote_copy(
                        src_ref=self.src, dst_ref=slot, send_sem=self.send.at[k], recv_sem=self.recv.at[k, c],
                        device_id=peer, device_id_type=MESH,
                    ).start()

        @pl.when(target == core)
        def _():
            pltpu.make_async_copy(self.src, slot, self.own).start()

        for c in (0, 1):

            @pl.when((target != core) & (core == c))
            def _(c=c):
                pltpu.make_async_remote_copy(
                    src_ref=self.src, dst_ref=slot, send_sem=self.send.at[0], recv_sem=self.recv.at[0, c],
                    device_id={"col": 1 - core}, device_id_type=MESH,
                ).start()

    def stage(self, wave):
        if wave != 1:
            return
        me, core = lax.axis_index(self.axis), lax.axis_index("col")
        for k in (0,) + offsets(self.axis):
            owner = source_of(self.axis, k)
            for c in (0, 1):
                expected = owner // self.half == core
                if k == 0:
                    expected = expected & (core != c)

                @pl.when(expected)
                def _(k=k, c=c, owner=owner):
                    slot = self.slot(owner, c)
                    self.arrive(slot, self.send.at[k], self.recv.at[k, c], {self.axis: owner, "col": c} if k else {"col": 1 - core})

    def drain(self):
        me, core = lax.axis_index(self.axis), lax.axis_index("col")
        target = me // self.half
        slot = self.slot(me, core)

        def left(k, peer):
            pltpu.make_async_remote_copy(
                src_ref=self.src, dst_ref=slot, send_sem=self.send.at[k], recv_sem=self.recv.at[k, 0],
                device_id=peer, device_id_type=MESH,
            ).wait_send()

        for k in offsets(self.axis):
            left(k, {self.axis: peer_of(self.axis, k), "col": target})

        @pl.when(target == core)
        def _():
            pltpu.make_async_copy(self.src, slot, self.own).wait()

        @pl.when(target != core)
        def _():
            left(0, {"col": 1 - core})


class Fold(Copies):
    def __init__(self, src, out, axis, scratch):
        super().__init__()
        self.src, self.out, self.axis = src, out, axis
        self.come, self.send, self.recv, self.own = scratch
        self.half = lax.axis_size(axis) // 2

    @staticmethod
    def scratch(axis, block, dtype):
        n = lax.axis_size(axis)
        return [
            pltpu.VMEM((n,) + block, dtype),
            pltpu.SemaphoreType.DMA((n, 2)),
            pltpu.SemaphoreType.DMA((n,)),
            pltpu.SemaphoreType.DMA,
        ]

    def each(self, visit, cores=(0, 1)):
        me, core = lax.axis_index(self.axis), lax.axis_index("col")
        for k in offsets(self.axis) + (0,):
            owner = peer_of(self.axis, k)
            for c in cores:

                @pl.when(owner // self.half == core)
                def _(k=k, c=c, owner=owner):
                    piece = self.src.at[c, owner % self.half]
                    if k:
                        visit(k, c, piece, {self.axis: owner, "col": c})
                    else:

                        @pl.when(core == c)
                        def _():
                            visit(k, None, piece, None)

                        @pl.when(core != c)
                        def _():
                            visit(k, c, piece, {"col": 1 - core})

    def begin(self, cores=(0, 1)):
        def start(k, c, piece, peer):
            if peer is None:
                pltpu.make_async_copy(piece, self.come.at[k], self.own).start()
            else:
                pltpu.make_async_remote_copy(
                    src_ref=piece, dst_ref=self.come.at[k], send_sem=self.send.at[k, c], recv_sem=self.recv.at[k],
                    device_id=peer, device_id_type=MESH,
                ).start()

        self.each(start, cores)

    def stage(self, wave):
        if wave != 1:
            return
        me, core = lax.axis_index(self.axis), lax.axis_index("col")
        holder = me // self.half
        for k in offsets(self.axis):
            peer = {self.axis: source_of(self.axis, k), "col": holder}
            self.arrive(self.come.at[k], self.send.at[k, 0], self.recv.at[k], peer)

        @pl.when(holder != core)
        def _():
            self.arrive(self.come.at[0], self.send.at[0, 0], self.recv.at[0], {"col": 1 - core})

        @pl.when(holder == core)
        def _():
            pltpu.make_async_copy(self.src.at[0, 0], self.come.at[0], self.own).wait()

        sum_into(self.out, [self.come.at[k] for k in (0,) + offsets(self.axis)])

    def drain(self):
        def left(k, c, piece, peer):
            if peer is not None:
                pltpu.make_async_remote_copy(
                    src_ref=piece, dst_ref=self.come.at[k], send_sem=self.send.at[k, c], recv_sem=self.recv.at[k],
                    device_id=peer, device_id_type=MESH,
                ).wait_send()

        self.each(left)


class Deal(Copies):
    def __init__(self, src, out, scratch):
        super().__init__()
        self.src, self.out = src, out
        self.cut, self.send, self.recv, self.own = scratch

    @staticmethod
    def scratch(piece, dtype):
        shape = shape_of(("t", "col"))
        sems = pltpu.SemaphoreType.DMA(shape + (lax.axis_size("f"),))
        return [pltpu.VMEM(shape + piece, dtype), sems, sems, pltpu.SemaphoreType.DMA]

    def onward(self, tag):
        t, c = source_of("t", tag[0]), source_of("col", tag[1])
        slot = self.out.at[c, t, lax.axis_index("f")]
        src = slot if any(tag) else self.cut.at[t, c]
        for k in offsets("f"):
            at = tag + (k,)
            self.push(src, slot, self.send.at[at], self.recv.at[at], {"f": peer_of("f", k)})

    def begin(self):
        share = self.cut.shape[-1]
        for i in range(2 * TEAM):
            self.cut[i // 2, i % 2] = self.src[:, i * share : (i + 1) * share]
        t, c, f = (lax.axis_index(a) for a in ("t", "col", "f"))
        for tag in grid_of(("t", "col")):
            to = peer_of("t", tag[0]), peer_of("col", tag[1])
            if any(tag):
                peer, at = {"t": to[0], "col": to[1]}, tag + (0,)
                self.push(self.cut.at[to], self.out.at[c, t, f], self.send.at[at], self.recv.at[at], peer)
        self.onward((0, 0))
        self.keep(self.cut.at[t, c], self.out.at[c, t, f], self.own)

    def stage(self, wave):
        f = lax.axis_index("f")
        for tag in grid_of(("t", "col")):
            t, c = source_of("t", tag[0]), source_of("col", tag[1])
            if wave == 1 and any(tag):
                at = tag + (0,)
                slot = self.out.at[c, t, f]
                self.arrive(slot, self.send.at[at], self.recv.at[at], {"t": t, "col": c})
                self.onward(tag)
            if wave == 2:
                for k in offsets("f"):
                    at = tag + (k,)
                    slot = self.out.at[c, t, source_of("f", k)]
                    self.arrive(slot, self.send.at[at], self.recv.at[at], {"f": source_of("f", k)})


class Undeal(Copies):
    def __init__(self, src, out, scratch):
        super().__init__()
        self.src, self.out = src, out
        self.come, self.part, self.send, self.recv, self.send_on, self.recv_on, self.own = scratch

    @staticmethod
    def scratch(block, dtype):
        f, t, c = (lax.axis_size(a) for a in ("f", "t", "col"))
        first, second = pltpu.SemaphoreType.DMA((f - 1, t, c)), pltpu.SemaphoreType.DMA((t, c))
        return [
            pltpu.VMEM((f - 1, t, c) + block, dtype),
            pltpu.VMEM((t, c) + block, dtype),
            first, first, second, second, pltpu.SemaphoreType.DMA,
        ]

    def begin(self):
        for tag in grid_of(("t", "col"), True):
            to = peer_of("t", tag[0]), peer_of("col", tag[1])
            for k in offsets("f"):
                at = (k - 1,) + tag
                self.push(
                    self.src.at[(peer_of("f", k),) + to], self.come.at[(k - 1,) + to],
                    self.send.at[at], self.recv.at[at], {"f": peer_of("f", k)},
                )

    def stage(self, wave):
        t, c, f = (lax.axis_index(a) for a in ("t", "col", "f"))
        if wave == 1:
            for tag in grid_of(("t", "col"), True):
                to = peer_of("t", tag[0]), peer_of("col", tag[1])
                parts = [self.src.at[(f,) + to]]
                for k in offsets("f"):
                    at = (k - 1,) + tag
                    slot = self.come.at[(k - 1,) + to]
                    self.arrive(slot, self.send.at[at], self.recv.at[at], {"f": source_of("f", k)})
                    parts.append(slot)
                sum_into(self.part.at[to], parts)
                if any(tag):
                    self.push(
                        self.part.at[to], self.out.at[t, c], self.send_on.at[tag], self.recv_on.at[tag],
                        {"t": to[0], "col": to[1]},
                    )
                else:
                    self.keep(self.part.at[to], self.out.at[t, c], self.own)
        if wave == 2:
            for tag in grid_of(("t", "col")):
                if any(tag):
                    peer = source_of("t", tag[0]), source_of("col", tag[1])
                    self.arrive(
                        self.out.at[peer], self.send_on.at[tag], self.recv_on.at[tag], {"t": peer[0], "col": peer[1]}
                    )


def run_jobs(jobs, order):
    done = [-1] * len(jobs)
    for i in tuple(order) + tuple(range(len(jobs))) * 7:
        done[i] += 1
        if done[i]:
            jobs[i].stage(done[i])
        else:
            jobs[i].begin()
    for job in jobs:
        job.drain()


def exchange(cid, peers, plan, operands, out_shapes, out_spaces, order=(), through=None):
    n_in, n_out = len(operands), len(out_shapes)
    in_specs, aliases = [VMEM] * n_in, {}
    if through is not None:
        aliases[n_in] = n_out
        operands, in_specs = list(operands) + [through], in_specs + [ANY]
        out_shapes, out_spaces = list(out_shapes) + [like(through.shape, through.dtype)], list(out_spaces) + [ANY]
    scratch = [s for job in plan for s in job[4]]

    def kernel(*refs):
        n_op, n_res = len(in_specs), len(out_shapes)
        ins, outs, rest = refs[:n_in], refs[n_op : n_op + n_out], refs[n_op + n_res :]
        greet(peers())
        jobs = []
        for make, src, out, options, own in plan:
            mine, rest = rest[: len(own)], rest[len(own) :]
            jobs.append(make(ins[src], outs[out], *options[0], mine, **options[1]))
        run_jobs(jobs, order)

    return pl.pallas_call(
        kernel,
        out_shape=tuple(out_shapes),
        in_specs=in_specs,
        out_specs=tuple(out_spaces),
        scratch_shapes=scratch,
        input_output_aliases=aliases,
        compiler_params=pltpu.CompilerParams(collective_id=cid, has_side_effects=True),
    )(*operands)


class Swap(Copies):
    def __init__(self, src, out, sems):
        super().__init__()
        self.src, self.out = src, out
        self.send, self.recv = sems

    @staticmethod
    def scratch():
        return [pltpu.SemaphoreType.DMA, pltpu.SemaphoreType.DMA]

    def begin(self):
        other = 1 - lax.axis_index("col")
        self.push(self.src.at[other], self.out, self.send, self.recv, {"col": other})

    def stage(self, wave):
        if wave == 1:
            self.arrive(self.out, self.send, self.recv, {"col": 1 - lax.axis_index("col")})


class AllReduce(Copies):
    def __init__(self, src, out, axes, scratch):
        super().__init__()
        n = Reduce.count(axes)
        self.depth = len(axes)
        self.reduce = Reduce(src, scratch[n], axes, scratch[:n])
        self.gather = Spread(scratch[n], out, axes, scratch[n + 1 :])

    @staticmethod
    def scratch(axes, block, dtype):
        return Reduce.scratch(axes, block, dtype) + [pltpu.VMEM(block, dtype)] + Spread.scratch(axes)

    def begin(self):
        self.reduce.begin()

    def stage(self, wave):
        if wave <= self.depth:
            self.reduce.stage(wave)
        if wave == self.depth:
            self.gather.begin()
        if wave > self.depth:
            self.gather.stage(wave - self.depth)

    def drain(self):
        self.reduce.drain()
        self.gather.drain()


def shape_of(axes):
    return tuple(lax.axis_size(a) for a in axes)


def lanes_of(width):
    def place(ref, coords):
        return ref.at[tuple(coords[:-1]) + (slice(None), pl.ds(pl.multiple_of(coords[-1] * width, width), width))]

    return place


def col_first(ref, coords):
    return ref.at[(coords[-1],) + tuple(coords[:-1])]


def like(shape, dtype):
    return jax.ShapeDtypeStruct(shape, dtype)


def pair_sum(values, cid, through=None):
    share = 128 // len(values)
    wide = jnp.concatenate([jnp.broadcast_to(v, (v.shape[0], share)) for v in values], axis=1)
    both, *passed = exchange(
        cid, lambda: along("col"),
        [(Gather, 0, 0, ((PAIR,), {}), Gather.scratch(PAIR))],
        [wide], [like((2,) + wide.shape, F32)], [VMEM], through=through,
    )
    total = both[0] + both[1]
    return [total[:, i * share : i * share + 1] for i in range(len(values))] + passed


def recurrence(retain, source, lead, backward, cid):
    rows, width = retain.shape
    tiles = rows // 8
    sizes = shape_of(ORDER)
    count = sizes[0] * sizes[1] * sizes[2]
    lines = width // 128
    block = (-(-2 * lines // 8) * 8, 128)

    def kernel(r_ref, s_ref, lead_ref, h_ref, in_ref, c_ref, mine, ends, send, recv, own):
        peers = across(*ORDER)
        hail(peers)
        row = lax.broadcasted_iota(jnp.int32, (8, width), 0)

        def tile(i):
            return pl.ds(pl.multiple_of(8 * (tiles - 1 - i if backward else i), 8), 8)

        def step(i, carry):
            decay, state = carry
            at = tile(i)
            r, s = r_ref[at, :], s_ref[at, :]
            for by in (1, 2, 4):
                keep = row < 8 - by if backward else row >= by
                shift = 8 - by if backward else by
                r_by = jnp.where(keep, pltpu.roll(r, shift, 0), 1.0)
                s_by = jnp.where(keep, pltpu.roll(s, shift, 0), 0.0)
                s = r * s_by + s
                r = r * r_by
            s = s + r * state
            r = r * decay
            c_ref[at, :] = r
            h_ref[at, :] = s
            end = 0 if backward else 7
            return r[end : end + 1, :], s[end : end + 1, :]

        one = jnp.ones((1, width), F32)
        decay, state = lax.fori_loop(0, tiles, step, (one, jnp.zeros((1, width), F32)))
        decay, state = lead_ref[0:1, :] * decay, lead_ref[0:1, :] * state
        for j in range(lines):
            mine[j : j + 1, :] = decay[:, 128 * j : 128 * (j + 1)]
            mine[lines + j : lines + j + 1, :] = state[:, 128 * j : 128 * (j + 1)]
        pl.semaphore_wait(pltpu.get_barrier_semaphore(), len(peers))
        jobs = Copies()
        here = tuple(lax.axis_index(a) for a in ORDER)
        for tag in grid_of(ORDER):
            if any(tag):
                peer = {a: peer_of(a, k) for a, k in zip(ORDER, tag)}
                jobs.push(mine, ends.at[here], send.at[tag], recv.at[tag], peer)
        jobs.keep(mine, ends.at[here], own)
        for tag in grid_of(ORDER):
            if any(tag):
                peer = {a: source_of(a, k) for a, k in zip(ORDER, tag)}
                jobs.arrive(ends.at[tuple(peer[a] for a in ORDER)], send.at[tag], recv.at[tag], peer)
        jobs.drain()
        me = (here[0] * sizes[1] + here[1]) * sizes[2] + here[2]
        entering = jnp.zeros((lines, 128), F32)
        for i in range(count):
            peer = count - 1 - i if backward else i
            t, rest = divmod(peer, sizes[1] * sizes[2])
            f, c = divmod(rest, sizes[2])
            pair = ends[t, f, c]
            ahead = jnp.where(peer > me if backward else peer < me, 1, 0)
            entering = jnp.where(ahead == 1, pair[:lines] * entering + pair[lines : 2 * lines], entering)
        entering = jnp.concatenate([entering[j : j + 1, :] for j in range(lines)], axis=1)
        in_ref[...] = jnp.broadcast_to(entering, (8, width))

        def fix(i, carry):
            at = tile(i)
            h_ref[at, :] = h_ref[at, :] + c_ref[at, :] * entering
            return carry

        lax.fori_loop(0, tiles, fix, 0)

    states, entering = pl.pallas_call(
        kernel,
        out_shape=(like((rows, width), F32), like((8, width), F32)),
        in_specs=[VMEM] * 3,
        out_specs=(VMEM, VMEM),
        scratch_shapes=[
            pltpu.VMEM((rows, width), F32),
            pltpu.VMEM(block, F32),
            pltpu.VMEM(sizes + block, F32),
            pltpu.SemaphoreType.DMA(sizes),
            pltpu.SemaphoreType.DMA(sizes),
            pltpu.SemaphoreType.DMA,
        ],
        compiler_params=pltpu.CompilerParams(collective_id=cid, has_side_effects=True),
        name="back_states" if backward else "states",
    )(retain, source, jnp.broadcast_to(lead, (8, width)))
    return states, entering[0]


def from_behind(x, axis, by):
    peers = lax.axis_size(axis)
    pairs = [(i, i + by) for i in range(peers) if 0 <= i + by < peers]
    return lax.ppermute(x, axis, pairs)


def gelu_tanh(values):
    return jax.nn.gelu(values, approximate=True)


def gates_of(decay_pre, input_pre, decay_param, conv_low, starts):
    rate_gate = jax.nn.sigmoid(decay_pre)
    in_gate = jax.nn.sigmoid(input_pre)
    log_decay = -8.0 * jax.nn.softplus(decay_param) * rate_gate
    retain = jnp.where(starts, 0.0, jnp.exp(log_decay))
    multiplier = jnp.where(
        starts, 1.0, jnp.sqrt(jnp.maximum(-jnp.expm1(2.0 * log_decay), SQRT_FLOOR))
    )
    return (retain, multiplier * in_gate * conv_low)


def normalize_back(gradient, values, inverse, scale_vec, cid, through=None):
    weighted = gradient * (1.0 + scale_vec)
    scale_grad = jnp.sum(gradient * values * inverse, axis=0)
    inner_sum, *passed = pair_sum([jnp.sum(weighted * values, axis=1, keepdims=True)], cid, through)
    return (inverse * weighted - values * inverse**3 * inner_sum / D, scale_grad, *passed)


def arrange(own, other):
    first = lax.axis_index("col") == 0
    return jnp.where(first, own, other), jnp.where(first, other, own)


def halves(x):
    width = x.shape[1] // 2
    return jnp.stack([x[:, :width], x[:, width:]])


def half_of(x):
    width = x.shape[1] // 2
    return jnp.where(lax.axis_index("col") == 0, x[:, :width], x[:, width:])


TOKEN_AXES = ("t", "row", "col")
WEIGHT_AXES = ("t", "f", "col")
PAIR = ("col",)


def fetch_first(mixer, branch, output, stream, scale, cotangent):
    t, f, c = shape_of(WEIGHT_AXES)
    width, inner = mixer.shape
    rows, half = cotangent.shape
    team, r, _ = shape_of(TOKEN_AXES)
    place = lanes_of(inner)
    axes = (WEIGHT_AXES,)
    plan = [
        (Gather, 0, 0, (axes, {"place": place}), Gather.scratch(WEIGHT_AXES)),
        (Fan, 3, 3, (("row",), {}), Fan.scratch("row")),
        (Gather, 1, 1, (axes, {"place": place}), Gather.scratch(WEIGHT_AXES)),
        (Gather, 2, 2, (axes, {"place": col_first}), Gather.scratch(WEIGHT_AXES)),
        (Gather, 4, 4, ((PAIR,), {}), Gather.scratch(PAIR)),
        (Gather, 5, 5, ((TOKEN_AXES,), {"place": lanes_of(half)}), Gather.scratch(TOKEN_AXES)),
    ]
    wide = like((t, f, width, 2 * inner), BF16)
    outs = [wide, wide, like((c, t, f) + output.shape, BF16), like((1, stream.shape[0], 2 * stream.shape[1]), BF16)]
    outs += [like((2, 1, scale.shape[0]), F32), like((team, r, rows, 2 * half), BF16)]
    mixer_t, branch_t, output_t, tokens, scale, every = exchange(
        0, lambda: along("t", "f") + across("row", "col"), plan,
        [mixer, branch, output, stream, scale[None], cotangent], outs, [ANY] * 4 + [VMEM, ANY],
    )
    return mixer_t.reshape(-1, 2 * inner), branch_t.reshape(-1, 2 * inner), output_t.reshape(-1, output.shape[1]), tokens[0], scale.reshape(-1), every.reshape(-1, 2 * half)


def fetch_second(normed, gate, up, down, gate_bias, up_bias):
    t, r, _ = shape_of(TOKEN_AXES)
    fleet = lax.axis_size("f")
    rows, width = normed.shape
    units, inner = gate.shape
    share = down.shape[1] // (2 * TEAM)
    piece = (down.shape[0], share)
    half = fleet // 2
    deal = Deal.scratch(piece, BF16)
    token, fan = Gather.scratch(TOKEN_AXES), Fan.scratch("f")
    place = lanes_of(width)
    step = next(n for n in (32, 16, 8, rows) if rows % n == 0)

    def kernel(n_ref, g_ref, u_ref, d_ref, gb, ub, n_all, gw, uw, d_all, g_out, u_out, h_out, held, sem, *rest):
        normed_job = Gather(n_ref, n_all, TOKEN_AXES, rest[:3], place)
        gate_job, up_job = Fan(g_ref, gw, "f", rest[3:6]), Fan(u_ref, uw, "f", rest[6:9])
        down_job = Deal(d_ref, d_all, rest[9:])
        greet(team_peers())
        for job in (normed_job, gate_job, up_job):
            job.begin()
        normed_job.stage(1)
        down_job.begin()
        normed_job.stage(2)
        normed_job.stage(3)
        normed_job.drain()
        for job in (gate_job, up_job):
            job.stage(1)
            job.drain()
        down_job.stage(1)
        blocks = t * r

        def fetch(i):
            return pltpu.make_async_copy(n_all.at[i // r, i % r], held.at[i % 2], sem.at[i % 2])

        fetch(0).start()

        def bend(i, carry):
            at = pl.ds(pl.multiple_of(i * step, step), step)
            v, u = g_out[at, :] + gb[...], u_out[at, :] + ub[...]
            bent = jnp.tanh(GELU * (v + 0.044715 * v * v * v))
            cdf = 0.5 * (1.0 + bent)
            slope = cdf + 0.5 * v * (1.0 - bent * bent) * (GELU * (1.0 + 3.0 * 0.044715 * v * v))
            h_out[at, :] = (v * cdf * u).astype(BF16)
            g_out[at, :] = u * slope
            u_out[at, :] = v * cdf
            return carry

        def product(i, carry):
            @pl.when(i + 1 < blocks)
            def _():
                fetch(i + 1).start()

            fetch(i).wait()
            at = pl.ds(pl.multiple_of(i * rows, rows), rows)
            for weight, out in ((gw, g_out), (uw, u_out)):
                for j in range(half):
                    out[at, j * units : (j + 1) * units] = dot_nt(held[i % 2], weight[j])
            lax.fori_loop(i * (rows // step), (i + 1) * (rows // step), bend, 0)
            return carry

        lax.fori_loop(0, blocks, product, 0)
        down_job.stage(2)
        down_job.drain()

    every = like((t, r, rows, 2 * width), BF16)
    weight = like((half, units, 2 * inner), BF16)
    first = like((t * r * rows, share), F32)
    n_all, gate_t, up_t, down_t, gate_slope, up_slope, hidden = pl.pallas_call(
        kernel,
        out_shape=(every, weight, weight, like((2, t, fleet) + piece, BF16), first, first, like(first.shape, BF16)),
        in_specs=[VMEM] * 6,
        out_specs=(ANY, VMEM, VMEM, ANY, VMEM, VMEM, VMEM),
        scratch_shapes=[pltpu.VMEM((2, rows, 2 * width), BF16), pltpu.SemaphoreType.DMA((2,))]
        + token + fan + fan + deal,
        compiler_params=pltpu.CompilerParams(collective_id=1, has_side_effects=True),
        name="fetch_second",
    )(normed, gate, up, down, gate_bias[None], up_bias[None])
    return (
        n_all.reshape(-1, 2 * width),
        gate_t.reshape(-1, 2 * inner),
        up_t.reshape(-1, 2 * inner),
        down_t.reshape(-1, share),
        gate_slope,
        up_slope,
        hidden,
    )


def diagonal(*axes):
    pairs = zip(across(*axes), [tag for tag in grid_of(axes) if any(tag)])
    return [peer for peer, tag in pairs if all(tag)]


def team_peers():
    return along("t", "row") + across("f", "col") + diagonal("t", "col")


def send_second(gate, up, hidden, gate_t, up_t, second_all, cot_all, late):
    t, r, _ = shape_of(TOKEN_AXES)
    fleet = lax.axis_size("f")
    tokens, wide = second_all.shape
    share = gate.shape[1]
    rows, width = tokens // (t * r), wide // 2
    half = fleet // 2
    units = share // half
    shard = width // (TEAM * fleet)
    block, weight, piece = (rows, width), (units, width), (shard, share)
    lane, tile = 512, wide // 4
    part, chunk = tile // shard, 256
    place = lanes_of(width)
    settle, fold = Settle.scratch(TOKEN_AXES, block, BF16), Fold.scratch("f", weight, BF16)
    undeal = Undeal.scratch(piece, BF16)

    def kernel(*refs):
        g_ref, u_ref, h_ref, gw_ref, uw_ref, all_ref, cot_ref, _ = refs[:8]
        delta_ref, grad_g, grad_u, grad_d = refs[8:12]
        src, fold_g, fold_u, down, gt_ref, ut_ref, ht_ref, tiles, tile_sem = refs[12:21]
        rest = refs[21:]
        sums = Settle(src, delta_ref, TOKEN_AXES, rest[: len(settle)], place)
        rest = rest[len(settle) :]
        g_job = Fold(fold_g, grad_g, "f", rest[: len(fold)])
        u_job = Fold(fold_u, grad_u, "f", rest[len(fold) : 2 * len(fold)])
        d_job = Undeal(down, grad_d, rest[2 * len(fold) :])

        def fetch(ref, i):
            at = pl.ds(pl.multiple_of(i * tile, tile), tile)
            return pltpu.make_async_copy(ref.at[:, at], tiles.at[i % 2], tile_sem.at[i % 2])

        def turn(src_ref, out_ref):
            def some(i, carry):
                at = pl.ds(pl.multiple_of(i * chunk, chunk), chunk)
                out_ref[:, at] = src_ref[at, :].T
                return carry

            lax.fori_loop(0, tokens // chunk, some, 0)

        def down_gradients(i, carry):
            @pl.when(i + 1 < wide // tile)
            def _():
                fetch(cot_ref, i + 1).start()

            @pl.when(i + 1 == wide // tile)
            def _():
                fetch(all_ref, 0).start()

            fetch(cot_ref, i).wait()
            value = dot_nn(ht_ref[...], tiles[i % 2]).T.astype(BF16)
            for j in range(part):
                n = i * part + j
                down[n % fleet, n // fleet % TEAM, n // (TEAM * fleet)] = value[j * shard : (j + 1) * shard]
            return carry

        def block_of(tag):
            coords = sums.coords(tag)
            at = pl.ds(pl.multiple_of((coords[0] * r + coords[1]) * rows, rows), rows)

            def product(j, carry):
                col = pl.ds(pl.multiple_of(j * lane, lane), lane)
                value = dot_nn(g_ref[at, :], gw_ref[:, col]) + dot_nn(u_ref[at, :], uw_ref[:, col])
                src[coords[0], coords[1], :, col] = value.astype(BF16)
                return carry

            lax.fori_loop(0, wide // lane, product, 0)
            for k in offsets("col"):
                sums.forward(tag + (k,), place(src, sums.coords(tag + (k,))))

        def gradients(i, carry):
            @pl.when(i + 1 < wide // tile)
            def _():
                fetch(all_ref, i + 1).start()

            fetch(all_ref, i).wait()
            h, at = i // (width // tile), pl.ds(pl.multiple_of(i % (width // tile) * tile, tile), tile)
            for left, out in ((gt_ref, fold_g), (ut_ref, fold_u)):
                value = dot_nn(left[...], tiles[i % 2]).astype(BF16)
                for j in range(half):
                    out[h, j, :, at] = value[j * units : (j + 1) * units]
            return carry

        def half_gradients(h):
            first = h * (width // tile)
            lax.fori_loop(first, first + width // tile, gradients, 0)
            g_job.begin((h,))
            u_job.begin((h,))

        away = [tag for tag in sums.order(2) if tag[-1]]
        home = [tag for tag in sums.order(2) if not tag[-1]]
        team = sums.order(1)
        fetch(cot_ref, 0).start()
        greet(team_peers())
        block_of(away[0])
        turn(h_ref, ht_ref)
        sums.step(2, away[0])
        lax.fori_loop(0, wide // tile, down_gradients, 0)
        d_job.begin()
        block_of(away[1])
        block_of(home[0])
        sums.step(2, away[1])
        block_of(away[2])
        sums.step(2, home[0])
        sums.step(1, team[0])
        turn(g_ref, gt_ref)
        turn(u_ref, ut_ref)
        half_gradients(0)
        sums.step(2, away[2])
        block_of(away[3])
        block_of(home[1])
        sums.step(2, away[3])
        block_of(home[2])
        sums.step(2, home[1])
        sums.step(1, team[1])
        half_gradients(1)
        d_job.stage(1)
        sums.step(2, home[2])
        block_of(home[3])
        sums.step(1, team[2])
        sums.step(2, home[3])
        sums.step(1, team[3])
        sums.stage(3)
        g_job.stage(1)
        u_job.stage(1)
        d_job.stage(2)
        for job in (sums, g_job, u_job, d_job):
            job.drain()

    delta, grad_gate, grad_up, grad_down = pl.pallas_call(
        kernel,
        out_shape=(like(block, F32), like(weight, BF16), like(weight, BF16), like((TEAM, 2) + piece, BF16)),
        in_specs=[VMEM] * 5 + [ANY] * 3,
        out_specs=(VMEM,) * 4,
        scratch_shapes=[
            pltpu.VMEM((t, r, rows, wide), BF16),
            pltpu.VMEM((2, half) + weight, BF16),
            pltpu.VMEM((2, half) + weight, BF16),
            pltpu.VMEM((fleet, TEAM, 2) + piece, BF16),
            pltpu.VMEM((share, tokens), BF16),
            pltpu.VMEM((share, tokens), BF16),
            pltpu.VMEM((share, tokens), BF16),
            pltpu.VMEM((2, tokens, tile), BF16),
            pltpu.SemaphoreType.DMA((2,)),
        ]
        + settle + fold + fold + undeal,
        compiler_params=pltpu.CompilerParams(
            collective_id=2, has_side_effects=True, vmem_limit_bytes=67_000_000
        ),
        name="send_second",
    )(gate, up, hidden, gate_t, up_t, second_all, cot_all, late)
    return delta, grad_gate, grad_up, grad_down


def to_stream(partial, cid):
    rows, width = partial.shape
    block = (rows, width // 2)
    (out,) = exchange(
        cid, lambda: across("row", "col"),
        [(Fold, 0, 0, (("row",), {}), Fold.scratch("row", block, BF16))],
        [halves(partial).reshape((2, 1) + block)], [like(block, F32)], [VMEM],
    )
    return out


class FanSwap(Fan):
    def __init__(self, src, out, sems, other):
        super().__init__(src, out, "row", sems[:3])
        self.send_on, self.recv_on = sems[3:]
        self.other = other

    @staticmethod
    def scratch():
        return Fan.scratch("row") + Swap.scratch()

    def stage(self, wave):
        super().stage(wave)
        other, width = 1 - lax.axis_index("col"), self.src.shape[-1]
        if wave == 1:
            src = self.out.at[0, :, pl.ds(pl.multiple_of(other * width, width), width)]
            self.push(src, self.other, self.send_on, self.recv_on, {"col": other})
        if wave == 2:
            self.arrive(self.other, self.send_on, self.recv_on, {"col": other})

    def drain(self):
        super().drain()
        Copies.drain(self)


def to_tokens(block, mixed, cid):
    rows, width = block.shape
    fan, gather = FanSwap.scratch(), Gather.scratch(PAIR)

    def kernel(block_ref, mixed_ref, out_ref, other_ref, both_ref, *sems):
        greet(across("row", "col"))
        jobs = [
            FanSwap(block_ref, out_ref, sems[: len(fan)], other_ref),
            Gather(mixed_ref, both_ref, PAIR, sems[len(fan) :]),
        ]
        run_jobs(jobs, ())

    out, other, both = pl.pallas_call(
        kernel,
        out_shape=(like((1, rows, 2 * width), BF16), like(block.shape, BF16), like((2,) + mixed.shape, BF16)),
        in_specs=[VMEM] * 2,
        out_specs=(VMEM,) * 3,
        scratch_shapes=fan + gather,
        compiler_params=pltpu.CompilerParams(collective_id=cid, has_side_effects=True),
        name="to_tokens",
    )(block, mixed)
    both_rows = jnp.concatenate(arrange(half_of(out[0]), other), axis=0)
    return out[0], both_rows, both.reshape(-1, mixed.shape[1])


def dealt(x, axes, dtype):
    sizes = shape_of(axes)
    members = sizes[0] * sizes[1] * sizes[2]
    width = -(-x.size // (members * 8 * 128)) * 128
    flat = jnp.pad(x.reshape(-1), (0, members * 8 * width - x.size))
    return flat.reshape(sizes + (8, width)).astype(dtype)


STREAM_AXES = ("t", "f", "row")


def finish_block(normed, branch, mixer, delta, cid):
    rows, width = delta.shape
    token = (rows, width // 2)
    plan = [
        (Fold, 0, 0, (("row",), {}), Fold.scratch("row", token, BF16)),
        (Swap, 1, 1, ((), {}), Swap.scratch()),
        (Gather, 2, 2, ((PAIR,), {}), Gather.scratch(PAIR)),
        (Gather, 3, 3, ((PAIR,), {}), Gather.scratch(PAIR)),
    ]
    outs = [like(token, F32), like(token, BF16), like((2,) + branch.shape, BF16), like((2,) + mixer.shape, BF16)]
    delta, other, branch, mixer = exchange(
        cid, lambda: across("row", "col"), plan,
        [halves(delta).reshape((2, 1) + token), halves(normed), branch, mixer], outs, [VMEM] * 4,
    )
    rows = jnp.concatenate(arrange(half_of(normed), other), axis=0)
    return delta, rows, branch.reshape(-1, branch.shape[2]), mixer.reshape(-1, mixer.shape[2])


def send_first(grads, inner_sums, head_grads, stream_sums, done, through, cid):
    sizes = shape_of(DP)
    n = len(grads)
    block = (grads[0].shape[0] // (sizes[0] * sizes[1]), grads[0].shape[1])
    axes_of = (ORDER, STREAM_AXES, ORDER)
    sums = (inner_sums, stream_sums, head_grads)
    lanes = head_grads.shape[-1]
    small = [dealt(x, axes, F32) for x, axes in zip(sums[:2], axes_of)]
    small.append(head_grads.reshape(shape_of(ORDER) + (-1, lanes)).astype(BF16))
    plan = [
        (AllReduce, n + i, n + i, ((axes,), {}), AllReduce.scratch(axes, x.shape[3:], x.dtype))
        for i, (x, axes) in enumerate(zip(small, axes_of))
    ]
    plan += [(Reduce, i, i, ((DP,), {}), Reduce.scratch(DP, block, BF16)) for i in range(n)]
    bulk = tuple(range(3, 3 + n))
    pieces = done[2].shape
    wide = [like(done[0].shape, F32), like(done[1].shape, F32), like((pieces[2], 2 * TEAM * pieces[3]), F32)]
    plan += [(cut, n + 3 + i, n + 3 + i, ((), {}), []) for i, cut in enumerate((Widen, Widen, Join))]
    rest = tuple(range(3 + n, 6 + n))
    got = exchange(
        cid, lambda: along("t", "f", "row", "col"), plan,
        [g.reshape(sizes + block) for g in grads] + small + list(done),
        [like(block, F32)] * n + [like(x.shape, x.dtype) for x in small] + wide, [VMEM] * (n + 6),
        order=(0, 1, 2) * 2 + bulk + (0, 1, 2) * 2 + rest * 2 + bulk * 2, through=through,
    )
    return got[:n], [x.reshape(-1)[: y.size].reshape(y.shape).astype(F32) for x, y in zip(got[n : n + 3], sums)], got[n + 3 : -1], got[-1]


def on_device(
    stream,
    scale_first,
    branch_weight,
    branch_bias,
    mixer_weight,
    mixer_bias,
    conv_weight,
    conv_bias,
    decay_weight,
    decay_bias,
    input_weight,
    input_bias,
    decay_param,
    output_weight,
    output_bias,
    scale_second,
    gate_weight,
    gate_bias,
    up_weight,
    up_bias,
    down_weight,
    down_bias,
    cotangent,
):
    mixer_t, branch_t, output_t, stream_all, scale_all, cot_all = fetch_first(
        mixer_weight.T, branch_weight.T, output_weight.T, stream, scale_first, cotangent
    )
    inner = mixer_t.shape[0]
    stream_wide = stream.astype(F32)
    tokens_wide = stream_all.astype(F32)
    inverse_all = lax.rsqrt(jnp.sum(tokens_wide * tokens_wide, axis=1, keepdims=True) / D + EPSILON)
    normed_first = (tokens_wide * inverse_all * (1.0 + scale_all)).astype(BF16)
    mixer_pre = dot_nt(normed_first, mixer_t) + mixer_bias
    branch_pre = dot_nt(normed_first, branch_t) + branch_bias
    branch_act, branch_back = jax.vjp(gelu_tanh, branch_pre)

    steps = mixer_pre.shape[0]
    first_token = lax.axis_index(ORDER) * steps
    position = (first_token + jnp.arange(steps, dtype=jnp.int32)) % LEN
    margin = CONV - 1
    left_edge = from_behind(mixer_pre[steps - margin :], ORDER, 1)
    padded = jnp.concatenate([left_edge, mixer_pre], axis=0)
    conv_out = conv_bias + jnp.zeros_like(mixer_pre)
    for offset in range(CONV):
        in_reach = (position >= offset)[:, None]
        conv_out = conv_out + jnp.where(
            in_reach, conv_weight[offset] * padded[margin - offset : margin - offset + steps], 0.0
        )
    conv_low = conv_out.astype(BF16)
    conv_wide = conv_low.astype(F32)
    heads, block = decay_weight.shape[0], decay_weight.shape[1]
    parts = [conv_low[:, h * block : (h + 1) * block] for h in range(heads)]
    decay_pre = jnp.concatenate([dot_nn(x, decay_weight[h]) for h, x in enumerate(parts)], 1) + decay_bias
    input_pre = jnp.concatenate([dot_nn(x, input_weight[h]) for h, x in enumerate(parts)], 1) + input_bias
    starts = (position == 0)[:, None]

    def gate_values(decay_in, input_in, param_in, conv_in):
        return gates_of(decay_in, input_in, param_in, conv_in, starts)

    (retain, source), gate_back = jax.vjp(gate_values, decay_pre, input_pre, decay_param, conv_wide)
    ones_row = jnp.ones((1, inner), F32)
    states, state_in = recurrence(retain, source, ones_row, False, 3)
    mixed_low = (states * branch_act).astype(BF16)
    first_out = stream_wide + to_stream(dot_nt(mixed_low, output_t).astype(BF16), 4) + output_bias
    second_total, first_total = pair_sum(
        [jnp.sum(x * x, axis=1, keepdims=True) for x in (first_out, stream_wide)], 5
    )
    inverse_second = lax.rsqrt(second_total / D + EPSILON)
    inverse_first = lax.rsqrt(first_total / D + EPSILON)
    normed_second = first_out * inverse_second * (1.0 + scale_second)

    share = down_weight.shape[0] // (2 * TEAM)
    mine = (lax.axis_index("t") * 2 + lax.axis_index("col")) * share
    gate_b = lax.dynamic_slice(gate_bias, (mine,), (share,))
    up_b = lax.dynamic_slice(up_bias, (mine,), (share,))

    second_all, gate_t, up_t, down_t, gate_slope, up_slope, hidden_low = fetch_second(
        normed_second.astype(BF16), gate_weight.T, up_weight.T, down_weight.T, gate_b, up_b
    )
    delta_hidden = dot_nn(cot_all, down_t)
    delta_gate, delta_up = delta_hidden * gate_slope, delta_hidden * up_slope
    gate_low, up_low = delta_gate.astype(BF16), delta_up.astype(BF16)
    down_part = dot_nt(hidden_low, down_t).astype(BF16)
    down_rows = lax.psum_scatter(down_part, "col", scatter_dimension=1, tiled=True)
    delta_second, grad_gate, grad_up, grad_down = send_second(
        gate_low, up_low, hidden_low, gate_t, up_t, second_all, cot_all, down_part
    )
    delta_result = cotangent.astype(F32)

    norm_second_part, grad_scale_second, down_rows = normalize_back(
        delta_second, first_out, inverse_second, scale_second, 6, down_rows
    )
    down_proj = lax.psum_scatter(down_rows, ("t", "row"), scatter_dimension=0, tiled=True)
    delta_first = delta_result + norm_second_part
    out_all, out_rows, mixed_rows = to_tokens(delta_first.astype(BF16), mixed_low, 7)
    output_part = dot_tn(out_rows, mixed_rows).astype(BF16)
    grad_output = lax.psum_scatter(output_part, DP, scatter_dimension=0, tiled=True)
    delta_mixed = dot_nn(out_all, output_t)
    delta_state = delta_mixed * branch_act
    (delta_branch,) = branch_back(delta_mixed * states)
    branch_low = delta_branch.astype(BF16)
    retain_next = jnp.concatenate([retain[1:], ones_row], axis=0)
    back_state, _ = recurrence(retain_next, delta_state, retain[:1], True, 8)
    state_prev = jnp.concatenate([state_in[None], states[:-1]], axis=0)
    delta_decay_pre, delta_input_pre, grad_decay_param, delta_conv = gate_back(
        (back_state * state_prev, back_state)
    )
    decay_low = delta_decay_pre.astype(BF16)
    input_low = delta_input_pre.astype(BF16)

    def split(x):
        return [x[:, h * block : (h + 1) * block] for h in range(heads)]

    grad_decay_weight = jnp.stack([dot_tn(a, b) for a, b in zip(parts, split(decay_low))])
    grad_input_weight = jnp.stack([dot_tn(a, b) for a, b in zip(parts, split(input_low))])
    delta_conv = delta_conv + jnp.concatenate(
        [dot_nt(a, decay_weight[h]) for h, a in enumerate(split(decay_low))], 1
    )
    delta_conv = delta_conv + jnp.concatenate(
        [dot_nt(a, input_weight[h]) for h, a in enumerate(split(input_low))], 1
    )
    delta_padded = jnp.zeros_like(padded)
    conv_grads = []
    for offset in range(CONV):
        in_reach = (position >= offset)[:, None]
        masked = jnp.where(in_reach, delta_conv, 0.0)
        conv_grads.append(
            jnp.sum(masked * padded[margin - offset : margin - offset + steps], axis=0)
        )
        delta_padded = delta_padded + jnp.pad(
            masked * conv_weight[offset], ((margin - offset, offset), (0, 0))
        )
    grad_conv_weight = jnp.stack(conv_grads, axis=0)
    right_edge = from_behind(delta_padded[:margin], ORDER, -1)
    delta_mixer = delta_padded[margin:] + jnp.pad(right_edge, ((steps - margin, 0), (0, 0)))
    mixer_low = delta_mixer.astype(BF16)

    def spread(x):
        return lax.dynamic_update_slice(jnp.zeros_like(gate_bias), x, (mine,))

    small = [
        jnp.sum(delta_branch, axis=0),
        jnp.sum(delta_mixer, axis=0),
        jnp.sum(delta_conv, axis=0),
        jnp.sum(delta_decay_pre, axis=0),
        jnp.sum(delta_input_pre, axis=0),
        grad_decay_param,
        spread(jnp.sum(delta_gate, axis=0)),
        spread(jnp.sum(delta_up, axis=0)),
        grad_conv_weight.reshape(-1),
    ]
    delta_normed_part = dot_nn(branch_low, branch_t) + dot_nn(mixer_low, mixer_t)
    delta_normed_first, first_rows, branch_rows, mixer_rows = finish_block(
        normed_first, branch_low, mixer_low, delta_normed_part.astype(BF16), 10
    )
    norm_first_part, grad_scale_first = normalize_back(
        delta_normed_first, stream_wide, inverse_first, scale_first, 12
    )
    (grad_mixer, grad_branch), (total, stream_sums, head_grads), wide_grads, down_proj = send_first(
        [dot_tn(mixer_rows, first_rows).astype(BF16), dot_tn(branch_rows, first_rows).astype(BF16)],
        jnp.concatenate(small),
        jnp.stack([grad_decay_weight, grad_input_weight]),
        jnp.stack(
            [grad_scale_second, jnp.sum(delta_first, axis=0), jnp.sum(delta_result, axis=0), grad_scale_first]
        ),
        (grad_gate, grad_up, grad_down),
        down_proj,
        13,
    )
    result = (first_out + down_proj.astype(F32) + down_bias).astype(BF16)
    grad_stream = delta_first + norm_first_part
    sums, at = [], 0
    for x in small:
        sums.append(total[at : at + x.shape[0]])
        at += x.shape[0]
    return (
        result,
        grad_stream,
        stream_sums[3],
        grad_branch.T,
        sums[0],
        grad_mixer.T,
        sums[1],
        sums[8].reshape(CONV, inner),
        sums[2],
        head_grads[0],
        sums[3],
        head_grads[1],
        sums[4],
        sums[5],
        grad_output.T.astype(F32),
        stream_sums[1],
        stream_sums[0],
        wide_grads[0].T,
        sums[6],
        wide_grads[1].T,
        sums[7],
        wide_grads[2].T,
        stream_sums[2],
    )


def solution(mesh):
    shape = mesh.devices.shape
    names = mesh.axis_names
    fleet = mesh.shape["dp"] // TEAM
    at = names.index("dp")
    split_mesh = Mesh(
        mesh.devices.reshape(shape[:at] + (TEAM, fleet) + shape[at + 1 :]),
        names[:at] + DP + names[at + 1 :],
    )
    tokens, fan_in = P((*DP, "row"), "col"), P("col", ("row", *DP))
    fan_out, inner, wide = P("row", ("col", *DP)), P("row"), P("col")
    heads = P("row", None, None)
    return jax.shard_map(
        on_device,
        mesh=split_mesh,
        in_specs=(
            tokens, wide, fan_in, inner, fan_in, inner, P(None, "row"), inner,
            heads, inner, heads, inner, inner, fan_out, wide, wide,
            fan_in, inner, fan_in, inner, fan_out, wide, tokens,
        ),
        out_specs=(
            tokens, tokens, wide, fan_in, inner, fan_in, inner, P(None, "row"), inner,
            heads, inner, heads, inner, inner, fan_out, wide, wide,
            fan_in, inner, fan_in, inner, fan_out, wide,
        ),
        check_vma=False,
    )
```

```python
import math

import jax
import jax.numpy as jnp
from jax import lax
from jax.experimental import pallas as pl
from jax.experimental.pallas import tpu as pltpu
from jax.sharding import Mesh, PartitionSpec as P


D = 2560
CONV = 4
LEN = 4096
EPSILON = 1e-06
SQRT_FLOOR = 0.0001
GELU = (2.0 / math.pi) ** 0.5
TEAM = 4
NT = (((1,), (1,)), ((), ()))
TN = (((0,), (0,)), ((), ()))
F32 = jnp.float32
BF16 = jnp.bfloat16
DP = ("t", "f")
ORDER = ("t", "f", "col")


def dot_nn(a, b):
    return jnp.dot(a, b, preferred_element_type=F32)


def dot_nt(a, b):
    return lax.dot_general(a, b, NT, preferred_element_type=F32)


def dot_tn(a, b):
    return lax.dot_general(a, b, TN, preferred_element_type=F32)


MESH = pl.DeviceIdType.MESH
ANY = pl.BlockSpec(memory_space=pl.ANY)
VMEM = pl.BlockSpec(memory_space=pltpu.VMEM)


def peer_of(axis, k):
    n, me = lax.axis_size(axis), lax.axis_index(axis)
    if k == 0:
        return me
    if n == 2:
        return 1 - me
    if n == 4:
        return (me + 1 - 2 * (me % 2), (me + 2) % 4, 3 - me)[k - 1]
    return (me + k) % n


def source_of(axis, k):
    n, me = lax.axis_size(axis), lax.axis_index(axis)
    return peer_of(axis, k) if n in (2, 4) else (me + n - k) % n


def offsets(axis):
    n = lax.axis_size(axis)
    return (1, 3, 2) if n == 4 else tuple(range(1, n))


def grid_of(axes, far_first=False):
    grid = [()]
    for axis in axes:
        near = (0,) + offsets(axis)
        grid = [tag + (k,) for tag in grid for k in (near[::-1] if far_first else near)]
    return grid


def hail(peers):
    for peer in peers:
        pl.semaphore_signal(pltpu.get_barrier_semaphore(), inc=1, device_id=peer, device_id_type=MESH)


def greet(peers):
    hail(peers)
    pl.semaphore_wait(pltpu.get_barrier_semaphore(), len(peers))


def only(condition, act):
    if condition is None:
        act()
    else:
        pl.when(condition)(act)


def along(*axes):
    return [{axis: peer_of(axis, k)} for axis in axes for k in offsets(axis)]


def across(*axes):
    return [
        {axis: peer_of(axis, k) for axis, k in zip(axes, tag)} for tag in grid_of(axes) if any(tag)
    ]


class Copies:
    def __init__(self):
        self.sent = []

    def push(self, src, dst, send, recv, peer, condition=None):
        copy = pltpu.make_async_remote_copy(
            src_ref=src, dst_ref=dst, send_sem=send, recv_sem=recv, device_id=peer, device_id_type=MESH
        )
        only(condition, copy.start)
        self.sent.append((condition, copy.wait_send))

    def arrive(self, dst, send, recv, peer):
        pltpu.make_async_remote_copy(
            src_ref=dst, dst_ref=dst, send_sem=send, recv_sem=recv, device_id=peer, device_id_type=MESH
        ).wait_recv()

    def keep(self, src, dst, sem):
        copy = pltpu.make_async_copy(src, dst, sem)
        copy.start()
        self.sent.append((None, copy.wait))

    def drain(self):
        for condition, wait in self.sent:
            only(condition, wait)


def leading(ref, coords):
    return ref.at[tuple(coords)]


class Gather(Copies):
    def __init__(self, src, out, axes, sems, place=leading):
        super().__init__()
        self.src, self.out, self.axes, self.place = src, out, axes, place
        self.send, self.recv, self.own = sems
        self.size, self.at = lax.axis_size(axes[0]), lax.axis_index(axes[0])
        self.nobody = (0,) * len(axes)
        self.waves = {}
        line = [0] + [v for far in range(1, self.size) for v in (-far, far)]
        for v in line:
            for rest in grid_of(axes[1:]):
                tag = (v,) + rest
                if any(tag):
                    self.waves.setdefault(sum(1 for k in tag if k), []).append(tag)

    @staticmethod
    def scratch(axes):
        sizes = [lax.axis_size(a) for a in axes]
        shape = (2 * sizes[0] - 1,) + tuple(sizes[1:])
        return [pltpu.SemaphoreType.DMA(shape), pltpu.SemaphoreType.DMA(shape), pltpu.SemaphoreType.DMA]

    def index(self, tag):
        return (tag[0] + self.size - 1,) + tag[1:]

    def exists(self, far):
        if far == 0:
            return None
        return self.at + far >= 0 if far < 0 else self.at + far < self.size

    def slot(self, tag):
        rest = [source_of(a, k) for a, k in zip(self.axes[1:], tag[1:])]
        return self.place(self.out, [self.at + tag[0]] + rest)

    def spread(self, tag):
        last = max([i for i, k in enumerate(tag) if k], default=-1)
        here = self.exists(tag[0])
        src = self.slot(tag) if any(tag) else self.src

        def send(there, peer, condition):
            if here is not None and condition is not None:
                condition = here & condition
            elif condition is None:
                condition = here
            at = self.index(there)
            self.push(src, self.slot(tag), self.send.at[at], self.recv.at[at], peer, condition)

        if last <= 0:
            if 0 <= tag[0] < self.size - 1:
                send((tag[0] + 1,) + tag[1:], {self.axes[0]: self.at - 1}, self.at > 0)
            if -self.size + 1 < tag[0] <= 0:
                send((tag[0] - 1,) + tag[1:], {self.axes[0]: self.at + 1}, self.at < self.size - 1)
        for level in range(max(last, 0) + 1, len(self.axes)):
            axis = self.axes[level]
            for k in offsets(axis):
                send(tag[:level] + (k,) + tag[level + 1 :], {axis: peer_of(axis, k)}, None)

    def begin(self):
        self.spread(self.nobody)
        self.keep(self.src, self.slot(self.nobody), self.own)

    def stage(self, wave):
        for tag in self.waves.get(wave, ()):
            last = max(i for i, k in enumerate(tag) if k)
            if last:
                peer = {self.axes[last]: peer_of(self.axes[last], tag[last])}
            else:
                peer = {self.axes[0]: self.at + (1 if tag[0] > 0 else -1)}
            at = self.index(tag)
            only(
                self.exists(tag[0]),
                lambda: self.arrive(self.slot(tag), self.send.at[at], self.recv.at[at], peer),
            )
            self.spread(tag)


def sum_into(out, parts):
    rows = out.shape[0]
    step = next(n for n in (32, 16, 8, rows) if rows % n == 0)

    def some(i, carry):
        at = pl.ds(pl.multiple_of(i * step, step), step)
        total = parts[0][at, :].astype(F32)
        for part in parts[1:]:
            total = total + part[at, :].astype(F32)
        out[at, :] = total.astype(out.dtype)
        return carry

    lax.fori_loop(0, rows // step, some, 0)


class Reduce(Copies):
    def __init__(self, src, out, axes, scratch, place=leading):
        super().__init__()
        n = len(axes)
        self.src, self.out, self.axes, self.place = src, out, axes, place
        self.part = {i + 1: scratch[i] for i in range(n - 1)}
        rest = scratch[n - 1 :]
        self.come = rest[:n]
        self.send = rest[n : 2 * n]
        self.recv = rest[2 * n : 3 * n]

    @staticmethod
    def count(axes):
        return 4 * len(axes) - 1

    @staticmethod
    def scratch(axes, block, dtype):
        sizes = tuple(lax.axis_size(a) for a in axes)
        n = len(axes)
        parts = [pltpu.VMEM(sizes[:i] + block, dtype) for i in range(1, n)]
        come = [pltpu.VMEM((sizes[i] - 1,) + sizes[:i] + block, dtype) for i in range(n)]
        sems = [pltpu.SemaphoreType.DMA((sizes[i] - 1,) + sizes[:i]) for i in range(n)]
        return parts + come + sems + sems

    def coords(self, tag):
        return tuple(peer_of(a, k) for a, k in zip(self.axes, tag))

    def forward(self, tag, src):
        level = len(tag) - 1
        k, prefix = tag[-1], tag[:-1]
        axis = self.axes[level]
        self.push(
            src,
            self.come[level].at[(k - 1,) + self.coords(prefix)],
            self.send[level].at[(k - 1,) + prefix],
            self.recv[level].at[(k - 1,) + prefix],
            {axis: peer_of(axis, k)},
        )

    def order(self, level):
        return sorted(grid_of(self.axes[:level], True), key=lambda tag: tag[-1:] == (0,))

    def begin(self):
        for tag in self.order(len(self.axes)):
            if tag[-1]:
                self.forward(tag, self.place(self.src, self.coords(tag)))

    def held(self, level, coords):
        return self.place(self.src, coords) if level == len(self.axes) else self.part[level].at[coords]

    def step(self, level, tag):
        axis = self.axes[level]
        here = self.coords(tag)
        parts = [self.held(level + 1, here + (lax.axis_index(axis),))]
        for k in offsets(axis):
            slot = self.come[level].at[(k - 1,) + here]
            at = (k - 1,) + tag
            self.arrive(slot, self.send[level].at[at], self.recv[level].at[at], {axis: source_of(axis, k)})
            parts.append(slot)
        target = self.held(level, here) if level else self.out
        sum_into(target, parts)
        if level and tag[-1]:
            self.forward(tag, target)

    def stage(self, wave):
        level = len(self.axes) - wave
        if level >= 0:
            for tag in self.order(level):
                self.step(level, tag)


class Settle(Reduce):
    def __init__(self, src, out, axes, scratch, place):
        Copies.__init__(self)
        n = len(axes)
        self.src, self.out, self.axes, self.place = src, out, axes, place
        self.come, self.send, self.recv = scratch[:n], scratch[n : 2 * n], scratch[2 * n :]

    @staticmethod
    def scratch(axes, block, dtype):
        return Reduce.scratch(axes, block, dtype)[len(axes) - 1 :]

    def held(self, level, coords):
        return self.place(self.src, coords + tuple(lax.axis_index(a) for a in self.axes[level:]))


class Spread(Copies):
    def __init__(self, src, out, axes, sems):
        super().__init__()
        self.src, self.out, self.axes = src, out, axes
        self.send, self.recv, self.own = sems
        self.waves = {}
        for tag in grid_of(axes):
            if any(tag):
                self.waves.setdefault(sum(1 for k in tag if k), []).append(tag)

    @staticmethod
    def scratch(axes):
        shape = shape_of(axes)
        return [pltpu.SemaphoreType.DMA(shape), pltpu.SemaphoreType.DMA(shape), pltpu.SemaphoreType.DMA]

    def slot(self, tag):
        return self.out.at[tuple(source_of(a, k) for a, k in zip(self.axes, tag))]

    def spread(self, tag):
        last = max([i for i, k in enumerate(tag) if k], default=-1)
        for level in range(last + 1, len(self.axes)):
            axis = self.axes[level]
            for k in offsets(axis):
                at = tag[:level] + (k,) + tag[level + 1 :]
                src = self.slot(tag) if any(tag) else self.src
                self.push(src, self.slot(tag), self.send.at[at], self.recv.at[at], {axis: peer_of(axis, k)})

    def begin(self):
        nobody = (0,) * len(self.axes)
        self.spread(nobody)
        self.keep(self.src, self.slot(nobody), self.own)

    def stage(self, wave):
        for tag in self.waves.get(wave, ()):
            last = max(i for i, k in enumerate(tag) if k)
            peer = {self.axes[last]: peer_of(self.axes[last], tag[last])}
            self.arrive(self.slot(tag), self.send.at[tag], self.recv.at[tag], peer)
            self.spread(tag)


class Widen(Copies):
    def __init__(self, src, out, scratch):
        super().__init__()
        self.src, self.out = src, out

    def begin(self):
        pass

    def stage(self, wave):
        if wave == 1:
            sum_into(self.out, [self.src])


class Join(Widen):
    def stage(self, wave):
        if wave == 1:
            share = self.src.shape[-1]
            for i in range(2 * TEAM):
                self.out[:, i * share : (i + 1) * share] = self.src[i // 2, i % 2].astype(self.out.dtype)


class Fan(Copies):
    def __init__(self, src, out, axis, sems):
        super().__init__()
        self.src, self.out, self.axis = src, out, axis
        self.send, self.recv, self.own = sems
        self.half = lax.axis_size(axis) // 2

    @staticmethod
    def scratch(axis):
        n = lax.axis_size(axis)
        return [pltpu.SemaphoreType.DMA((n,)), pltpu.SemaphoreType.DMA((n, 2)), pltpu.SemaphoreType.DMA]

    def slot(self, owner, core):
        width = self.src.shape[-1]
        return self.out.at[owner % self.half, :, pl.ds(pl.multiple_of(core * width, width), width)]

    def begin(self):
        me, core = lax.axis_index(self.axis), lax.axis_index("col")
        target = me // self.half
        slot = self.slot(me, core)
        self.copies = []
        for k in offsets(self.axis):
            peer = {self.axis: peer_of(self.axis, k), "col": target}
            for c in (0, 1):

                @pl.when(core == c)
                def _(c=c):
                    pltpu.make_async_remote_copy(
                        src_ref=self.src, dst_ref=slot, send_sem=self.send.at[k], recv_sem=self.recv.at[k, c],
                        device_id=peer, device_id_type=MESH,
                    ).start()

        @pl.when(target == core)
        def _():
            pltpu.make_async_copy(self.src, slot, self.own).start()

        for c in (0, 1):

            @pl.when((target != core) & (core == c))
            def _(c=c):
                pltpu.make_async_remote_copy(
                    src_ref=self.src, dst_ref=slot, send_sem=self.send.at[0], recv_sem=self.recv.at[0, c],
                    device_id={"col": 1 - core}, device_id_type=MESH,
                ).start()

    def stage(self, wave):
        if wave != 1:
            return
        me, core = lax.axis_index(self.axis), lax.axis_index("col")
        for k in (0,) + offsets(self.axis):
            owner = source_of(self.axis, k)
            for c in (0, 1):
                expected = owner // self.half == core
                if k == 0:
                    expected = expected & (core != c)

                @pl.when(expected)
                def _(k=k, c=c, owner=owner):
                    slot = self.slot(owner, c)
                    self.arrive(slot, self.send.at[k], self.recv.at[k, c], {self.axis: owner, "col": c} if k else {"col": 1 - core})

    def drain(self):
        me, core = lax.axis_index(self.axis), lax.axis_index("col")
        target = me // self.half
        slot = self.slot(me, core)

        def left(k, peer):
            pltpu.make_async_remote_copy(
                src_ref=self.src, dst_ref=slot, send_sem=self.send.at[k], recv_sem=self.recv.at[k, 0],
                device_id=peer, device_id_type=MESH,
            ).wait_send()

        for k in offsets(self.axis):
            left(k, {self.axis: peer_of(self.axis, k), "col": target})

        @pl.when(target == core)
        def _():
            pltpu.make_async_copy(self.src, slot, self.own).wait()

        @pl.when(target != core)
        def _():
            left(0, {"col": 1 - core})


class Fold(Copies):
    def __init__(self, src, out, axis, scratch):
        super().__init__()
        self.src, self.out, self.axis = src, out, axis
        self.come, self.send, self.recv, self.own = scratch
        self.half = lax.axis_size(axis) // 2

    @staticmethod
    def scratch(axis, block, dtype):
        n = lax.axis_size(axis)
        return [
            pltpu.VMEM((n,) + block, dtype),
            pltpu.SemaphoreType.DMA((n, 2)),
            pltpu.SemaphoreType.DMA((n,)),
            pltpu.SemaphoreType.DMA,
        ]

    def each(self, visit, cores=(0, 1)):
        me, core = lax.axis_index(self.axis), lax.axis_index("col")
        for k in offsets(self.axis) + (0,):
            owner = peer_of(self.axis, k)
            for c in cores:

                @pl.when(owner // self.half == core)
                def _(k=k, c=c, owner=owner):
                    piece = self.src.at[c, owner % self.half]
                    if k:
                        visit(k, c, piece, {self.axis: owner, "col": c})
                    else:

                        @pl.when(core == c)
                        def _():
                            visit(k, None, piece, None)

                        @pl.when(core != c)
                        def _():
                            visit(k, c, piece, {"col": 1 - core})

    def begin(self, cores=(0, 1)):
        def start(k, c, piece, peer):
            if peer is None:
                pltpu.make_async_copy(piece, self.come.at[k], self.own).start()
            else:
                pltpu.make_async_remote_copy(
                    src_ref=piece, dst_ref=self.come.at[k], send_sem=self.send.at[k, c], recv_sem=self.recv.at[k],
                    device_id=peer, device_id_type=MESH,
                ).start()

        self.each(start, cores)

    def stage(self, wave):
        if wave != 1:
            return
        me, core = lax.axis_index(self.axis), lax.axis_index("col")
        holder = me // self.half
        for k in offsets(self.axis):
            peer = {self.axis: source_of(self.axis, k), "col": holder}
            self.arrive(self.come.at[k], self.send.at[k, 0], self.recv.at[k], peer)

        @pl.when(holder != core)
        def _():
            self.arrive(self.come.at[0], self.send.at[0, 0], self.recv.at[0], {"col": 1 - core})

        @pl.when(holder == core)
        def _():
            pltpu.make_async_copy(self.src.at[0, 0], self.come.at[0], self.own).wait()

        sum_into(self.out, [self.come.at[k] for k in (0,) + offsets(self.axis)])

    def drain(self):
        def left(k, c, piece, peer):
            if peer is not None:
                pltpu.make_async_remote_copy(
                    src_ref=piece, dst_ref=self.come.at[k], send_sem=self.send.at[k, c], recv_sem=self.recv.at[k],
                    device_id=peer, device_id_type=MESH,
                ).wait_send()

        self.each(left)


class Deal(Copies):
    def __init__(self, src, out, scratch):
        super().__init__()
        self.src, self.out = src, out
        self.cut, self.send, self.recv, self.own = scratch

    @staticmethod
    def scratch(piece, dtype):
        shape = shape_of(("t", "col"))
        sems = pltpu.SemaphoreType.DMA(shape + (lax.axis_size("f"),))
        return [pltpu.VMEM(shape + piece, dtype), sems, sems, pltpu.SemaphoreType.DMA]

    def onward(self, tag):
        t, c = source_of("t", tag[0]), source_of("col", tag[1])
        slot = self.out.at[c, t, lax.axis_index("f")]
        src = slot if any(tag) else self.cut.at[t, c]
        for k in offsets("f"):
            at = tag + (k,)
            self.push(src, slot, self.send.at[at], self.recv.at[at], {"f": peer_of("f", k)})

    def begin(self):
        share = self.cut.shape[-1]
        for i in range(2 * TEAM):
            self.cut[i // 2, i % 2] = self.src[:, i * share : (i + 1) * share]
        t, c, f = (lax.axis_index(a) for a in ("t", "col", "f"))
        for tag in grid_of(("t", "col")):
            to = peer_of("t", tag[0]), peer_of("col", tag[1])
            if any(tag):
                peer, at = {"t": to[0], "col": to[1]}, tag + (0,)
                self.push(self.cut.at[to], self.out.at[c, t, f], self.send.at[at], self.recv.at[at], peer)
        self.onward((0, 0))
        self.keep(self.cut.at[t, c], self.out.at[c, t, f], self.own)

    def stage(self, wave):
        f = lax.axis_index("f")
        for tag in grid_of(("t", "col")):
            t, c = source_of("t", tag[0]), source_of("col", tag[1])
            if wave == 1 and any(tag):
                at = tag + (0,)
                slot = self.out.at[c, t, f]
                self.arrive(slot, self.send.at[at], self.recv.at[at], {"t": t, "col": c})
                self.onward(tag)
            if wave == 2:
                for k in offsets("f"):
                    at = tag + (k,)
                    slot = self.out.at[c, t, source_of("f", k)]
                    self.arrive(slot, self.send.at[at], self.recv.at[at], {"f": source_of("f", k)})


class Undeal(Copies):
    def __init__(self, src, out, scratch):
        super().__init__()
        self.src, self.out = src, out
        self.come, self.part, self.send, self.recv, self.send_on, self.recv_on, self.own = scratch

    @staticmethod
    def scratch(block, dtype):
        f, t, c = (lax.axis_size(a) for a in ("f", "t", "col"))
        first, second = pltpu.SemaphoreType.DMA((f - 1, t, c)), pltpu.SemaphoreType.DMA((t, c))
        return [
            pltpu.VMEM((f - 1, t, c) + block, dtype),
            pltpu.VMEM((t, c) + block, dtype),
            first, first, second, second, pltpu.SemaphoreType.DMA,
        ]

    def begin(self, core=None):
        for tag in grid_of(("t", "col"), True):
            to = peer_of("t", tag[0]), peer_of("col", tag[1])
            condition = None if core is None else to[1] == core
            for k in offsets("f"):
                at = (k - 1,) + tag
                self.push(
                    self.src.at[(peer_of("f", k),) + to], self.come.at[(k - 1,) + to],
                    self.send.at[at], self.recv.at[at], {"f": peer_of("f", k)}, condition,
                )

    def stage(self, wave):
        t, c, f = (lax.axis_index(a) for a in ("t", "col", "f"))
        if wave == 1:
            for tag in grid_of(("t", "col"), True):
                to = peer_of("t", tag[0]), peer_of("col", tag[1])
                parts = [self.src.at[(f,) + to]]
                for k in offsets("f"):
                    at = (k - 1,) + tag
                    slot = self.come.at[(k - 1,) + to]
                    self.arrive(slot, self.send.at[at], self.recv.at[at], {"f": source_of("f", k)})
                    parts.append(slot)
                sum_into(self.part.at[to], parts)
                if any(tag):
                    self.push(
                        self.part.at[to], self.out.at[t, c], self.send_on.at[tag], self.recv_on.at[tag],
                        {"t": to[0], "col": to[1]},
                    )
                else:
                    self.keep(self.part.at[to], self.out.at[t, c], self.own)
        if wave == 2:
            for tag in grid_of(("t", "col")):
                if any(tag):
                    peer = source_of("t", tag[0]), source_of("col", tag[1])
                    self.arrive(
                        self.out.at[peer], self.send_on.at[tag], self.recv_on.at[tag], {"t": peer[0], "col": peer[1]}
                    )


def run_jobs(jobs, order):
    done = [-1] * len(jobs)
    for i in tuple(order) + tuple(range(len(jobs))) * 7:
        done[i] += 1
        if done[i]:
            jobs[i].stage(done[i])
        else:
            jobs[i].begin()
    for job in jobs:
        job.drain()


def exchange(cid, peers, plan, operands, out_shapes, out_spaces, order=(), through=None):
    n_in, n_out = len(operands), len(out_shapes)
    in_specs, aliases = [VMEM] * n_in, {}
    if through is not None:
        aliases[n_in] = n_out
        operands, in_specs = list(operands) + [through], in_specs + [ANY]
        out_shapes, out_spaces = list(out_shapes) + [like(through.shape, through.dtype)], list(out_spaces) + [ANY]
    scratch = [s for job in plan for s in job[4]]

    def kernel(*refs):
        n_op, n_res = len(in_specs), len(out_shapes)
        ins, outs, rest = refs[:n_in], refs[n_op : n_op + n_out], refs[n_op + n_res :]
        greet(peers())
        jobs = []
        for make, src, out, options, own in plan:
            mine, rest = rest[: len(own)], rest[len(own) :]
            jobs.append(make(ins[src], outs[out], *options[0], mine, **options[1]))
        run_jobs(jobs, order)

    return pl.pallas_call(
        kernel,
        out_shape=tuple(out_shapes),
        in_specs=in_specs,
        out_specs=tuple(out_spaces),
        scratch_shapes=scratch,
        input_output_aliases=aliases,
        compiler_params=pltpu.CompilerParams(collective_id=cid, has_side_effects=True),
    )(*operands)


class Swap(Copies):
    def __init__(self, src, out, sems):
        super().__init__()
        self.src, self.out = src, out
        self.send, self.recv = sems

    @staticmethod
    def scratch():
        return [pltpu.SemaphoreType.DMA, pltpu.SemaphoreType.DMA]

    def begin(self):
        other = 1 - lax.axis_index("col")
        self.push(self.src.at[other], self.out, self.send, self.recv, {"col": other})

    def stage(self, wave):
        if wave == 1:
            self.arrive(self.out, self.send, self.recv, {"col": 1 - lax.axis_index("col")})


class AllReduce(Copies):
    def __init__(self, src, out, axes, scratch):
        super().__init__()
        n = Reduce.count(axes)
        self.depth = len(axes)
        self.reduce = Reduce(src, scratch[n], axes, scratch[:n])
        self.gather = Spread(scratch[n], out, axes, scratch[n + 1 :])

    @staticmethod
    def scratch(axes, block, dtype):
        return Reduce.scratch(axes, block, dtype) + [pltpu.VMEM(block, dtype)] + Spread.scratch(axes)

    def begin(self):
        self.reduce.begin()

    def stage(self, wave):
        if wave <= self.depth:
            self.reduce.stage(wave)
        if wave == self.depth:
            self.gather.begin()
        if wave > self.depth:
            self.gather.stage(wave - self.depth)

    def drain(self):
        self.reduce.drain()
        self.gather.drain()


def shape_of(axes):
    return tuple(lax.axis_size(a) for a in axes)


def lanes_of(width):
    def place(ref, coords):
        return ref.at[tuple(coords[:-1]) + (slice(None), pl.ds(pl.multiple_of(coords[-1] * width, width), width))]

    return place


def col_first(ref, coords):
    return ref.at[(coords[-1],) + tuple(coords[:-1])]


def like(shape, dtype):
    return jax.ShapeDtypeStruct(shape, dtype)


def pair_sum(values, cid, through=None):
    share = 128 // len(values)
    wide = jnp.concatenate([jnp.broadcast_to(v, (v.shape[0], share)) for v in values], axis=1)
    both, *passed = exchange(
        cid, lambda: along("col"),
        [(Gather, 0, 0, ((PAIR,), {}), Gather.scratch(PAIR))],
        [wide], [like((2,) + wide.shape, F32)], [VMEM], through=through,
    )
    total = both[0] + both[1]
    return [total[:, i * share : i * share + 1] for i in range(len(values))] + passed


def recurrence(retain, source, lead, backward, cid):
    rows, width = retain.shape
    tiles = rows // 8
    sizes = shape_of(ORDER)
    count = sizes[0] * sizes[1] * sizes[2]
    lines = width // 128
    block = (-(-2 * lines // 8) * 8, 128)

    def kernel(r_ref, s_ref, lead_ref, h_ref, in_ref, c_ref, mine, ends, send, recv, own):
        peers = across(*ORDER)
        hail(peers)
        row = lax.broadcasted_iota(jnp.int32, (8, width), 0)

        def tile(i):
            return pl.ds(pl.multiple_of(8 * (tiles - 1 - i if backward else i), 8), 8)

        def step(i, carry):
            decay, state = carry
            at = tile(i)
            r, s = r_ref[at, :], s_ref[at, :]
            for by in (1, 2, 4):
                keep = row < 8 - by if backward else row >= by
                shift = 8 - by if backward else by
                r_by = jnp.where(keep, pltpu.roll(r, shift, 0), 1.0)
                s_by = jnp.where(keep, pltpu.roll(s, shift, 0), 0.0)
                s = r * s_by + s
                r = r * r_by
            s = s + r * state
            r = r * decay
            c_ref[at, :] = r
            h_ref[at, :] = s
            end = 0 if backward else 7
            return r[end : end + 1, :], s[end : end + 1, :]

        one = jnp.ones((1, width), F32)
        decay, state = lax.fori_loop(0, tiles, step, (one, jnp.zeros((1, width), F32)))
        decay, state = lead_ref[0:1, :] * decay, lead_ref[0:1, :] * state
        for j in range(lines):
            mine[j : j + 1, :] = decay[:, 128 * j : 128 * (j + 1)]
            mine[lines + j : lines + j + 1, :] = state[:, 128 * j : 128 * (j + 1)]
        pl.semaphore_wait(pltpu.get_barrier_semaphore(), len(peers))
        jobs = Copies()
        here = tuple(lax.axis_index(a) for a in ORDER)
        for tag in grid_of(ORDER):
            if any(tag):
                peer = {a: peer_of(a, k) for a, k in zip(ORDER, tag)}
                jobs.push(mine, ends.at[here], send.at[tag], recv.at[tag], peer)
        jobs.keep(mine, ends.at[here], own)
        for tag in grid_of(ORDER):
            if any(tag):
                peer = {a: source_of(a, k) for a, k in zip(ORDER, tag)}
                jobs.arrive(ends.at[tuple(peer[a] for a in ORDER)], send.at[tag], recv.at[tag], peer)
        jobs.drain()
        me = (here[0] * sizes[1] + here[1]) * sizes[2] + here[2]
        entering = jnp.zeros((lines, 128), F32)
        for i in range(count):
            peer = count - 1 - i if backward else i
            t, rest = divmod(peer, sizes[1] * sizes[2])
            f, c = divmod(rest, sizes[2])
            pair = ends[t, f, c]
            ahead = jnp.where(peer > me if backward else peer < me, 1, 0)
            entering = jnp.where(ahead == 1, pair[:lines] * entering + pair[lines : 2 * lines], entering)
        entering = jnp.concatenate([entering[j : j + 1, :] for j in range(lines)], axis=1)
        in_ref[...] = jnp.broadcast_to(entering, (8, width))

        def fix(i, carry):
            at = tile(i)
            h_ref[at, :] = h_ref[at, :] + c_ref[at, :] * entering
            return carry

        lax.fori_loop(0, tiles, fix, 0)

    states, entering = pl.pallas_call(
        kernel,
        out_shape=(like((rows, width), F32), like((8, width), F32)),
        in_specs=[VMEM] * 3,
        out_specs=(VMEM, VMEM),
        scratch_shapes=[
            pltpu.VMEM((rows, width), F32),
            pltpu.VMEM(block, F32),
            pltpu.VMEM(sizes + block, F32),
            pltpu.SemaphoreType.DMA(sizes),
            pltpu.SemaphoreType.DMA(sizes),
            pltpu.SemaphoreType.DMA,
        ],
        compiler_params=pltpu.CompilerParams(collective_id=cid, has_side_effects=True),
        name="back_states" if backward else "states",
    )(retain, source, jnp.broadcast_to(lead, (8, width)))
    return states, entering[0]


def from_behind(x, axis, by):
    peers = lax.axis_size(axis)
    pairs = [(i, i + by) for i in range(peers) if 0 <= i + by < peers]
    return lax.ppermute(x, axis, pairs)


def gelu_tanh(values):
    return jax.nn.gelu(values, approximate=True)


def gates_of(decay_pre, input_pre, decay_param, conv_low, starts):
    rate_gate = jax.nn.sigmoid(decay_pre)
    in_gate = jax.nn.sigmoid(input_pre)
    log_decay = -8.0 * jax.nn.softplus(decay_param) * rate_gate
    retain = jnp.where(starts, 0.0, jnp.exp(log_decay))
    multiplier = jnp.where(
        starts, 1.0, jnp.sqrt(jnp.maximum(-jnp.expm1(2.0 * log_decay), SQRT_FLOOR))
    )
    return (retain, multiplier * in_gate * conv_low)


def normalize_back(gradient, values, inverse, scale_vec, cid, through=None):
    weighted = gradient * (1.0 + scale_vec)
    scale_grad = jnp.sum(gradient * values * inverse, axis=0)
    inner_sum, *passed = pair_sum([jnp.sum(weighted * values, axis=1, keepdims=True)], cid, through)
    return (inverse * weighted - values * inverse**3 * inner_sum / D, scale_grad, *passed)


def arrange(own, other):
    first = lax.axis_index("col") == 0
    return jnp.where(first, own, other), jnp.where(first, other, own)


def halves(x):
    width = x.shape[1] // 2
    return jnp.stack([x[:, :width], x[:, width:]])


def half_of(x):
    width = x.shape[1] // 2
    return jnp.where(lax.axis_index("col") == 0, x[:, :width], x[:, width:])


TOKEN_AXES = ("t", "row", "col")
WEIGHT_AXES = ("t", "f", "col")
PAIR = ("col",)


def fetch_first(mixer, branch, output, stream, scale, cotangent):
    t, f, c = shape_of(WEIGHT_AXES)
    width, inner = mixer.shape
    rows, half = cotangent.shape
    team, r, _ = shape_of(TOKEN_AXES)
    place = lanes_of(inner)
    axes = (WEIGHT_AXES,)
    plan = [
        (Gather, 0, 0, (axes, {"place": place}), Gather.scratch(WEIGHT_AXES)),
        (Fan, 3, 3, (("row",), {}), Fan.scratch("row")),
        (Gather, 1, 1, (axes, {"place": place}), Gather.scratch(WEIGHT_AXES)),
        (Gather, 2, 2, (axes, {"place": col_first}), Gather.scratch(WEIGHT_AXES)),
        (Gather, 4, 4, ((PAIR,), {}), Gather.scratch(PAIR)),
        (Gather, 5, 5, ((TOKEN_AXES,), {"place": lanes_of(half)}), Gather.scratch(TOKEN_AXES)),
    ]
    wide = like((t, f, width, 2 * inner), BF16)
    outs = [wide, wide, like((c, t, f) + output.shape, BF16), like((1, stream.shape[0], 2 * stream.shape[1]), BF16)]
    outs += [like((2, 1, scale.shape[0]), F32), like((team, r, rows, 2 * half), BF16)]
    mixer_t, branch_t, output_t, tokens, scale, every = exchange(
        0, lambda: along("t", "f") + across("row", "col"), plan,
        [mixer, branch, output, stream, scale[None], cotangent], outs, [ANY] * 4 + [VMEM, ANY],
    )
    return mixer_t.reshape(-1, 2 * inner), branch_t.reshape(-1, 2 * inner), output_t.reshape(-1, output.shape[1]), tokens[0], scale.reshape(-1), every.reshape(-1, 2 * half)


def fetch_second(normed, gate, up, down, gate_bias, up_bias):
    t, r, _ = shape_of(TOKEN_AXES)
    fleet = lax.axis_size("f")
    rows, width = normed.shape
    units, inner = gate.shape
    share = down.shape[1] // (2 * TEAM)
    piece = (down.shape[0], share)
    half = fleet // 2
    deal = Deal.scratch(piece, BF16)
    token, fan = Gather.scratch(TOKEN_AXES), Fan.scratch("f")
    place = lanes_of(width)
    step = next(n for n in (32, 16, 8, rows) if rows % n == 0)

    def kernel(n_ref, g_ref, u_ref, d_ref, gb, ub, n_all, gw, uw, d_all, g_out, u_out, h_out, held, sem, *rest):
        normed_job = Gather(n_ref, n_all, TOKEN_AXES, rest[:3], place)
        gate_job, up_job = Fan(g_ref, gw, "f", rest[3:6]), Fan(u_ref, uw, "f", rest[6:9])
        down_job = Deal(d_ref, d_all, rest[9:])
        greet(team_peers())
        for job in (normed_job, gate_job, up_job):
            job.begin()
        normed_job.stage(1)
        down_job.begin()
        normed_job.stage(2)
        normed_job.stage(3)
        normed_job.drain()
        for job in (gate_job, up_job):
            job.stage(1)
            job.drain()
        down_job.stage(1)
        blocks = t * r

        def fetch(i):
            return pltpu.make_async_copy(n_all.at[i // r, i % r], held.at[i % 2], sem.at[i % 2])

        fetch(0).start()

        def bend(i, carry):
            at = pl.ds(pl.multiple_of(i * step, step), step)
            v, u = g_out[at, :] + gb[...], u_out[at, :] + ub[...]
            bent = jnp.tanh(GELU * (v + 0.044715 * v * v * v))
            cdf = 0.5 * (1.0 + bent)
            slope = cdf + 0.5 * v * (1.0 - bent * bent) * (GELU * (1.0 + 3.0 * 0.044715 * v * v))
            h_out[at, :] = (v * cdf * u).astype(BF16)
            g_out[at, :] = u * slope
            u_out[at, :] = v * cdf
            return carry

        def product(i, carry):
            @pl.when(i + 1 < blocks)
            def _():
                fetch(i + 1).start()

            fetch(i).wait()
            at = pl.ds(pl.multiple_of(i * rows, rows), rows)
            for weight, out in ((gw, g_out), (uw, u_out)):
                for j in range(half):
                    out[at, j * units : (j + 1) * units] = dot_nt(held[i % 2], weight[j])
            lax.fori_loop(i * (rows // step), (i + 1) * (rows // step), bend, 0)
            return carry

        lax.fori_loop(0, blocks, product, 0)
        down_job.stage(2)
        down_job.drain()

    every = like((t, r, rows, 2 * width), BF16)
    weight = like((half, units, 2 * inner), BF16)
    first = like((t * r * rows, share), F32)
    n_all, gate_t, up_t, down_t, gate_slope, up_slope, hidden = pl.pallas_call(
        kernel,
        out_shape=(every, weight, weight, like((2, t, fleet) + piece, BF16), first, first, like(first.shape, BF16)),
        in_specs=[VMEM] * 6,
        out_specs=(ANY, VMEM, VMEM, ANY, VMEM, VMEM, VMEM),
        scratch_shapes=[pltpu.VMEM((2, rows, 2 * width), BF16), pltpu.SemaphoreType.DMA((2,))]
        + token + fan + fan + deal,
        compiler_params=pltpu.CompilerParams(collective_id=1, has_side_effects=True),
        name="fetch_second",
    )(normed, gate, up, down, gate_bias[None], up_bias[None])
    return (
        n_all.reshape(-1, 2 * width),
        gate_t.reshape(-1, 2 * inner),
        up_t.reshape(-1, 2 * inner),
        down_t.reshape(-1, share),
        gate_slope,
        up_slope,
        hidden,
    )


def diagonal(*axes):
    pairs = zip(across(*axes), [tag for tag in grid_of(axes) if any(tag)])
    return [peer for peer, tag in pairs if all(tag)]


def team_peers():
    return along("t", "row") + across("f", "col") + diagonal("t", "col")


def send_second(gate, up, hidden, gate_t, up_t, second_all, cot_all, late):
    t, r, _ = shape_of(TOKEN_AXES)
    fleet = lax.axis_size("f")
    tokens, wide = second_all.shape
    share = gate.shape[1]
    rows, width = tokens // (t * r), wide // 2
    half = fleet // 2
    units = share // half
    shard = width // (TEAM * fleet)
    block, weight, piece = (rows, width), (units, width), (shard, share)
    lane, tile = 512, wide // 4
    part, chunk = tile // shard, 256
    place = lanes_of(width)
    settle, fold = Settle.scratch(TOKEN_AXES, block, BF16), Fold.scratch("f", weight, BF16)
    undeal = Undeal.scratch(piece, BF16)

    def kernel(*refs):
        g_ref, u_ref, h_ref, gw_ref, uw_ref, all_ref, cot_ref, _ = refs[:8]
        delta_ref, grad_g, grad_u, grad_d = refs[8:12]
        src, fold_g, fold_u, down, gt_ref, ut_ref, ht_ref, tiles, tile_sem = refs[12:21]
        rest = refs[21:]
        sums = Settle(src, delta_ref, TOKEN_AXES, rest[: len(settle)], place)
        rest = rest[len(settle) :]
        g_job = Fold(fold_g, grad_g, "f", rest[: len(fold)])
        u_job = Fold(fold_u, grad_u, "f", rest[len(fold) : 2 * len(fold)])
        d_job = Undeal(down, grad_d, rest[2 * len(fold) :])

        def fetch(ref, i):
            at = pl.ds(pl.multiple_of(i * tile, tile), tile)
            return pltpu.make_async_copy(ref.at[:, at], tiles.at[i % 2], tile_sem.at[i % 2])

        def turn(src_ref, out_ref):
            def some(i, carry):
                at = pl.ds(pl.multiple_of(i * chunk, chunk), chunk)
                out_ref[:, at] = src_ref[at, :].T
                return carry

            lax.fori_loop(0, tokens // chunk, some, 0)

        def down_gradients(i, carry):
            @pl.when(i + 1 < wide // tile)
            def _():
                fetch(cot_ref, i + 1).start()

            @pl.when(i + 1 == wide // tile)
            def _():
                fetch(all_ref, 0).start()

            fetch(cot_ref, i).wait()
            value = dot_nn(ht_ref[...], tiles[i % 2]).T.astype(BF16)
            for j in range(part):
                n = i * part + j
                down[n % fleet, n // fleet % TEAM, n // (TEAM * fleet)] = value[j * shard : (j + 1) * shard]
            return carry

        def block_of(tag):
            coords = sums.coords(tag)
            at = pl.ds(pl.multiple_of((coords[0] * r + coords[1]) * rows, rows), rows)

            def product(j, carry):
                col = pl.ds(pl.multiple_of(j * lane, lane), lane)
                value = dot_nn(g_ref[at, :], gw_ref[:, col]) + dot_nn(u_ref[at, :], uw_ref[:, col])
                src[coords[0], coords[1], :, col] = value.astype(BF16)
                return carry

            lax.fori_loop(0, wide // lane, product, 0)
            for k in offsets("col"):
                sums.forward(tag + (k,), place(src, sums.coords(tag + (k,))))

        def gradients(i, carry):
            @pl.when(i + 1 < wide // tile)
            def _():
                fetch(all_ref, i + 1).start()

            fetch(all_ref, i).wait()
            h, at = i // (width // tile), pl.ds(pl.multiple_of(i % (width // tile) * tile, tile), tile)
            for left, out in ((gt_ref, fold_g), (ut_ref, fold_u)):
                value = dot_nn(left[...], tiles[i % 2]).astype(BF16)
                for j in range(half):
                    out[h, j, :, at] = value[j * units : (j + 1) * units]
            return carry

        def half_gradients(h):
            first = h * (width // tile)
            lax.fori_loop(first, first + width // tile, gradients, 0)
            g_job.begin((h,))
            u_job.begin((h,))

        away = [tag for tag in sums.order(2) if tag[-1]]
        home = [tag for tag in sums.order(2) if not tag[-1]]
        team = sums.order(1)
        fetch(cot_ref, 0).start()
        greet(team_peers())
        turn(h_ref, ht_ref)
        lax.fori_loop(0, wide // tile // 2, down_gradients, 0)
        d_job.begin(0)
        block_of(away[0])
        lax.fori_loop(wide // tile // 2, wide // tile, down_gradients, 0)
        d_job.begin(1)
        sums.step(2, away[0])
        block_of(away[1])
        block_of(home[0])
        sums.step(2, away[1])
        block_of(away[2])
        sums.step(2, home[0])
        sums.step(1, team[0])
        turn(g_ref, gt_ref)
        turn(u_ref, ut_ref)
        half_gradients(0)
        sums.step(2, away[2])
        block_of(away[3])
        block_of(home[1])
        sums.step(2, away[3])
        block_of(home[2])
        sums.step(2, home[1])
        sums.step(1, team[1])
        half_gradients(1)
        d_job.stage(1)
        sums.step(2, home[2])
        block_of(home[3])
        sums.step(1, team[2])
        sums.step(2, home[3])
        sums.step(1, team[3])
        sums.stage(3)
        g_job.stage(1)
        u_job.stage(1)
        d_job.stage(2)
        for job in (sums, g_job, u_job, d_job):
            job.drain()

    delta, grad_gate, grad_up, grad_down = pl.pallas_call(
        kernel,
        out_shape=(like(block, F32), like(weight, BF16), like(weight, BF16), like((TEAM, 2) + piece, BF16)),
        in_specs=[VMEM] * 5 + [ANY] * 3,
        out_specs=(VMEM,) * 4,
        scratch_shapes=[
            pltpu.VMEM((t, r, rows, wide), BF16),
            pltpu.VMEM((2, half) + weight, BF16),
            pltpu.VMEM((2, half) + weight, BF16),
            pltpu.VMEM((fleet, TEAM, 2) + piece, BF16),
            pltpu.VMEM((share, tokens), BF16),
            pltpu.VMEM((share, tokens), BF16),
            pltpu.VMEM((share, tokens), BF16),
            pltpu.VMEM((2, tokens, tile), BF16),
            pltpu.SemaphoreType.DMA((2,)),
        ]
        + settle + fold + fold + undeal,
        compiler_params=pltpu.CompilerParams(
            collective_id=2, has_side_effects=True, vmem_limit_bytes=67_000_000
        ),
        name="send_second",
    )(gate, up, hidden, gate_t, up_t, second_all, cot_all, late)
    return delta, grad_gate, grad_up, grad_down


def to_stream(partial, cid):
    rows, width = partial.shape
    block = (rows, width // 2)
    (out,) = exchange(
        cid, lambda: across("row", "col"),
        [(Fold, 0, 0, (("row",), {}), Fold.scratch("row", block, BF16))],
        [halves(partial).reshape((2, 1) + block)], [like(block, F32)], [VMEM],
    )
    return out


class FanSwap(Fan):
    def __init__(self, src, out, sems, other):
        super().__init__(src, out, "row", sems[:3])
        self.send_on, self.recv_on = sems[3:]
        self.other = other

    @staticmethod
    def scratch():
        return Fan.scratch("row") + Swap.scratch()

    def stage(self, wave):
        super().stage(wave)
        other, width = 1 - lax.axis_index("col"), self.src.shape[-1]
        if wave == 1:
            src = self.out.at[0, :, pl.ds(pl.multiple_of(other * width, width), width)]
            self.push(src, self.other, self.send_on, self.recv_on, {"col": other})
        if wave == 2:
            self.arrive(self.other, self.send_on, self.recv_on, {"col": other})

    def drain(self):
        super().drain()
        Copies.drain(self)


def to_tokens(block, mixed, cid):
    rows, width = block.shape
    fan, gather = FanSwap.scratch(), Gather.scratch(PAIR)

    def kernel(block_ref, mixed_ref, out_ref, other_ref, both_ref, *sems):
        greet(across("row", "col"))
        jobs = [
            FanSwap(block_ref, out_ref, sems[: len(fan)], other_ref),
            Gather(mixed_ref, both_ref, PAIR, sems[len(fan) :]),
        ]
        run_jobs(jobs, ())

    out, other, both = pl.pallas_call(
        kernel,
        out_shape=(like((1, rows, 2 * width), BF16), like(block.shape, BF16), like((2,) + mixed.shape, BF16)),
        in_specs=[VMEM] * 2,
        out_specs=(VMEM,) * 3,
        scratch_shapes=fan + gather,
        compiler_params=pltpu.CompilerParams(collective_id=cid, has_side_effects=True),
        name="to_tokens",
    )(block, mixed)
    both_rows = jnp.concatenate(arrange(half_of(out[0]), other), axis=0)
    return out[0], both_rows, both.reshape(-1, mixed.shape[1])


def dealt(x, axes, dtype):
    sizes = shape_of(axes)
    members = sizes[0] * sizes[1] * sizes[2]
    width = -(-x.size // (members * 8 * 128)) * 128
    flat = jnp.pad(x.reshape(-1), (0, members * 8 * width - x.size))
    return flat.reshape(sizes + (8, width)).astype(dtype)


STREAM_AXES = ("t", "f", "row")


def finish_block(normed, branch, mixer, delta, cid):
    rows, width = delta.shape
    token = (rows, width // 2)
    plan = [
        (Fold, 0, 0, (("row",), {}), Fold.scratch("row", token, BF16)),
        (Swap, 1, 1, ((), {}), Swap.scratch()),
        (Gather, 2, 2, ((PAIR,), {}), Gather.scratch(PAIR)),
        (Gather, 3, 3, ((PAIR,), {}), Gather.scratch(PAIR)),
    ]
    outs = [like(token, F32), like(token, BF16), like((2,) + branch.shape, BF16), like((2,) + mixer.shape, BF16)]
    delta, other, branch, mixer = exchange(
        cid, lambda: across("row", "col"), plan,
        [halves(delta).reshape((2, 1) + token), halves(normed), branch, mixer], outs, [VMEM] * 4,
    )
    rows = jnp.concatenate(arrange(half_of(normed), other), axis=0)
    return delta, rows, branch.reshape(-1, branch.shape[2]), mixer.reshape(-1, mixer.shape[2])


def send_first(grads, inner_sums, head_grads, stream_sums, done, through, cid):
    sizes = shape_of(DP)
    n = len(grads)
    block = (grads[0].shape[0] // (sizes[0] * sizes[1]), grads[0].shape[1])
    axes_of = (ORDER, STREAM_AXES, ORDER)
    sums = (inner_sums, stream_sums, head_grads)
    lanes = head_grads.shape[-1]
    small = [dealt(x, axes, F32) for x, axes in zip(sums[:2], axes_of)]
    small.append(head_grads.reshape(shape_of(ORDER) + (-1, lanes)).astype(BF16))
    plan = [
        (AllReduce, n + i, n + i, ((axes,), {}), AllReduce.scratch(axes, x.shape[3:], x.dtype))
        for i, (x, axes) in enumerate(zip(small, axes_of))
    ]
    plan += [(Reduce, i, i, ((DP,), {}), Reduce.scratch(DP, block, BF16)) for i in range(n)]
    bulk = tuple(range(3, 3 + n))
    pieces = done[2].shape
    wide = [like(done[0].shape, F32), like(done[1].shape, F32), like((pieces[2], 2 * TEAM * pieces[3]), F32)]
    plan += [(cut, n + 3 + i, n + 3 + i, ((), {}), []) for i, cut in enumerate((Widen, Widen, Join))]
    rest = tuple(range(3 + n, 6 + n))
    got = exchange(
        cid, lambda: along("t", "f", "row", "col"), plan,
        [g.reshape(sizes + block) for g in grads] + small + list(done),
        [like(block, F32)] * n + [like(x.shape, x.dtype) for x in small] + wide, [VMEM] * (n + 6),
        order=(0, 1, 2) * 2 + bulk + (0, 1, 2) * 2 + rest * 2 + bulk * 2, through=through,
    )
    return got[:n], [x.reshape(-1)[: y.size].reshape(y.shape).astype(F32) for x, y in zip(got[n : n + 3], sums)], got[n + 3 : -1], got[-1]


def on_device(
    stream,
    scale_first,
    branch_weight,
    branch_bias,
    mixer_weight,
    mixer_bias,
    conv_weight,
    conv_bias,
    decay_weight,
    decay_bias,
    input_weight,
    input_bias,
    decay_param,
    output_weight,
    output_bias,
    scale_second,
    gate_weight,
    gate_bias,
    up_weight,
    up_bias,
    down_weight,
    down_bias,
    cotangent,
):
    mixer_t, branch_t, output_t, stream_all, scale_all, cot_all = fetch_first(
        mixer_weight.T, branch_weight.T, output_weight.T, stream, scale_first, cotangent
    )
    inner = mixer_t.shape[0]
    stream_wide = stream.astype(F32)
    tokens_wide = stream_all.astype(F32)
    inverse_all = lax.rsqrt(jnp.sum(tokens_wide * tokens_wide, axis=1, keepdims=True) / D + EPSILON)
    normed_first = (tokens_wide * inverse_all * (1.0 + scale_all)).astype(BF16)
    mixer_pre = dot_nt(normed_first, mixer_t) + mixer_bias
    branch_pre = dot_nt(normed_first, branch_t) + branch_bias
    branch_act, branch_back = jax.vjp(gelu_tanh, branch_pre)

    steps = mixer_pre.shape[0]
    first_token = lax.axis_index(ORDER) * steps
    position = (first_token + jnp.arange(steps, dtype=jnp.int32)) % LEN
    margin = CONV - 1
    left_edge = from_behind(mixer_pre[steps - margin :], ORDER, 1)
    padded = jnp.concatenate([left_edge, mixer_pre], axis=0)
    conv_out = conv_bias + jnp.zeros_like(mixer_pre)
    for offset in range(CONV):
        in_reach = (position >= offset)[:, None]
        conv_out = conv_out + jnp.where(
            in_reach, conv_weight[offset] * padded[margin - offset : margin - offset + steps], 0.0
        )
    conv_low = conv_out.astype(BF16)
    conv_wide = conv_low.astype(F32)
    heads, block = decay_weight.shape[0], decay_weight.shape[1]
    parts = [conv_low[:, h * block : (h + 1) * block] for h in range(heads)]
    decay_pre = jnp.concatenate([dot_nn(x, decay_weight[h]) for h, x in enumerate(parts)], 1) + decay_bias
    input_pre = jnp.concatenate([dot_nn(x, input_weight[h]) for h, x in enumerate(parts)], 1) + input_bias
    starts = (position == 0)[:, None]

    def gate_values(decay_in, input_in, param_in, conv_in):
        return gates_of(decay_in, input_in, param_in, conv_in, starts)

    (retain, source), gate_back = jax.vjp(gate_values, decay_pre, input_pre, decay_param, conv_wide)
    ones_row = jnp.ones((1, inner), F32)
    states, state_in = recurrence(retain, source, ones_row, False, 3)
    mixed_low = (states * branch_act).astype(BF16)
    first_out = stream_wide + to_stream(dot_nt(mixed_low, output_t).astype(BF16), 4) + output_bias
    second_total, first_total = pair_sum(
        [jnp.sum(x * x, axis=1, keepdims=True) for x in (first_out, stream_wide)], 5
    )
    inverse_second = lax.rsqrt(second_total / D + EPSILON)
    inverse_first = lax.rsqrt(first_total / D + EPSILON)
    normed_second = first_out * inverse_second * (1.0 + scale_second)

    share = down_weight.shape[0] // (2 * TEAM)
    mine = (lax.axis_index("t") * 2 + lax.axis_index("col")) * share
    gate_b = lax.dynamic_slice(gate_bias, (mine,), (share,))
    up_b = lax.dynamic_slice(up_bias, (mine,), (share,))

    second_all, gate_t, up_t, down_t, gate_slope, up_slope, hidden_low = fetch_second(
        normed_second.astype(BF16), gate_weight.T, up_weight.T, down_weight.T, gate_b, up_b
    )
    delta_hidden = dot_nn(cot_all, down_t)
    delta_gate, delta_up = delta_hidden * gate_slope, delta_hidden * up_slope
    gate_low, up_low = delta_gate.astype(BF16), delta_up.astype(BF16)
    down_part = dot_nt(hidden_low, down_t).astype(BF16)
    down_rows = lax.psum_scatter(down_part, "col", scatter_dimension=1, tiled=True)
    delta_second, grad_gate, grad_up, grad_down = send_second(
        gate_low, up_low, hidden_low, gate_t, up_t, second_all, cot_all, down_part
    )
    delta_result = cotangent.astype(F32)

    norm_second_part, grad_scale_second, down_rows = normalize_back(
        delta_second, first_out, inverse_second, scale_second, 6, down_rows
    )
    down_proj = lax.psum_scatter(down_rows, ("t", "row"), scatter_dimension=0, tiled=True)
    delta_first = delta_result + norm_second_part
    out_all, out_rows, mixed_rows = to_tokens(delta_first.astype(BF16), mixed_low, 7)
    output_part = dot_tn(out_rows, mixed_rows).astype(BF16)
    grad_output = lax.psum_scatter(output_part, DP, scatter_dimension=0, tiled=True)
    delta_mixed = dot_nn(out_all, output_t)
    delta_state = delta_mixed * branch_act
    (delta_branch,) = branch_back(delta_mixed * states)
    branch_low = delta_branch.astype(BF16)
    retain_next = jnp.concatenate([retain[1:], ones_row], axis=0)
    back_state, _ = recurrence(retain_next, delta_state, retain[:1], True, 8)
    state_prev = jnp.concatenate([state_in[None], states[:-1]], axis=0)
    delta_decay_pre, delta_input_pre, grad_decay_param, delta_conv = gate_back(
        (back_state * state_prev, back_state)
    )
    decay_low = delta_decay_pre.astype(BF16)
    input_low = delta_input_pre.astype(BF16)

    def split(x):
        return [x[:, h * block : (h + 1) * block] for h in range(heads)]

    grad_decay_weight = jnp.stack([dot_tn(a, b) for a, b in zip(parts, split(decay_low))])
    grad_input_weight = jnp.stack([dot_tn(a, b) for a, b in zip(parts, split(input_low))])
    delta_conv = delta_conv + jnp.concatenate(
        [dot_nt(a, decay_weight[h]) for h, a in enumerate(split(decay_low))], 1
    )
    delta_conv = delta_conv + jnp.concatenate(
        [dot_nt(a, input_weight[h]) for h, a in enumerate(split(input_low))], 1
    )
    delta_padded = jnp.zeros_like(padded)
    conv_grads = []
    for offset in range(CONV):
        in_reach = (position >= offset)[:, None]
        masked = jnp.where(in_reach, delta_conv, 0.0)
        conv_grads.append(
            jnp.sum(masked * padded[margin - offset : margin - offset + steps], axis=0)
        )
        delta_padded = delta_padded + jnp.pad(
            masked * conv_weight[offset], ((margin - offset, offset), (0, 0))
        )
    grad_conv_weight = jnp.stack(conv_grads, axis=0)
    right_edge = from_behind(delta_padded[:margin], ORDER, -1)
    delta_mixer = delta_padded[margin:] + jnp.pad(right_edge, ((steps - margin, 0), (0, 0)))
    mixer_low = delta_mixer.astype(BF16)

    def spread(x):
        return lax.dynamic_update_slice(jnp.zeros_like(gate_bias), x, (mine,))

    small = [
        jnp.sum(delta_branch, axis=0),
        jnp.sum(delta_mixer, axis=0),
        jnp.sum(delta_conv, axis=0),
        jnp.sum(delta_decay_pre, axis=0),
        jnp.sum(delta_input_pre, axis=0),
        grad_decay_param,
        spread(jnp.sum(delta_gate, axis=0)),
        spread(jnp.sum(delta_up, axis=0)),
        grad_conv_weight.reshape(-1),
    ]
    delta_normed_part = dot_nn(branch_low, branch_t) + dot_nn(mixer_low, mixer_t)
    delta_normed_first, first_rows, branch_rows, mixer_rows = finish_block(
        normed_first, branch_low, mixer_low, delta_normed_part.astype(BF16), 10
    )
    norm_first_part, grad_scale_first = normalize_back(
        delta_normed_first, stream_wide, inverse_first, scale_first, 12
    )
    (grad_mixer, grad_branch), (total, stream_sums, head_grads), wide_grads, down_proj = send_first(
        [dot_tn(mixer_rows, first_rows).astype(BF16), dot_tn(branch_rows, first_rows).astype(BF16)],
        jnp.concatenate(small),
        jnp.stack([grad_decay_weight, grad_input_weight]),
        jnp.stack(
            [grad_scale_second, jnp.sum(delta_first, axis=0), jnp.sum(delta_result, axis=0), grad_scale_first]
        ),
        (grad_gate, grad_up, grad_down),
        down_proj,
        13,
    )
    result = (first_out + down_proj.astype(F32) + down_bias).astype(BF16)
    grad_stream = delta_first + norm_first_part
    sums, at = [], 0
    for x in small:
        sums.append(total[at : at + x.shape[0]])
        at += x.shape[0]
    return (
        result,
        grad_stream,
        stream_sums[3],
        grad_branch.T,
        sums[0],
        grad_mixer.T,
        sums[1],
        sums[8].reshape(CONV, inner),
        sums[2],
        head_grads[0],
        sums[3],
        head_grads[1],
        sums[4],
        sums[5],
        grad_output.T.astype(F32),
        stream_sums[1],
        stream_sums[0],
        wide_grads[0].T,
        sums[6],
        wide_grads[1].T,
        sums[7],
        wide_grads[2].T,
        stream_sums[2],
    )


def solution(mesh):
    shape = mesh.devices.shape
    names = mesh.axis_names
    fleet = mesh.shape["dp"] // TEAM
    at = names.index("dp")
    split_mesh = Mesh(
        mesh.devices.reshape(shape[:at] + (TEAM, fleet) + shape[at + 1 :]),
        names[:at] + DP + names[at + 1 :],
    )
    tokens, fan_in = P((*DP, "row"), "col"), P("col", ("row", *DP))
    fan_out, inner, wide = P("row", ("col", *DP)), P("row"), P("col")
    heads = P("row", None, None)
    return jax.shard_map(
        on_device,
        mesh=split_mesh,
        in_specs=(
            tokens, wide, fan_in, inner, fan_in, inner, P(None, "row"), inner,
            heads, inner, heads, inner, inner, fan_out, wide, wide,
            fan_in, inner, fan_in, inner, fan_out, wide, tokens,
        ),
        out_specs=(
            tokens, tokens, wide, fan_in, inner, fan_in, inner, P(None, "row"), inner,
            heads, inner, heads, inner, inner, fan_out, wide, wide,
            fan_in, inner, fan_in, inner, fan_out, wide,
        ),
        check_vma=False,
    )
```
